128 devices in a mesh: gx: 8 (over x_lo, z), gy: 4 (over x_hi, core), gz: 4 (over y).
Axes of the slice: x: 4 (x_hi: 2, x_lo: 2; x = x_hi * 2 + x_lo), y: 4, z: 4, core: 2. Of those that a mesh axis runs over, the one named last changes fastest.
Arguments:
- field: bfloat16 [81, 64, 64, 1024], P(None, 'gx', 'gy', 'gz'), may hold values from -6 to 6
- samples: int32 [3, 8, 524288], P(None, None, ('gx', 'gy', 'gz')), may hold values from 0 to 1023, as said below
- weights: float32 [8, 524288], P(None, ('gx', 'gy', 'gz')), may hold values from 0.05 to 0.25
- destination: int32 [2, 524288], P(None, ('gx', 'gy', 'gz')), may hold values from 0 to 127, as said below
- transfer: bfloat16 [81, 524288], P(None, ('gx', 'gy', 'gz')), may hold values from -5 to 5
Outputs:
- shadowed: bfloat16 [81, 524288], P(None, ('gx', 'gy', 'gz'))
The draws below stay inside these ranges and needn't reach their ends.
Inputs may be any that keep to these rules, and one draw needn't show every extreme that they name: Number the devices with gz fastest and gx slowest; device b holds grid cells b_x * 8 to (b_x + 1) * 8 - 1 along the first dimension and likewise along the others. Every sample of a receiver in the b-th block of 4096 receivers lies at most 2 cells, periodically along each dimension, outside device b's cells; samples[0] is below 64, samples[1] below 64, samples[2] below 1024. destination[0] is below 128 and destination[1] below 32. Of the b-th block of 4096 receivers exactly 32 have each value of destination[0], and those take each value of destination[1] once, so the columns of the output are a permutation of the receivers.
All inputs are finite; a program needn't handle non-finite values.
Results may differ from the reference program's by a relative error of at most 0.011.
Values may be sent and summed in bfloat16 or wider, within the bound.
No kernel may reach another device: no remote copies, remote signals or barrier semaphores. Data moves between devices by JAX's collectives and lax.ppermute only.
A program may use at most 128 MiB of HBM per device.

```python
import math
import jax
import jax.numpy as jnp
from jax import lax

CX = 8
CY = 16
CZ = 256
RECV_DEV = 4096
HALO = 2
SAMPLES = 8
DEGREES = 9
POLAR = 32
AZIMUTH = 32
COEFFS = 81
NX = 64
NY = 64
NZ = 1024
RECEIVERS = 524288
PER_PAIR = 32
N_GX = 8
N_GY = 4
N_GZ = 4


def draw_samples(key, part):
    receiver = jnp.arange(RECEIVERS, dtype=jnp.int32)
    block = receiver // RECV_DEV
    block_x = block // (N_GY * N_GZ)
    block_y = block // N_GZ % N_GY
    block_z = block % N_GZ
    subkeys = jax.random.split(key, 3)
    offset_x = jax.random.randint(subkeys[0], (SAMPLES, RECEIVERS), -HALO, CX + HALO, dtype=jnp.int32)
    offset_y = jax.random.randint(subkeys[1], (SAMPLES, RECEIVERS), -HALO, CY + HALO, dtype=jnp.int32)
    offset_z = jax.random.randint(subkeys[2], (SAMPLES, RECEIVERS), -HALO, CZ + HALO, dtype=jnp.int32)
    coord_x = (block_x[None, :] * CX + offset_x) % NX
    coord_y = (block_y[None, :] * CY + offset_y) % NY
    coord_z = (block_z[None, :] * CZ + offset_z) % NZ
    return jnp.stack([coord_x, coord_y, coord_z]).astype(jnp.int32)


def draw_destination(key, part):
    devices = N_GX * N_GY * N_GZ
    scores = jax.random.randint(key, (devices, RECV_DEV), 0, 4096, dtype=jnp.int32) * RECV_DEV + jnp.arange(RECV_DEV, dtype=jnp.int32)[None, :]
    ordering = jnp.argsort(scores, axis=1, stable=True).astype(jnp.int32)
    owners = ordering // PER_PAIR
    inside = ordering % PER_PAIR
    return jnp.stack([owners.reshape(RECEIVERS), inside.reshape(RECEIVERS)]).astype(jnp.int32)


def level_of(own_key, dims, shards, least, high):
    def one(position, blocks):
        draws = jax.random.uniform(jax.random.fold_in(jax.random.fold_in(own_key, 6), position), (blocks,), jnp.float32, least / len(shards), high / len(shards))
        return jnp.repeat(jnp.exp(draws), dims[position] // blocks).reshape((-1,) + (1,) * (len(dims) - position - 1))

    level = one(*shards[0])
    for cut in shards[1:]:
        level = level * one(*cut)
    return level


def normal_values(key, dims, deviation, most, cuts=(), kind=jnp.bfloat16):
    loudness = level_of(key, dims, cuts, -0.22, 0.18) if cuts else 1.0
    array = jax.random.normal(key, dims, jnp.float32) * deviation * loudness
    return jnp.minimum(jnp.maximum(array, -most), most).astype(kind)


def setup_inputs(seed: int = 0) -> dict:
    seeds = jax.random.split(jax.random.key(seed), 6)
    return {
        "field": normal_values(seeds[0], (COEFFS, NX, NY, NZ), 1.0, 6.0, ((1, 8), (2, 4), (3, 4))),
        "samples": draw_samples(jax.random.fold_in(seeds[5], 71), 0),
        "weights": jnp.clip(0.05 + 0.2 * jax.random.uniform(seeds[2], (SAMPLES, RECEIVERS), jnp.float32) ** level_of(seeds[2], (SAMPLES, RECEIVERS), ((1, 128),), -0.2, 0.2), 0.05, 0.25),
        "destination": draw_destination(jax.random.fold_in(seeds[5], 71), 0),
        "transfer": normal_values(seeds[4], (COEFFS, RECEIVERS), 0.8, 5.0, ((1, 128),)),
    }


def harmonic_values(cosines, angles):
    sines = jnp.sqrt(jnp.maximum(1.0 - cosines * cosines, 0.0))
    entries = {}
    for azimuthal in range(DEGREES):
        diagonal_term = (-1.0) ** azimuthal * float(math.prod(range(1, 2 * azimuthal, 2))) * sines ** azimuthal
        legendre = {azimuthal: diagonal_term}
        if azimuthal + 1 < DEGREES:
            legendre[azimuthal + 1] = cosines * (2 * azimuthal + 1) * diagonal_term
        for degree in range(azimuthal + 2, DEGREES):
            legendre[degree] = ((2 * degree - 1) * cosines * legendre[degree - 1] - (degree + azimuthal - 1) * legendre[degree - 2]) / (degree - azimuthal)
        for degree in range(azimuthal, DEGREES):
            factor = math.sqrt((2 * degree + 1) / (4.0 * math.pi) * math.factorial(degree - azimuthal) / math.factorial(degree + azimuthal))
            if azimuthal == 0:
                entries[degree, 0] = factor * legendre[degree]
            else:
                entries[degree, azimuthal] = math.sqrt(2.0) * factor * jnp.cos(azimuthal * angles) * legendre[degree]
                entries[degree, -azimuthal] = math.sqrt(2.0) * factor * jnp.sin(azimuthal * angles) * legendre[degree]
    return jnp.stack([entries[degree, signed] for degree in range(DEGREES) for signed in range(-degree, degree + 1)])

def direction_tables():
    polar_cos = (jnp.arange(POLAR, dtype=jnp.float32) + 0.5) * (2.0 / POLAR) - 1.0
    beside_all = (jnp.arange(AZIMUTH, dtype=jnp.float32) + 0.5) * (2.0 * math.pi / AZIMUTH)
    cosines = jnp.repeat(polar_cos, AZIMUTH)
    angles = jnp.tile(beside_all, POLAR)
    values = harmonic_values(cosines, angles)
    basis = values.T.astype(jnp.bfloat16)
    projector = (values * (4.0 * math.pi / (POLAR * AZIMUTH))).astype(jnp.bfloat16)
    return (basis, projector)

def triple_product(transfer_block, shadow_block, basis, projector):
    transfer_dirs = jnp.dot(basis, transfer_block, preferred_element_type=jnp.float32)
    shadow_dirs = jnp.dot(basis, shadow_block, preferred_element_type=jnp.float32)
    product = (transfer_dirs * shadow_dirs).astype(jnp.bfloat16)
    return jnp.dot(projector, product, preferred_element_type=jnp.float32).astype(jnp.bfloat16)

def reference(field, samples, weights, destination, transfer):
    basis, projector = direction_tables()
    flat_field = field.reshape(COEFFS, NX * NY * NZ)
    blocks = RECEIVERS // RECV_DEV
    flat_index = ((samples[0] * NY + samples[1]) * NZ + samples[2]).astype(jnp.int32)

    def interpolate(index):
        start = (index * RECV_DEV).astype(jnp.int32)
        columns = lax.dynamic_slice_in_dim(flat_index, start, RECV_DEV, 1)
        block_weights = lax.dynamic_slice_in_dim(weights, start, RECV_DEV, 1)
        gathered = jnp.take(flat_field, columns.reshape(-1), axis=1).reshape(COEFFS, SAMPLES, RECV_DEV)
        return lax.optimization_barrier(jnp.sum(gathered.astype(jnp.float32) * block_weights[None].astype(jnp.float32), axis=1)).astype(jnp.bfloat16)
    pieces = lax.map(interpolate, jnp.arange(blocks, dtype=jnp.int32))
    visibility = jnp.transpose(pieces, (1, 0, 2)).reshape(COEFFS, RECEIVERS)
    source_block = jnp.arange(RECEIVERS, dtype=jnp.int32) // RECV_DEV
    columns_out = (destination[0] * RECV_DEV + source_block * PER_PAIR + destination[1]).astype(jnp.int32)
    routed = jnp.zeros((COEFFS, RECEIVERS), jnp.bfloat16).at[:, columns_out].set(visibility)

    def relight(index):
        start = (index * RECV_DEV).astype(jnp.int32)
        transfer_block = lax.dynamic_slice_in_dim(transfer, start, RECV_DEV, 1)
        shadow_block = lax.dynamic_slice_in_dim(routed, start, RECV_DEV, 1)
        return triple_product(transfer_block, shadow_block, basis, projector)
    results = lax.map(relight, jnp.arange(blocks, dtype=jnp.int32))
    return jnp.transpose(results, (1, 0, 2)).reshape(COEFFS, RECEIVERS)
```

```python
import math

import jax
import jax.numpy as jnp
import numpy as np
from jax import lax
from jax.experimental import pallas as pl
from jax.experimental.pallas import tpu as pltpu
from jax.sharding import PartitionSpec as P

HALO = 2
SAMPLES = 8
DEGREES = 9
POLAR = 32
AZIMUTH = 32
LANES = 128
MIB = 1024 * 1024


def harmonic_values():
    polar = (np.arange(POLAR, dtype=np.float64) + 0.5) * (2.0 / POLAR) - 1.0
    beside = (np.arange(AZIMUTH, dtype=np.float64) + 0.5) * (2.0 * math.pi / AZIMUTH)
    cosines = np.repeat(polar, AZIMUTH)
    angles = np.tile(beside, POLAR)
    sines = np.sqrt(np.maximum(1.0 - cosines * cosines, 0.0))
    entries = {}
    for m in range(DEGREES):
        diagonal = (-1.0) ** m * float(math.prod(range(1, 2 * m, 2))) * sines**m
        legendre = {m: diagonal}
        if m + 1 < DEGREES:
            legendre[m + 1] = cosines * (2 * m + 1) * diagonal
        for l in range(m + 2, DEGREES):
            legendre[l] = (
                (2 * l - 1) * cosines * legendre[l - 1] - (l + m - 1) * legendre[l - 2]
            ) / (l - m)
        for l in range(m, DEGREES):
            factor = math.sqrt(
                (2 * l + 1) / (4.0 * math.pi) * math.factorial(l - m) / math.factorial(l + m)
            )
            if m == 0:
                entries[l, 0] = factor * legendre[l]
            else:
                entries[l, m] = math.sqrt(2.0) * factor * np.cos(m * angles) * legendre[l]
                entries[l, -m] = math.sqrt(2.0) * factor * np.sin(m * angles) * legendre[l]
    return np.stack([entries[l, m] for l in range(DEGREES) for m in range(-l, l + 1)])


def direction_tables():
    values = harmonic_values()
    basis = values.T.astype(np.float32).astype(jnp.bfloat16)
    projector = (values * (4.0 * math.pi / (POLAR * AZIMUTH))).astype(np.float32)
    return basis, projector.astype(jnp.bfloat16)


def build_planes(planes, coeffs, rows_y, cells_z, base, buf, sems, spread, eye, table):
    halves = cells_z // LANES
    keep = -(-coeffs // 16) * 16
    zeros = jnp.zeros((LANES - keep, cells_z), jnp.bfloat16)

    def one(p, _):
        pltpu.make_async_copy(planes(0), buf.at[p], sems.at[p]).wait()
        for c in range(coeffs):
            for h in range(halves):
                block = buf[p, c, :, h * LANES : (h + 1) * LANES].astype(jnp.float32)
                spread[h, pl.ds(c, rows_y, stride=coeffs), :] = block
        for y in range(0, rows_y, 2):
            parts = []
            for i in (y, y + 1):
                rows = jnp.concatenate(
                    [spread[h, i * coeffs : i * coeffs + keep, :] for h in range(halves)], axis=1
                )
                parts += [rows.astype(jnp.bfloat16), zeros]
            both = lax.dot_general(
                eye[...],
                jnp.concatenate(parts, axis=0),
                (((1,), (1,)), ((), ())),
                preferred_element_type=jnp.float32,
            )
            at = pl.multiple_of(base + (p * rows_y + y) * cells_z, 8)
            table[pl.ds(at, cells_z), :] = both[:, :LANES]
            table[pl.ds(at + cells_z, cells_z), :] = both[:, LANES:]
        return 0

    return one


def own_table(field, eye, total_rows):
    coeffs, cells_x, cells_y, cells_z = field.shape

    def kernel(field, eye, table, buf, sems, spread):
        for x in range(cells_x):
            pltpu.make_async_copy(field.at[:, x], buf.at[x], sems.at[x]).start()
        one = build_planes(
            lambda p: field.at[:, p], coeffs, cells_y, cells_z, 0, buf, sems, spread, eye, table
        )
        lax.fori_loop(0, cells_x, one, 0)

    return pl.pallas_call(
        kernel,
        out_shape=pltpu.VMEM((total_rows, LANES), jnp.float32),
        in_specs=[
            pl.BlockSpec(memory_space=pl.ANY),
            pl.BlockSpec(memory_space=pltpu.VMEM),
        ],
        out_specs=pl.BlockSpec(memory_space=pltpu.VMEM),
        scratch_shapes=[
            pltpu.VMEM((cells_x, coeffs, cells_y, cells_z), jnp.bfloat16),
            pltpu.SemaphoreType.DMA((cells_x,)),
            pltpu.VMEM((cells_z // LANES, cells_y * coeffs + 16, LANES), jnp.float32),
        ],
        compiler_params=pltpu.CompilerParams(vmem_limit_bytes=24 * MIB),
        cost_estimate=pl.CostEstimate(
            flops=2 * 10**10, transcendentals=0, bytes_accessed=2 * 10**7
        ),
        name="own_table",
    )(field, eye)


def halo_table(table, xlo, xhi, ylo, yhi, corners, eye, first_line):
    coeffs, _, cells_y, cells_z = xlo.shape
    count = 2 * HALO + 3
    lines = first_line + count * cells_y

    def kernel(_, xlo, xhi, ylo, yhi, corners, eye, table, zhi, zlo, buf, sems, spread):
        sources = [xlo.at[:, 0], xlo.at[:, 1], xhi.at[:, 0], xhi.at[:, 1], ylo, yhi, corners]
        for p, source in enumerate(sources):
            pltpu.make_async_copy(source, buf.at[p], sems.at[p]).start()
        one = build_planes(
            lambda p: ylo,
            coeffs,
            cells_y,
            cells_z,
            first_line * cells_z,
            buf,
            sems,
            spread,
            eye,
            table,
        )
        lax.fori_loop(0, count, one, 0)
        for out, start in ((zhi, 0), (zlo, cells_z - HALO)):
            for j in range(HALO):
                for line in range(0, lines, 16):
                    parts = [
                        table[pl.ds((line + i) * cells_z + start + j, 8, stride=cells_z), :]
                        for i in (0, 8)
                    ]
                    out[j * lines + line : j * lines + line + 16, :] = jnp.concatenate(
                        parts, axis=0
                    ).astype(jnp.bfloat16)

    edge = jax.ShapeDtypeStruct((HALO * lines, LANES), jnp.bfloat16)
    vmem = pl.BlockSpec(memory_space=pltpu.VMEM)
    hbm = pl.BlockSpec(memory_space=pl.ANY)
    return pl.pallas_call(
        kernel,
        out_shape=(pltpu.VMEM(table.shape, jnp.float32), edge, edge),
        in_specs=[vmem] + [hbm] * 5 + [vmem],
        out_specs=(vmem, vmem, vmem),
        scratch_shapes=[
            pltpu.VMEM((count, coeffs, cells_y, cells_z), jnp.bfloat16),
            pltpu.SemaphoreType.DMA((count,)),
            pltpu.VMEM((cells_z // LANES, cells_y * coeffs + 16, LANES), jnp.float32),
        ],
        input_output_aliases={0: 0},
        compiler_params=pltpu.CompilerParams(vmem_limit_bytes=24 * MIB),
        cost_estimate=pl.CostEstimate(
            flops=2 * 10**10, transcendentals=0, bytes_accessed=2 * 10**7
        ),
        name="halo_table",
    )(table, xlo, xhi, ylo, yhi, corners, eye)


GROUPS = 2


def gather_rows(index, slot, weights, table, zlo, zhi, first_edge, coeffs):
    receivers = slot.shape[0]
    edges = zlo.shape[0]
    steps = receivers // (8 * GROUPS)

    def kernel(index, slot, weights, zlo, zhi, table_in, table, out, rows):
        table[pl.ds(first_edge, edges), :] = zlo[...].astype(jnp.float32)
        table[pl.ds(first_edge + edges, edges), :] = zhi[...].astype(jnp.float32)
        sublane = lax.broadcasted_iota(jnp.int32, (8, LANES), 0)
        masks = [sublane == k for k in range(8)]
        used = lax.broadcasted_iota(jnp.int32, (8, LANES), 1) < coeffs

        def spread_weights(g):
            result = []
            for q in range(GROUPS):
                tile = weights[pl.ds(pl.multiple_of((g * GROUPS + q) * 8, 8), 8), :]
                for s in range(SAMPLES):
                    result.append(jnp.broadcast_to(tile[:, s : s + 1], (8, LANES)))
            return tuple(result)

        def body(g, scales):
            following = spread_weights(jnp.minimum(g + 1, steps - 1))
            index_g = index.at[pl.ds(g * (64 * GROUPS), 64 * GROUPS)]
            slot_g = slot.at[pl.ds(g * (8 * GROUPS), 8 * GROUPS)]
            for q in range(GROUPS):
                total = None
                for s in range(SAMPLES):
                    merged = None
                    for k in range(8):
                        row = table[pl.ds(index_g[q * 64 + s * 8 + k], 8, stride=0), :]
                        merged = row if merged is None else jnp.where(masks[k], row, merged)
                    term = merged * scales[q * 8 + s]
                    total = term if total is None else total + term
                total = jnp.where(used, total, 0.0)
                for k in range(8):
                    rows[pl.ds(slot_g[q * 8 + k], 1), :] = total[k : k + 1, :]
            return following

        lax.fori_loop(0, steps, body, spread_weights(0))

        def convert(i, _):
            at = pl.multiple_of(i * 256, 256)
            out[pl.ds(at, 256), :] = rows[pl.ds(at, 256), :].astype(jnp.bfloat16)
            return 0

        lax.fori_loop(0, receivers // 256, convert, 0)

    vmem = pl.BlockSpec(memory_space=pltpu.VMEM)
    smem = pl.BlockSpec(memory_space=pltpu.SMEM)
    return pl.pallas_call(
        kernel,
        out_shape=(
            pltpu.VMEM(table.shape, jnp.float32),
            jax.ShapeDtypeStruct((receivers, LANES), jnp.bfloat16),
        ),
        in_specs=[smem, smem, vmem, vmem, vmem, vmem],
        out_specs=(vmem, vmem),
        scratch_shapes=[pltpu.VMEM((receivers, LANES), jnp.float32)],
        input_output_aliases={5: 0},
        compiler_params=pltpu.CompilerParams(vmem_limit_bytes=24 * MIB),
        cost_estimate=pl.CostEstimate(
            flops=4 * 10**10, transcendentals=0, bytes_accessed=2 * 10**7
        ),
        name="gather_rows",
    )(index, slot, weights, zlo, zhi, table)[1]


def relight(transfer, routed, basis, projector):
    coeffs, count = transfer.shape
    block = 512

    def kernel(transfer, routed, basis, wide, projector, out):
        lit = jnp.dot(basis[...], transfer[...], preferred_element_type=jnp.float32)
        shade = lax.dot_general(
            wide[...],
            routed[...],
            (((1,), (1,)), ((), ())),
            preferred_element_type=jnp.float32,
        )
        product = (lit * shade).astype(jnp.bfloat16)
        out[...] = jnp.dot(projector[...], product, preferred_element_type=jnp.float32).astype(
            jnp.bfloat16
        )

    directions = basis.shape[0]
    wide = np.zeros((directions, LANES), jnp.bfloat16)
    wide[:, :coeffs] = basis
    return pl.pallas_call(
        kernel,
        out_shape=jax.ShapeDtypeStruct((coeffs, count), jnp.bfloat16),
        grid=(count // block,),
        in_specs=[
            pl.BlockSpec((coeffs, block), lambda i: (0, i)),
            pl.BlockSpec((block, LANES), lambda i: (i, 0)),
            pl.BlockSpec((directions, coeffs), lambda i: (0, 0)),
            pl.BlockSpec((directions, LANES), lambda i: (0, 0)),
            pl.BlockSpec((coeffs, directions), lambda i: (0, 0)),
        ],
        out_specs=pl.BlockSpec((coeffs, block), lambda i: (0, i)),
        compiler_params=pltpu.CompilerParams(vmem_limit_bytes=40 * MIB),
        name="relight",
    )(transfer, routed, jnp.asarray(basis), jnp.asarray(wide), jnp.asarray(projector))


def ring(axis):
    count = lax.axis_size(axis)
    forward = [(i, (i + 1) % count) for i in range(count)]
    return forward, [(target, source) for source, target in forward]


def per_device(field, samples, weights, destination, transfer):
    basis, projector = direction_tables()
    coeffs, cells_x, cells_y, cells_z = field.shape
    count = transfer.shape[1]
    along_x = lax.axis_size("gx")
    along_y = lax.axis_size("gy")
    along_z = lax.axis_size("gz")
    up_x, down_x = ring("gx")
    up_y, down_y = ring("gy")
    up_z, down_z = ring("gz")

    xlo = lax.ppermute(field[:, cells_x - HALO :], "gx", up_x)
    xhi = lax.ppermute(field[:, :HALO], "gx", down_x)
    plane = (coeffs, cells_x * HALO, cells_z)
    ylo = lax.ppermute(field[:, :, cells_y - HALO :].reshape(plane), "gy", up_y)
    yhi = lax.ppermute(field[:, :, :HALO].reshape(plane), "gy", down_y)
    half = (coeffs, 2 * HALO * HALO, cells_z)
    outer = jnp.concatenate([xlo[:, :, cells_y - HALO :], xhi[:, :, cells_y - HALO :]], axis=1)
    inner = jnp.concatenate([xlo[:, :, :HALO], xhi[:, :, :HALO]], axis=1)
    corner_lo = lax.ppermute(outer.reshape(half), "gy", up_y)
    corner_hi = lax.ppermute(inner.reshape(half), "gy", down_y)
    corners = jnp.concatenate([corner_lo, corner_hi], axis=1)

    own_lines = cells_x * cells_y
    lines = own_lines + (2 * HALO + 3) * cells_y
    rows = lines * cells_z
    total_rows = rows + 2 * HALO * lines

    near_x = (samples[0] - lax.axis_index("gx") * cells_x + HALO) % (cells_x * along_x)
    near_y = (samples[1] - lax.axis_index("gy") * cells_y + HALO) % (cells_y * along_y)
    near_z = (samples[2] - lax.axis_index("gz") * cells_z + HALO) % (cells_z * along_z)
    own_x = (near_x >= HALO) & (near_x < HALO + cells_x)
    own_y = (near_y >= HALO) & (near_y < HALO + cells_y)
    low_y = near_y < HALO
    side_x = jnp.where(near_x < HALO, near_x, near_x - cells_x)
    side_y = jnp.where(low_y, near_y, near_y - HALO - cells_y)
    line_own = jnp.where(own_x, near_x - HALO, cells_x + side_x) * cells_y + near_y - HALO
    line_y = (
        (cells_x + 2 * HALO + jnp.where(low_y, 0, 1)) * cells_y + (near_x - HALO) * HALO + side_y
    )
    line_corner = (
        (cells_x + 2 * HALO + 2) * cells_y
        + jnp.where(low_y, 0, 2 * HALO * HALO)
        + side_x * HALO
        + side_y
    )
    line = jnp.where(own_y, line_own, jnp.where(own_x, line_y, line_corner))
    inside = line * cells_z + near_z - HALO
    below = rows + near_z * lines + line
    above = rows + (HALO + near_z - HALO - cells_z) * lines + line
    position = jnp.where(
        near_z < HALO, below, jnp.where(near_z < HALO + cells_z, inside, above)
    )
    index = position.reshape(SAMPLES, count // 8, 8).transpose(1, 0, 2).reshape(-1)
    devices = along_x * along_y * along_z
    per_pair = count // devices
    slot = destination[0] * per_pair + destination[1]

    eye = jnp.asarray(np.eye(cells_z, dtype=np.float32).astype(jnp.bfloat16))
    table = own_table(field, eye, total_rows)
    table, edge_lo, edge_hi = halo_table(table, xlo, xhi, ylo, yhi, corners, eye, own_lines)
    zhi = lax.ppermute(edge_lo, "gz", down_z)
    zlo = lax.ppermute(edge_hi, "gz", up_z)
    outgoing = gather_rows(index, slot, weights.T, table, zlo, zhi, rows, coeffs)
    routed = lax.all_to_all(
        outgoing.reshape(devices, per_pair, LANES),
        ("gx", "gy", "gz"),
        split_axis=0,
        concat_axis=0,
        tiled=True,
    ).reshape(count, LANES)
    return relight(transfer, routed, basis, projector)


def solution(mesh):
    placed = (
        P(None, "gx", "gy", "gz"),
        P(None, None, ("gx", "gy", "gz")),
        P(None, ("gx", "gy", "gz")),
        P(None, ("gx", "gy", "gz")),
        P(None, ("gx", "gy", "gz")),
    )
    return jax.shard_map(
        per_device,
        mesh=mesh,
        in_specs=placed,
        out_specs=P(None, ("gx", "gy", "gz")),
        check_vma=False,
    )
```

```python
import math

import jax
import jax.numpy as jnp
import numpy as np
from jax import lax
from jax.experimental import pallas as pl
from jax.experimental.pallas import tpu as pltpu
from jax.sharding import PartitionSpec as P


HALO = 2
SAMPLES = 8
DEGREES = 9
POLAR = 32
AZIMUTH = 32
LANES = 128
MIB = 1024 * 1024


def harmonic_values():
    polar = (np.arange(POLAR, dtype=np.float64) + 0.5) * (2.0 / POLAR) - 1.0
    beside = (np.arange(AZIMUTH, dtype=np.float64) + 0.5) * (2.0 * math.pi / AZIMUTH)
    cosines = np.repeat(polar, AZIMUTH)
    angles = np.tile(beside, POLAR)
    sines = np.sqrt(np.maximum(1.0 - cosines * cosines, 0.0))
    entries = {}
    for m in range(DEGREES):
        diagonal = (-1.0) ** m * float(math.prod(range(1, 2 * m, 2))) * sines**m
        legendre = {m: diagonal}
        if m + 1 < DEGREES:
            legendre[m + 1] = cosines * (2 * m + 1) * diagonal
        for l in range(m + 2, DEGREES):
            legendre[l] = (
                (2 * l - 1) * cosines * legendre[l - 1] - (l + m - 1) * legendre[l - 2]
            ) / (l - m)
        for l in range(m, DEGREES):
            factor = math.sqrt(
                (2 * l + 1) / (4.0 * math.pi) * math.factorial(l - m) / math.factorial(l + m)
            )
            if m == 0:
                entries[l, 0] = factor * legendre[l]
            else:
                entries[l, m] = math.sqrt(2.0) * factor * np.cos(m * angles) * legendre[l]
                entries[l, -m] = math.sqrt(2.0) * factor * np.sin(m * angles) * legendre[l]
    return np.stack([entries[l, m] for l in range(DEGREES) for m in range(-l, l + 1)])


def direction_tables():
    values = harmonic_values()
    basis = values.T.astype(np.float32).astype(jnp.bfloat16)
    projector = (values * (4.0 * math.pi / (POLAR * AZIMUTH))).astype(np.float32)
    return basis, projector.astype(jnp.bfloat16)


def fill_rows(get, spread, coeffs, rows_y, cells_z):
    halves = cells_z // LANES
    for c in range(coeffs):
        for h in range(halves):
            block = get(c, h).astype(jnp.float32)
            spread[h, pl.ds(c, rows_y, stride=coeffs), :] = block


def turn_rows(spread, eye, coeffs, rows_y, cells_z, put):
    halves = cells_z // LANES
    keep = -(-coeffs // 16) * 16
    zeros = jnp.zeros((LANES - keep, cells_z), jnp.bfloat16)
    for y in range(0, rows_y, 2):
        parts = []
        for i in (y, y + 1):
            rows = jnp.concatenate(
                [spread[h, i * coeffs : i * coeffs + keep, :] for h in range(halves)], axis=1
            )
            parts += [rows.astype(jnp.bfloat16), zeros]
        both = lax.dot_general(
            eye[...],
            jnp.concatenate(parts, axis=0),
            (((1,), (1,)), ((), ())),
            preferred_element_type=jnp.float32,
        )
        put(y, both[:, :LANES])
        put(y + 1, both[:, LANES:])


def spread_shape(coeffs, cells_y, cells_z):
    return pltpu.VMEM((cells_z // LANES, cells_y * coeffs + 16, LANES), jnp.float32)


def own_table(field, eye):
    coeffs, cells_x, cells_y, cells_z = field.shape
    plane = cells_y * cells_z

    def kernel(field, eye, out, spread):
        fill_rows(
            lambda c, h: field[c, 0, :, h * LANES : (h + 1) * LANES],
            spread,
            coeffs,
            cells_y,
            cells_z,
        )

        def put(y, block):
            out[y * cells_z : (y + 1) * cells_z, :] = block

        turn_rows(spread, eye, coeffs, cells_y, cells_z, put)

    return pl.pallas_call(
        kernel,
        out_shape=pltpu.HBM((cells_x * plane, LANES), jnp.float32),
        grid=(cells_x,),
        in_specs=[
            pl.BlockSpec((coeffs, 1, cells_y, cells_z), lambda x: (0, x, 0, 0)),
            pl.BlockSpec((cells_z, cells_z), lambda x: (0, 0)),
        ],
        out_specs=pl.BlockSpec((plane, LANES), lambda x: (x, 0)),
        scratch_shapes=[spread_shape(coeffs, cells_y, cells_z)],
        compiler_params=pltpu.CompilerParams(vmem_limit_bytes=16 * MIB),
        cost_estimate=pl.CostEstimate(
            flops=2 * 10**10, transcendentals=0, bytes_accessed=2 * 10**7
        ),
        name="own_table",
    )(field, eye)


def full_table(own, xlo, xhi, ylo, yhi, corners, eye, total_rows):
    coeffs, _, cells_y, cells_z = xlo.shape
    count = 2 * HALO + 3
    own_rows = own.shape[0]
    lines = own_rows // cells_z + count * cells_y
    halves = range(cells_z // LANES)

    def kernel(own, xlo, xhi, ylo, yhi, corners, eye, table, zhi, zlo, buf, sems, spread, done):
        sources = [xlo.at[:, 0], xlo.at[:, 1], xhi.at[:, 0], xhi.at[:, 1], ylo, yhi, corners]
        for p, source in enumerate(sources):
            pltpu.make_async_copy(source, buf.at[p], sems.at[p]).start()
        inherit = pltpu.make_async_copy(own, table.at[pl.ds(0, own_rows), :], done)
        inherit.start()

        def one(p, _):
            pltpu.make_async_copy(ylo, buf.at[p], sems.at[p]).wait()
            fill_rows(
                lambda c, h: buf[p, c, :, h * LANES : (h + 1) * LANES],
                spread,
                coeffs,
                cells_y,
                cells_z,
            )

            def put(y, block):
                at = pl.multiple_of(own_rows + (p * cells_y + y) * cells_z, 8)
                table[pl.ds(at, cells_z), :] = block

            turn_rows(spread, eye, coeffs, cells_y, cells_z, put)
            return 0

        lax.fori_loop(0, count, one, 0)
        inherit.wait()
        for out, start in ((zhi, 0), (zlo, cells_z - HALO)):
            for j in range(HALO):
                for line in range(0, lines, 16):
                    parts = [
                        table[pl.ds((line + i) * cells_z + start + j, 8, stride=cells_z), :]
                        for i in (0, 8)
                    ]
                    out[j * lines + line : j * lines + line + 16, :] = jnp.concatenate(
                        parts, axis=0
                    ).astype(jnp.bfloat16)

    del halves
    edge = jax.ShapeDtypeStruct((HALO * lines, LANES), jnp.bfloat16)
    vmem = pl.BlockSpec(memory_space=pltpu.VMEM)
    hbm = pl.BlockSpec(memory_space=pl.ANY)
    return pl.pallas_call(
        kernel,
        out_shape=(pltpu.VMEM((total_rows, LANES), jnp.float32), edge, edge),
        in_specs=[hbm] * 6 + [vmem],
        out_specs=(vmem, vmem, vmem),
        scratch_shapes=[
            pltpu.VMEM((count, coeffs, cells_y, cells_z), jnp.bfloat16),
            pltpu.SemaphoreType.DMA((count,)),
            spread_shape(coeffs, cells_y, cells_z),
            pltpu.SemaphoreType.DMA(()),
        ],
        compiler_params=pltpu.CompilerParams(vmem_limit_bytes=12 * MIB),
        cost_estimate=pl.CostEstimate(
            flops=2 * 10**10, transcendentals=0, bytes_accessed=2 * 10**7
        ),
        name="full_table",
    )(own, xlo, xhi, ylo, yhi, corners, eye)


GROUP = 8


def prepare(samples, weights, slot, origin, cells, total):
    count = slot.shape[0]
    cells_x, cells_y, cells_z = cells
    own_lines = cells_x * cells_y
    lines = own_lines + (2 * HALO + 3) * cells_y
    rows = lines * cells_z
    per_row = LANES // SAMPLES

    def locate(near_x, near_y, near_z):
        own_x = (near_x >= HALO) & (near_x < HALO + cells_x)
        own_y = (near_y >= HALO) & (near_y < HALO + cells_y)
        low_y = near_y < HALO
        side_x = jnp.where(near_x < HALO, near_x, near_x - cells_x)
        side_y = jnp.where(low_y, near_y, near_y - HALO - cells_y)
        line_own = jnp.where(own_x, near_x - HALO, cells_x + side_x) * cells_y + near_y - HALO
        line_y = (
            (cells_x + 2 * HALO) * cells_y
            + jnp.where(low_y, 0, cells_y)
            + (near_x - HALO) * HALO
            + side_y
        )
        line_corner = (
            (cells_x + 2 * HALO + 2) * cells_y
            + jnp.where(low_y, 0, 2 * HALO * HALO)
            + side_x * HALO
            + side_y
        )
        line = jnp.where(own_y, line_own, jnp.where(own_x, line_y, line_corner))
        inside = line * cells_z + near_z - HALO
        below = rows + near_z * lines + line
        above = rows + (near_z - cells_z) * lines + line
        return jnp.where(near_z < HALO, below, jnp.where(near_z < HALO + cells_z, inside, above))

    def kernel(origin, slot, samples, weights, index, ordered):
        def scatter(j, _):
            at = pl.multiple_of(j * LANES, LANES)
            near = []
            for d in range(3):
                shift = samples[d, :, pl.ds(at, LANES)] - origin[d] + HALO
                shift = jnp.where(shift < 0, shift + total[d], shift)
                near.append(jnp.where(shift >= total[d], shift - total[d], shift))
            block = jnp.concatenate(
                [
                    locate(*near).astype(jnp.float32),
                    weights[:, pl.ds(at, LANES)],
                    jnp.zeros((LANES - 2 * SAMPLES, LANES), jnp.float32),
                ],
                axis=0,
            ).T
            mine = slot.at[pl.ds(at, LANES)]
            for r in range(LANES):
                ordered[pl.ds(mine[r], 1), :] = block[r : r + 1, :]
            return 0

        lax.fori_loop(0, count // LANES, scatter, 0)
        sub = lax.broadcasted_iota(jnp.int32, (SAMPLES, LANES), 0)
        group = lax.broadcasted_iota(jnp.int32, (SAMPLES, LANES), 1) // per_row

        def turn(j, _):
            block = ordered[pl.ds(pl.multiple_of(j * LANES, LANES), LANES), :].T
            tile = block[:SAMPLES, :].astype(jnp.int32)
            for b in (1, 2, 4):
                up = pltpu.roll(pltpu.roll(tile, b, 0), LANES - b * per_row, 1)
                down = pltpu.roll(pltpu.roll(tile, SAMPLES - b, 0), b * per_row, 1)
                row_bit = (sub & b) != 0
                lane_bit = (group & b) != 0
                tile = jnp.where(row_bit == lane_bit, tile, jnp.where(row_bit, up, down))
            index[pl.ds(pl.multiple_of(j * SAMPLES, SAMPLES), SAMPLES), :] = tile
            return 0

        lax.fori_loop(0, count // LANES, turn, 0)

    vmem = pl.BlockSpec(memory_space=pltpu.VMEM)
    smem = pl.BlockSpec(memory_space=pltpu.SMEM)
    return pl.pallas_call(
        kernel,
        out_shape=(
            jax.ShapeDtypeStruct((count * SAMPLES // LANES, LANES), jnp.int32),
            jax.ShapeDtypeStruct((count, LANES), jnp.float32),
        ),
        in_specs=[smem, smem, vmem, vmem],
        out_specs=(vmem, vmem),
        compiler_params=pltpu.CompilerParams(vmem_limit_bytes=12 * MIB),
        cost_estimate=pl.CostEstimate(
            flops=2 * 10**10, transcendentals=0, bytes_accessed=3 * 10**6
        ),
        name="prepare",
    )(origin, slot, samples, weights)


def spread_weights(ordered):
    count = ordered.shape[0]
    step = 4

    def kernel(ordered, wide):
        def body(i, _):
            for q in range(step):
                g = i * step + q
                tile = ordered[pl.ds(pl.multiple_of(g * GROUP, GROUP), GROUP), :]
                for s in range(SAMPLES):
                    at = pl.multiple_of((g * SAMPLES + s) * GROUP, GROUP)
                    wide[pl.ds(at, GROUP), :] = jnp.broadcast_to(
                        tile[:, SAMPLES + s : SAMPLES + s + 1], (GROUP, LANES)
                    )
            return 0

        lax.fori_loop(0, count // (GROUP * step), body, 0)

    vmem = pl.BlockSpec(memory_space=pltpu.VMEM)
    return pl.pallas_call(
        kernel,
        out_shape=pltpu.VMEM((count * SAMPLES, LANES), jnp.float32),
        in_specs=[vmem],
        out_specs=vmem,
        compiler_params=pltpu.CompilerParams(vmem_limit_bytes=4 * MIB),
        cost_estimate=pl.CostEstimate(
            flops=10**10, transcendentals=0, bytes_accessed=3 * 10**6
        ),
        name="spread_weights",
    )(ordered)


RING = 8
CHUNK = 256


def gather_rows(index, wide, table, zlo, zhi, first_edge, coeffs):
    edges = zlo.shape[0]
    chunks = index.shape[0] // CHUNK
    per_chunk = CHUNK // SAMPLES
    packed = per_chunk * 3 // 4
    groups = per_chunk // GROUP

    def kernel(index, zlo, zhi, table_in, wide_in, table, wide, out, local, sems):
        table[pl.ds(first_edge, edges), :] = zlo[...].astype(jnp.float32)
        table[pl.ds(first_edge + edges, edges), :] = zhi[...].astype(jnp.float32)
        sublane = lax.broadcasted_iota(jnp.int32, (GROUP, LANES), 0)
        masks = [sublane == k for k in range(GROUP)]
        lane = lax.broadcasted_iota(jnp.int32, (GROUP, LANES), 1)
        used = lane < coeffs
        low = lane < 64
        quarters = [lane < 32, lane < 64, lane < 96]

        def fetch(n, slot):
            return pltpu.make_async_copy(
                index.at[pl.ds(pl.multiple_of(n * CHUNK, CHUNK), CHUNK)],
                local.at[slot],
                sems.at[slot],
            )

        for b in range(RING - 1):
            fetch(b, b).start()

        def body(i, _):
            for b in range(RING):
                n = i * RING + b
                fetch(n, b).wait()
                ahead = n + RING - 1

                @pl.when(ahead < chunks)
                def _():
                    fetch(ahead, (b + RING - 1) % RING).start()

                sums = []
                for q in range(groups):
                    total = None
                    for s in range(SAMPLES):
                        merged = None
                        for k in range(GROUP):
                            place = (q // 2) * LANES + s * 16 + (q % 2) * GROUP + k
                            row = table[pl.ds(local[b, place], GROUP, stride=0), :]
                            merged = row if merged is None else jnp.where(masks[k], row, merged)
                        at = pl.multiple_of(n * CHUNK + (q * SAMPLES + s) * GROUP, GROUP)
                        term = merged * wide[pl.ds(at, GROUP), :]
                        total = term if total is None else total + term
                    sums.append(jnp.where(used, total, 0.0))
                first = jnp.where(low, sums[0], pltpu.roll(sums[2], 64, 1))
                second = jnp.where(low, sums[1], pltpu.roll(sums[3], 64, 1))
                third = jnp.where(
                    quarters[0],
                    pltpu.roll(sums[0], 64, 1),
                    jnp.where(
                        quarters[1],
                        pltpu.roll(sums[1], 96, 1),
                        jnp.where(quarters[2], sums[2], pltpu.roll(sums[3], 32, 1)),
                    ),
                )
                out[n, :16, :] = jnp.concatenate([first, second], axis=0).astype(jnp.bfloat16)
                out[n, 16:, :] = third.astype(jnp.bfloat16)
            return 0

        lax.fori_loop(0, chunks // RING, body, 0)

    vmem = pl.BlockSpec(memory_space=pltpu.VMEM)
    return pl.pallas_call(
        kernel,
        out_shape=(
            pltpu.VMEM(table.shape, jnp.float32),
            pltpu.VMEM(wide.shape, jnp.float32),
            jax.ShapeDtypeStruct((chunks, packed, LANES), jnp.bfloat16),
        ),
        in_specs=[vmem] * 5,
        out_specs=(vmem, vmem, vmem),
        scratch_shapes=[
            pltpu.SMEM((RING, CHUNK), jnp.int32),
            pltpu.SemaphoreType.DMA((RING,)),
        ],
        input_output_aliases={3: 0, 4: 1},
        compiler_params=pltpu.CompilerParams(vmem_limit_bytes=8 * MIB),
        cost_estimate=pl.CostEstimate(
            flops=4 * 10**10, transcendentals=0, bytes_accessed=2 * 10**7
        ),
        name="gather_rows",
    )(index, zlo, zhi, table, wide)[2]


def relight(transfer, routed, basis, projector):
    coeffs, count = transfer.shape
    sources, packed, _ = routed.shape
    per_pair = count // sources
    block = 512
    step = block // per_pair

    def kernel(transfer, routed, basis, wide, projector, out):
        low = lax.broadcasted_iota(jnp.int32, (GROUP, LANES), 1) < 64
        parts = []
        for i in range(step):
            head = routed[i, :16, :].astype(jnp.float32)
            first, second = head[:GROUP], head[GROUP:]
            third = routed[i, 16:, :].astype(jnp.float32)
            parts += [
                jnp.where(low, first, pltpu.roll(third, 64, 1)),
                jnp.where(low, second, pltpu.roll(third, 32, 1)),
                jnp.where(low, pltpu.roll(first, 64, 1), third),
                jnp.where(low, pltpu.roll(second, 64, 1), pltpu.roll(third, 96, 1)),
            ]
        rows = jnp.concatenate(parts, axis=0).astype(jnp.bfloat16)
        lit = jnp.dot(basis[...], transfer[...], preferred_element_type=jnp.float32)
        shade = lax.dot_general(
            wide[...], rows, (((1,), (1,)), ((), ())), preferred_element_type=jnp.float32
        )
        product = (lit * shade).astype(jnp.bfloat16)
        out[...] = jnp.dot(projector[...], product, preferred_element_type=jnp.float32).astype(
            jnp.bfloat16
        )

    directions = basis.shape[0]
    wide = np.zeros((directions, LANES), jnp.bfloat16)
    wide[:, :coeffs] = basis
    return pl.pallas_call(
        kernel,
        out_shape=jax.ShapeDtypeStruct((coeffs, count), jnp.bfloat16),
        grid=(count // block,),
        in_specs=[
            pl.BlockSpec((coeffs, block), lambda i: (0, i)),
            pl.BlockSpec((step, packed, LANES), lambda i: (i, 0, 0)),
            pl.BlockSpec((directions, coeffs), lambda i: (0, 0)),
            pl.BlockSpec((directions, LANES), lambda i: (0, 0)),
            pl.BlockSpec((coeffs, directions), lambda i: (0, 0)),
        ],
        out_specs=pl.BlockSpec((coeffs, block), lambda i: (0, i)),
        compiler_params=pltpu.CompilerParams(vmem_limit_bytes=40 * MIB),
        name="relight",
    )(transfer, routed, jnp.asarray(basis), jnp.asarray(wide), jnp.asarray(projector))


def moves(sizes, steps):
    pairs = []
    for x in range(sizes[0]):
        for y in range(sizes[1]):
            to_x, to_y = (x + steps[0]) % sizes[0], (y + steps[1]) % sizes[1]
            pairs.append((x * sizes[1] + y, to_x * sizes[1] + to_y))
    return pairs


def halo_step(field, samples, weights, destination, transfer):
    basis, projector = direction_tables()
    coeffs, cells_x, cells_y, cells_z = field.shape
    count = transfer.shape[1]
    along = tuple(lax.axis_size(axis) for axis in ("gx", "gy", "gz"))
    ups = [moves((n, 1), (1, 0)) for n in along]
    downs = [moves((n, 1), (-1, 0)) for n in along]

    last, first, cut = lax.optimization_barrier(
        (field[:, cells_x - HALO :], field[:, :HALO], field)
    )
    xlo = lax.ppermute(last, "gx", ups[0])
    xhi = lax.ppermute(first, "gx", downs[0])
    plane = (coeffs, cells_x * HALO, cells_z)
    top = cut[:, :, cells_y - HALO :]
    bottom = cut[:, :, :HALO]
    ylo = lax.ppermute(top.reshape(plane), "gy", ups[1])
    yhi = lax.ppermute(bottom.reshape(plane), "gy", downs[1])
    corners = []
    for edge, step_y in ((top, 1), (bottom, -1)):
        for piece, step_x in ((edge[:, cells_x - HALO :], 1), (edge[:, :HALO], -1)):
            piece = piece.reshape(coeffs, HALO * HALO, cells_z)
            corners.append(lax.ppermute(piece, ("gx", "gy"), moves(along[:2], (step_x, step_y))))
    corners = jnp.concatenate(corners, axis=1)

    lines = cells_x * cells_y + (2 * HALO + 3) * cells_y
    rows = lines * cells_z
    cells = (cells_x, cells_y, cells_z)
    total = tuple(c * n for c, n in zip(cells, along))
    origin = jnp.stack(
        [lax.axis_index(axis) * c for axis, c in zip(("gx", "gy", "gz"), cells)]
    ).astype(jnp.int32)
    devices = math.prod(along)
    per_pair = count // devices
    slot = destination[0] * per_pair + destination[1]

    eye = jnp.asarray(np.eye(cells_z, dtype=np.float32).astype(jnp.bfloat16))
    own = own_table(field, eye)
    index, ordered = prepare(samples, weights, slot, origin, cells, total)
    own, index, ordered, corners = lax.optimization_barrier((own, index, ordered, corners))
    table, edge_lo, edge_hi = full_table(
        own, xlo, xhi, ylo, yhi, corners, eye, rows + 2 * HALO * lines
    )
    zhi = lax.ppermute(edge_lo, "gz", downs[2])
    zlo = lax.ppermute(edge_hi, "gz", ups[2])
    wide = spread_weights(ordered)
    outgoing = gather_rows(index.reshape(-1), wide, table, zlo, zhi, rows, coeffs)
    routed = lax.all_to_all(
        outgoing, ("gx", "gy", "gz"), split_axis=0, concat_axis=0, tiled=True
    )
    return relight(transfer, routed, basis, projector)


def solution(mesh):
    placed = (
        P(None, "gx", "gy", "gz"),
        P(None, None, ("gx", "gy", "gz")),
        P(None, ("gx", "gy", "gz")),
        P(None, ("gx", "gy", "gz")),
        P(None, ("gx", "gy", "gz")),
    )
    return jax.shard_map(
        halo_step,
        mesh=mesh,
        in_specs=placed,
        out_specs=P(None, ("gx", "gy", "gz")),
        check_vma=False,
    )
```

```python
import math

import jax
import jax.numpy as jnp
import numpy as np
from jax import lax
from jax.experimental import pallas as pl
from jax.experimental.pallas import tpu as pltpu
from jax.sharding import PartitionSpec as P


HALO = 2
SAMPLES = 8
DEGREES = 9
POLAR = 32
AZIMUTH = 32
LANES = 128
MIB = 1024 * 1024


def harmonic_values():
    polar = (np.arange(POLAR, dtype=np.float64) + 0.5) * (2.0 / POLAR) - 1.0
    beside = (np.arange(AZIMUTH, dtype=np.float64) + 0.5) * (2.0 * math.pi / AZIMUTH)
    cosines = np.repeat(polar, AZIMUTH)
    angles = np.tile(beside, POLAR)
    sines = np.sqrt(np.maximum(1.0 - cosines * cosines, 0.0))
    entries = {}
    for m in range(DEGREES):
        diagonal = (-1.0) ** m * float(math.prod(range(1, 2 * m, 2))) * sines**m
        legendre = {m: diagonal}
        if m + 1 < DEGREES:
            legendre[m + 1] = cosines * (2 * m + 1) * diagonal
        for l in range(m + 2, DEGREES):
            legendre[l] = (
                (2 * l - 1) * cosines * legendre[l - 1] - (l + m - 1) * legendre[l - 2]
            ) / (l - m)
        for l in range(m, DEGREES):
            factor = math.sqrt(
                (2 * l + 1) / (4.0 * math.pi) * math.factorial(l - m) / math.factorial(l + m)
            )
            if m == 0:
                entries[l, 0] = factor * legendre[l]
            else:
                entries[l, m] = math.sqrt(2.0) * factor * np.cos(m * angles) * legendre[l]
                entries[l, -m] = math.sqrt(2.0) * factor * np.sin(m * angles) * legendre[l]
    return np.stack([entries[l, m] for l in range(DEGREES) for m in range(-l, l + 1)])


def direction_tables():
    values = harmonic_values()
    basis = values.T.astype(np.float32).astype(jnp.bfloat16)
    projector = (values * (4.0 * math.pi / (POLAR * AZIMUTH))).astype(np.float32)
    return basis, projector.astype(jnp.bfloat16)


def fill_rows(get, spread, coeffs, rows_y, cells_z):
    halves = cells_z // LANES
    for c in range(coeffs):
        for h in range(halves):
            block = get(c, h).astype(jnp.float32)
            spread[h, pl.ds(c, rows_y, stride=coeffs), :] = block


def turn_rows(spread, eye, coeffs, rows_y, cells_z, put):
    halves = cells_z // LANES
    keep = -(-coeffs // 16) * 16
    zeros = jnp.zeros((LANES - keep, cells_z), jnp.bfloat16)
    for y in range(0, rows_y, 2):
        parts = []
        for i in (y, y + 1):
            rows = jnp.concatenate(
                [spread[h, i * coeffs : i * coeffs + keep, :] for h in range(halves)], axis=1
            )
            parts += [rows.astype(jnp.bfloat16), zeros]
        both = lax.dot_general(
            eye[...],
            jnp.concatenate(parts, axis=0),
            (((1,), (1,)), ((), ())),
            preferred_element_type=jnp.float32,
        )
        put(y, both[:, :LANES])
        put(y + 1, both[:, LANES:])


def spread_shape(coeffs, cells_y, cells_z):
    return pltpu.VMEM((cells_z // LANES, cells_y * coeffs + 16, LANES), jnp.float32)


def own_table(field, eye):
    coeffs, cells_x, cells_y, cells_z = field.shape
    plane = cells_y * cells_z

    def kernel(field, eye, out, spread):
        fill_rows(
            lambda c, h: field[c, 0, :, h * LANES : (h + 1) * LANES],
            spread,
            coeffs,
            cells_y,
            cells_z,
        )

        def put(y, block):
            out[y * cells_z : (y + 1) * cells_z, :] = block

        turn_rows(spread, eye, coeffs, cells_y, cells_z, put)

    return pl.pallas_call(
        kernel,
        out_shape=pltpu.HBM((cells_x * plane, LANES), jnp.float32),
        grid=(cells_x,),
        in_specs=[
            pl.BlockSpec((coeffs, 1, cells_y, cells_z), lambda x: (0, x, 0, 0)),
            pl.BlockSpec((cells_z, cells_z), lambda x: (0, 0)),
        ],
        out_specs=pl.BlockSpec((plane, LANES), lambda x: (x, 0)),
        scratch_shapes=[spread_shape(coeffs, cells_y, cells_z)],
        compiler_params=pltpu.CompilerParams(vmem_limit_bytes=16 * MIB),
        cost_estimate=pl.CostEstimate(
            flops=2 * 10**10, transcendentals=0, bytes_accessed=2 * 10**7
        ),
        name="own_table",
    )(field, eye)


def full_table(own, xlo, xhi, ylo, yhi, corners, eye, total_rows):
    coeffs, _, cells_y, cells_z = xlo.shape
    count = 2 * HALO + 3
    own_rows = own.shape[0]
    lines = own_rows // cells_z + count * cells_y
    halves = range(cells_z // LANES)

    def kernel(own, xlo, xhi, ylo, yhi, corners, eye, table, zhi, zlo, buf, sems, spread, done):
        sources = [xlo.at[:, 0], xlo.at[:, 1], xhi.at[:, 0], xhi.at[:, 1], ylo, yhi, corners]
        for p, source in enumerate(sources):
            pltpu.make_async_copy(source, buf.at[p], sems.at[p]).start()
        inherit = pltpu.make_async_copy(own, table.at[pl.ds(0, own_rows), :], done)
        inherit.start()

        def one(p, _):
            pltpu.make_async_copy(ylo, buf.at[p], sems.at[p]).wait()
            fill_rows(
                lambda c, h: buf[p, c, :, h * LANES : (h + 1) * LANES],
                spread,
                coeffs,
                cells_y,
                cells_z,
            )

            def put(y, block):
                at = pl.multiple_of(own_rows + (p * cells_y + y) * cells_z, 8)
                table[pl.ds(at, cells_z), :] = block

            turn_rows(spread, eye, coeffs, cells_y, cells_z, put)
            return 0

        lax.fori_loop(0, count, one, 0)
        inherit.wait()
        for out, start in ((zhi, 0), (zlo, cells_z - HALO)):
            for j in range(HALO):
                for line in range(0, lines, 16):
                    parts = [
                        table[pl.ds((line + i) * cells_z + start + j, 8, stride=cells_z), :]
                        for i in (0, 8)
                    ]
                    out[j * lines + line : j * lines + line + 16, :] = jnp.concatenate(
                        parts, axis=0
                    ).astype(jnp.bfloat16)

    del halves
    edge = jax.ShapeDtypeStruct((HALO * lines, LANES), jnp.bfloat16)
    vmem = pl.BlockSpec(memory_space=pltpu.VMEM)
    hbm = pl.BlockSpec(memory_space=pl.ANY)
    return pl.pallas_call(
        kernel,
        out_shape=(pltpu.VMEM((total_rows, LANES), jnp.float32), edge, edge),
        in_specs=[hbm] * 6 + [vmem],
        out_specs=(vmem, vmem, vmem),
        scratch_shapes=[
            pltpu.VMEM((count, coeffs, cells_y, cells_z), jnp.bfloat16),
            pltpu.SemaphoreType.DMA((count,)),
            spread_shape(coeffs, cells_y, cells_z),
            pltpu.SemaphoreType.DMA(()),
        ],
        compiler_params=pltpu.CompilerParams(vmem_limit_bytes=12 * MIB),
        cost_estimate=pl.CostEstimate(
            flops=2 * 10**10, transcendentals=0, bytes_accessed=2 * 10**7
        ),
        name="full_table",
    )(own, xlo, xhi, ylo, yhi, corners, eye)


GROUP = 8
PARTS = 3


def prepare(samples, weights, slot, origin, cells, total):
    count = slot.shape[0]
    cells_x, cells_y, cells_z = cells
    own_lines = cells_x * cells_y
    lines = own_lines + (2 * HALO + 3) * cells_y
    rows = lines * cells_z
    block = 256
    burst = 32
    kinds = (2 + PARTS) * SAMPLES

    def locate(near_x, near_y, near_z):
        own_x = (near_x >= HALO) & (near_x < HALO + cells_x)
        own_y = (near_y >= HALO) & (near_y < HALO + cells_y)
        low_y = near_y < HALO
        side_x = jnp.where(near_x < HALO, near_x, near_x - cells_x)
        side_y = jnp.where(low_y, near_y, near_y - HALO - cells_y)
        line_own = jnp.where(own_x, near_x - HALO, cells_x + side_x) * cells_y + near_y - HALO
        line_y = (
            (cells_x + 2 * HALO) * cells_y
            + jnp.where(low_y, 0, cells_y)
            + (near_x - HALO) * HALO
            + side_y
        )
        line_corner = (
            (cells_x + 2 * HALO + 2) * cells_y
            + jnp.where(low_y, 0, 2 * HALO * HALO)
            + side_x * HALO
            + side_y
        )
        line = jnp.where(own_y, line_own, jnp.where(own_x, line_y, line_corner))
        inside = line * cells_z + near_z - HALO
        below = rows + near_z * lines + line
        above = rows + (near_z - cells_z) * lines + line
        return jnp.where(near_z < HALO, below, jnp.where(near_z < HALO + cells_z, inside, above))

    def kernel(origin, slot, samples, weights, eye, join, index, ordered, natural):
        def turn(j, _):
            at = pl.multiple_of(j * block, block)
            near = []
            for d in range(3):
                shift = samples[d, :, pl.ds(at, block)] - origin[d] + HALO
                shift = jnp.where(shift < 0, shift + total[d], shift)
                near.append(jnp.where(shift >= total[d], shift - total[d], shift))
            row = locate(*near)
            pieces = [(row >> 8).astype(jnp.float32), (row & 255).astype(jnp.float32)]
            rest = weights[:, pl.ds(at, block)]
            for _ in range(PARTS):
                piece = rest.astype(jnp.bfloat16).astype(jnp.float32)
                pieces.append(piece)
                rest = rest - piece
            pieces.append(jnp.zeros((LANES - kinds, block), jnp.float32))
            natural[pl.ds(at, block), :] = lax.dot_general(
                eye[...],
                jnp.concatenate(pieces, axis=0).astype(jnp.bfloat16),
                (((1,), (1,)), ((), ())),
                preferred_element_type=jnp.float32,
            )
            return 0

        lax.fori_loop(0, count // block, turn, 0)

        def scatter(j, _):
            at = pl.multiple_of(j * burst, burst)
            mine = slot.at[pl.ds(at, burst)]
            for g in range(0, burst, GROUP):
                tile = natural[pl.ds(at + g, GROUP), :]
                for k in range(GROUP):
                    ordered[pl.ds(mine[g + k], 1), :] = tile[k : k + 1, :]
            return 0

        lax.fori_loop(0, count // burst, scatter, 0)

        def collect(j, _):
            at = pl.multiple_of(j * 4 * LANES, 4 * LANES)
            wide = lax.dot_general(
                join[...],
                ordered[pl.ds(at, 4 * LANES), :].astype(jnp.bfloat16),
                (((1,), (1,)), ((), ())),
                preferred_element_type=jnp.float32,
            ).astype(jnp.int32)
            for i in range(4):
                to = pl.multiple_of((j * 4 + i) * SAMPLES, SAMPLES)
                index[pl.ds(to, SAMPLES), :] = wide[:SAMPLES, i * LANES : (i + 1) * LANES]
            return 0

        lax.fori_loop(0, count // (4 * LANES), collect, 0)

    join = np.zeros((16, LANES), np.float32)
    for s in range(SAMPLES):
        join[s, s] = 256.0
        join[s, SAMPLES + s] = 1.0
    vmem = pl.BlockSpec(memory_space=pltpu.VMEM)
    smem = pl.BlockSpec(memory_space=pltpu.SMEM)
    return pl.pallas_call(
        kernel,
        out_shape=(
            jax.ShapeDtypeStruct((count * SAMPLES // LANES, LANES), jnp.int32),
            jax.ShapeDtypeStruct((count, LANES), jnp.float32),
        ),
        in_specs=[smem, smem, vmem, vmem, vmem, vmem],
        out_specs=(vmem, vmem),
        scratch_shapes=[pltpu.VMEM((count, LANES), jnp.float32)],
        compiler_params=pltpu.CompilerParams(vmem_limit_bytes=12 * MIB),
        cost_estimate=pl.CostEstimate(
            flops=2 * 10**10, transcendentals=0, bytes_accessed=3 * 10**6
        ),
        name="prepare",
    )(
        origin,
        slot,
        samples,
        weights,
        jnp.asarray(np.eye(block, dtype=np.float32).astype(jnp.bfloat16)),
        jnp.asarray(join.astype(jnp.bfloat16)),
    )


def spread_weights(ordered):
    count = ordered.shape[0]
    block = 128

    def kernel(ordered, ones, wide):
        def body(i, _):
            at = pl.multiple_of(i * block, block)
            rows = ordered[pl.ds(at, block), :].astype(jnp.bfloat16)
            for h in range(0, SAMPLES, 2):
                both = jnp.dot(
                    rows,
                    ones[:, h * LANES : (h + 2) * LANES],
                    preferred_element_type=jnp.float32,
                )
                for s in range(2):
                    for g in range(block // GROUP):
                        to = (i * (block // GROUP) + g) * SAMPLES + h + s
                        wide[pl.ds(pl.multiple_of(to * GROUP, GROUP), GROUP), :] = both[
                            g * GROUP : (g + 1) * GROUP, s * LANES : (s + 1) * LANES
                        ]
            return 0

        lax.fori_loop(0, count // block, body, 0)

    ones = np.zeros((LANES, SAMPLES * LANES), np.float32)
    for s in range(SAMPLES):
        for p in range(PARTS):
            ones[(2 + p) * SAMPLES + s, s * LANES : (s + 1) * LANES] = 1.0
    vmem = pl.BlockSpec(memory_space=pltpu.VMEM)
    return pl.pallas_call(
        kernel,
        out_shape=pltpu.VMEM((count * SAMPLES, LANES), jnp.float32),
        in_specs=[vmem, vmem],
        out_specs=vmem,
        compiler_params=pltpu.CompilerParams(vmem_limit_bytes=4 * MIB),
        cost_estimate=pl.CostEstimate(
            flops=10**10, transcendentals=0, bytes_accessed=3 * 10**6
        ),
        name="spread_weights",
    )(ordered, jnp.asarray(ones.astype(jnp.bfloat16)))


RING = 2
CHUNK = 1024


def gather_rows(index, wide, table, zlo, zhi, first_edge, count, coeffs):
    edges = zlo.shape[0]
    chunks = index.shape[0] // CHUNK
    per_chunk = CHUNK // SAMPLES
    groups = per_chunk // GROUP
    pairs = count // 32
    half = LANES // 2

    def kernel(index, zlo, zhi, pick, table_in, wide_in, table, wide, out, local, sems, rows):
        table[pl.ds(first_edge, edges), :] = zlo[...].astype(jnp.float32)
        table[pl.ds(first_edge + edges, edges), :] = zhi[...].astype(jnp.float32)
        sublane = lax.broadcasted_iota(jnp.int32, (GROUP, LANES), 0)
        masks = [sublane == k for k in range(GROUP)]
        used = lax.broadcasted_iota(jnp.int32, (GROUP, LANES), 1) < coeffs

        def fetch(n, slot):
            return pltpu.make_async_copy(
                index.at[pl.ds(pl.multiple_of(n * CHUNK, CHUNK), CHUNK)],
                local.at[slot],
                sems.at[slot],
            )

        for b in range(RING - 1):
            fetch(b, b).start()

        def body(i, _):
            for b in range(RING):
                n = i * RING + b
                fetch(n, b).wait()
                ahead = n + RING - 1

                @pl.when(ahead < chunks)
                def _():
                    fetch(ahead, (b + RING - 1) % RING).start()

                for q in range(groups):
                    total = None
                    for s in range(SAMPLES):
                        merged = None
                        for k in range(GROUP):
                            place = s * per_chunk + q * GROUP + k
                            row = table[pl.ds(local[b, place], GROUP, stride=0), :]
                            merged = row if merged is None else jnp.where(masks[k], row, merged)
                        at = pl.multiple_of(n * CHUNK + (q * SAMPLES + s) * GROUP, GROUP)
                        term = merged * wide[pl.ds(at, GROUP), :]
                        total = term if total is None else total + term
                    to = pl.multiple_of((n * (groups // 4) + q // 4) * GROUP, GROUP)
                    rows[q % 4, pl.ds(to, GROUP), :] = jnp.where(used, total, 0.0)
            return 0

        lax.fori_loop(0, chunks // RING, body, 0)

        def pack(i, _):
            at = pl.multiple_of(i * 128, 128)
            part = [rows[q, pl.ds(at, 128), :].astype(jnp.bfloat16) for q in range(4)]
            outer = [jnp.concatenate([part[0], part[2]], axis=1)]
            outer.append(jnp.concatenate([part[1], part[3]], axis=1))
            first = jnp.dot(outer[0], pick[0], preferred_element_type=jnp.float32)
            second = jnp.dot(outer[1], pick[0], preferred_element_type=jnp.float32)
            third = jnp.dot(outer[0], pick[1], preferred_element_type=jnp.float32)
            third += jnp.dot(outer[1], pick[2], preferred_element_type=jnp.float32)
            for d in range(128 // GROUP):
                here = slice(d * GROUP, (d + 1) * GROUP)
                out[i * (128 // GROUP) + d, :16, :] = jnp.concatenate(
                    [first[here], second[here]], axis=0
                ).astype(jnp.bfloat16)
                out[i * (128 // GROUP) + d, 16:, :] = third[here].astype(jnp.bfloat16)
            return 0

        lax.fori_loop(0, pairs * GROUP // 128, pack, 0)

    pick = np.zeros((3, 2 * LANES, LANES), np.float32)
    for c in range(half):
        pick[0, c, c] = 1.0
        pick[0, LANES + c, half + c] = 1.0
    for c in range(32):
        pick[1, half + c, c] = 1.0
        pick[1, LANES + half + c, 64 + c] = 1.0
        pick[2, half + c, 32 + c] = 1.0
        pick[2, LANES + half + c, 96 + c] = 1.0
    vmem = pl.BlockSpec(memory_space=pltpu.VMEM)
    return pl.pallas_call(
        kernel,
        out_shape=(
            pltpu.VMEM(table.shape, jnp.float32),
            pltpu.VMEM(wide.shape, jnp.float32),
            jax.ShapeDtypeStruct((pairs, 24, LANES), jnp.bfloat16),
        ),
        in_specs=[vmem] * 6,
        out_specs=(vmem, vmem, vmem),
        scratch_shapes=[
            pltpu.SMEM((RING, CHUNK), jnp.int32),
            pltpu.SemaphoreType.DMA((RING,)),
            pltpu.VMEM((4, pairs * GROUP, LANES), jnp.float32),
        ],
        input_output_aliases={4: 0, 5: 1},
        compiler_params=pltpu.CompilerParams(vmem_limit_bytes=8 * MIB),
        cost_estimate=pl.CostEstimate(
            flops=4 * 10**10, transcendentals=0, bytes_accessed=2 * 10**7
        ),
        name="gather_rows",
    )(index, zlo, zhi, jnp.asarray(pick.astype(jnp.bfloat16)), table, wide)[2]


def relight(transfer, routed, basis, projector):
    coeffs, count = transfer.shape
    sources, packed, _ = routed.shape
    per_pair = count // sources
    block = 512
    step = block // per_pair

    def kernel(transfer, routed, basis, wide, projector, out):
        low = lax.broadcasted_iota(jnp.int32, (GROUP, LANES), 1) < 64
        parts = []
        for i in range(step):
            head = routed[i, :16, :].astype(jnp.float32)
            first, second = head[:GROUP], head[GROUP:]
            third = routed[i, 16:, :].astype(jnp.float32)
            parts += [
                jnp.where(low, first, pltpu.roll(third, 64, 1)),
                jnp.where(low, second, pltpu.roll(third, 32, 1)),
                jnp.where(low, pltpu.roll(first, 64, 1), third),
                jnp.where(low, pltpu.roll(second, 64, 1), pltpu.roll(third, 96, 1)),
            ]
        rows = jnp.concatenate(parts, axis=0).astype(jnp.bfloat16)
        lit = jnp.dot(basis[...], transfer[...], preferred_element_type=jnp.float32)
        shade = lax.dot_general(
            wide[...], rows, (((1,), (1,)), ((), ())), preferred_element_type=jnp.float32
        )
        product = (lit * shade).astype(jnp.bfloat16)
        out[...] = jnp.dot(projector[...], product, preferred_element_type=jnp.float32).astype(
            jnp.bfloat16
        )

    directions = basis.shape[0]
    wide = np.zeros((directions, LANES), jnp.bfloat16)
    wide[:, :coeffs] = basis
    return pl.pallas_call(
        kernel,
        out_shape=jax.ShapeDtypeStruct((coeffs, count), jnp.bfloat16),
        grid=(count // block,),
        in_specs=[
            pl.BlockSpec((coeffs, block), lambda i: (0, i)),
            pl.BlockSpec((step, packed, LANES), lambda i: (i, 0, 0)),
            pl.BlockSpec((directions, coeffs), lambda i: (0, 0)),
            pl.BlockSpec((directions, LANES), lambda i: (0, 0)),
            pl.BlockSpec((coeffs, directions), lambda i: (0, 0)),
        ],
        out_specs=pl.BlockSpec((coeffs, block), lambda i: (0, i)),
        compiler_params=pltpu.CompilerParams(vmem_limit_bytes=40 * MIB),
        name="relight",
    )(transfer, routed, jnp.asarray(basis), jnp.asarray(wide), jnp.asarray(projector))


def moves(sizes, steps):
    pairs = []
    for x in range(sizes[0]):
        for y in range(sizes[1]):
            to_x, to_y = (x + steps[0]) % sizes[0], (y + steps[1]) % sizes[1]
            pairs.append((x * sizes[1] + y, to_x * sizes[1] + to_y))
    return pairs


def halo_step(field, samples, weights, destination, transfer):
    basis, projector = direction_tables()
    coeffs, cells_x, cells_y, cells_z = field.shape
    count = transfer.shape[1]
    along = tuple(lax.axis_size(axis) for axis in ("gx", "gy", "gz"))
    ups = [moves((n, 1), (1, 0)) for n in along]
    downs = [moves((n, 1), (-1, 0)) for n in along]

    last, first, cut = lax.optimization_barrier(
        (field[:, cells_x - HALO :], field[:, :HALO], field)
    )
    xlo = lax.ppermute(last, "gx", ups[0])
    xhi = lax.ppermute(first, "gx", downs[0])
    plane = (coeffs, cells_x * HALO, cells_z)
    top = cut[:, :, cells_y - HALO :]
    bottom = cut[:, :, :HALO]
    ylo = lax.ppermute(top.reshape(plane), "gy", ups[1])
    yhi = lax.ppermute(bottom.reshape(plane), "gy", downs[1])
    corners = []
    for edge, step_y in ((top, 1), (bottom, -1)):
        for piece, step_x in ((edge[:, cells_x - HALO :], 1), (edge[:, :HALO], -1)):
            piece = piece.reshape(coeffs, HALO * HALO, cells_z)
            corners.append(lax.ppermute(piece, ("gx", "gy"), moves(along[:2], (step_x, step_y))))
    corners = jnp.concatenate(corners, axis=1)

    lines = cells_x * cells_y + (2 * HALO + 3) * cells_y
    rows = lines * cells_z
    cells = (cells_x, cells_y, cells_z)
    total = tuple(c * n for c, n in zip(cells, along))
    origin = jnp.stack(
        [lax.axis_index(axis) * c for axis, c in zip(("gx", "gy", "gz"), cells)]
    ).astype(jnp.int32)
    devices = math.prod(along)
    per_pair = count // devices
    slot = destination[0] * per_pair + destination[1]

    eye = jnp.asarray(np.eye(cells_z, dtype=np.float32).astype(jnp.bfloat16))
    own = own_table(field, eye)
    index, ordered = prepare(samples, weights, slot, origin, cells, total)
    own, index, ordered, corners = lax.optimization_barrier((own, index, ordered, corners))
    table, edge_lo, edge_hi = full_table(
        own, xlo, xhi, ylo, yhi, corners, eye, rows + 2 * HALO * lines
    )
    zhi = lax.ppermute(edge_lo, "gz", downs[2])
    zlo = lax.ppermute(edge_hi, "gz", ups[2])
    wide = spread_weights(ordered)
    outgoing = gather_rows(index.reshape(-1), wide, table, zlo, zhi, rows, count, coeffs)
    routed = lax.all_to_all(
        outgoing, ("gx", "gy", "gz"), split_axis=0, concat_axis=0, tiled=True
    )
    return relight(transfer, routed, basis, projector)


def solution(mesh):
    placed = (
        P(None, "gx", "gy", "gz"),
        P(None, None, ("gx", "gy", "gz")),
        P(None, ("gx", "gy", "gz")),
        P(None, ("gx", "gy", "gz")),
        P(None, ("gx", "gy", "gz")),
    )
    return jax.shard_map(
        halo_step,
        mesh=mesh,
        in_specs=placed,
        out_specs=P(None, ("gx", "gy", "gz")),
        check_vma=False,
    )
```

```python
import math

import jax
import jax.numpy as jnp
import numpy as np
from jax import lax
from jax.experimental import pallas as pl
from jax.experimental.pallas import tpu as pltpu
from jax.sharding import PartitionSpec as P


HALO = 2
SAMPLES = 8
DEGREES = 9
POLAR = 32
AZIMUTH = 32
LANES = 128
MIB = 1024 * 1024


def harmonic_values():
    polar = (np.arange(POLAR, dtype=np.float64) + 0.5) * (2.0 / POLAR) - 1.0
    beside = (np.arange(AZIMUTH, dtype=np.float64) + 0.5) * (2.0 * math.pi / AZIMUTH)
    cosines = np.repeat(polar, AZIMUTH)
    angles = np.tile(beside, POLAR)
    sines = np.sqrt(np.maximum(1.0 - cosines * cosines, 0.0))
    entries = {}
    for m in range(DEGREES):
        diagonal = (-1.0) ** m * float(math.prod(range(1, 2 * m, 2))) * sines**m
        legendre = {m: diagonal}
        if m + 1 < DEGREES:
            legendre[m + 1] = cosines * (2 * m + 1) * diagonal
        for l in range(m + 2, DEGREES):
            legendre[l] = (
                (2 * l - 1) * cosines * legendre[l - 1] - (l + m - 1) * legendre[l - 2]
            ) / (l - m)
        for l in range(m, DEGREES):
            factor = math.sqrt(
                (2 * l + 1) / (4.0 * math.pi) * math.factorial(l - m) / math.factorial(l + m)
            )
            if m == 0:
                entries[l, 0] = factor * legendre[l]
            else:
                entries[l, m] = math.sqrt(2.0) * factor * np.cos(m * angles) * legendre[l]
                entries[l, -m] = math.sqrt(2.0) * factor * np.sin(m * angles) * legendre[l]
    return np.stack([entries[l, m] for l in range(DEGREES) for m in range(-l, l + 1)])


def direction_tables():
    values = harmonic_values()
    basis = values.T.astype(np.float32).astype(jnp.bfloat16)
    projector = (values * (4.0 * math.pi / (POLAR * AZIMUTH))).astype(np.float32)
    return basis, projector.astype(jnp.bfloat16)


def fill_rows(get, spread, coeffs, rows_y, cells_z):
    halves = cells_z // LANES
    for c in range(coeffs):
        for h in range(halves):
            block = get(c, h).astype(jnp.float32)
            spread[h, pl.ds(c, rows_y, stride=coeffs), :] = block


def turn_rows(spread, eye, coeffs, rows_y, cells_z, put):
    halves = cells_z // LANES
    keep = -(-coeffs // 16) * 16
    zeros = jnp.zeros((LANES - keep, cells_z), jnp.bfloat16)
    for y in range(0, rows_y, 2):
        parts = []
        for i in (y, y + 1):
            rows = jnp.concatenate(
                [spread[h, i * coeffs : i * coeffs + keep, :] for h in range(halves)], axis=1
            )
            parts += [rows.astype(jnp.bfloat16), zeros]
        both = lax.dot_general(
            eye[...],
            jnp.concatenate(parts, axis=0),
            (((1,), (1,)), ((), ())),
            preferred_element_type=jnp.float32,
        )
        put(y, both[:, :LANES])
        put(y + 1, both[:, LANES:])


def spread_shape(coeffs, cells_y, cells_z):
    return pltpu.VMEM((cells_z // LANES, cells_y * coeffs + 16, LANES), jnp.float32)


def cut_faces(field):
    coeffs, cells_x, cells_y, cells_z = field.shape
    per_step = 9
    rows = cells_x * HALO
    corner = HALO * HALO

    def kernel(field, pick, last, first, top, bottom, *corners):
        for c in range(per_step):
            last[c] = field[c, cells_x - HALO :]
            first[c] = field[c, :HALO]
            chosen = jnp.dot(
                pick[...],
                field[c].reshape(cells_x * cells_y, cells_z),
                preferred_element_type=jnp.float32,
            ).astype(jnp.bfloat16)
            top[c] = chosen[:rows]
            bottom[c] = chosen[rows : 2 * rows]
            for q in range(4):
                at = 2 * rows + q * 16
                corners[q][c] = chosen[at : at + corner]

    pick = np.zeros((2 * rows + 64, cells_x * cells_y), np.float32)
    for x in range(cells_x):
        for j in range(HALO):
            pick[x * HALO + j, x * cells_y + cells_y - HALO + j] = 1.0
            pick[rows + x * HALO + j, x * cells_y + j] = 1.0
    for q in range(4):
        start_y = cells_y - HALO if q < 2 else 0
        start_x = cells_x - HALO if q % 2 == 0 else 0
        for i in range(HALO):
            for j in range(HALO):
                pick[2 * rows + q * 16 + i * HALO + j, (start_x + i) * cells_y + start_y + j] = 1.0
    shapes = [(coeffs, HALO, cells_y, cells_z)] * 2
    shapes += [(coeffs, rows, cells_z)] * 2 + [(coeffs, corner, cells_z)] * 4

    def whole(shape):
        zeros = (0,) * (len(shape) - 1)
        return pl.BlockSpec((per_step,) + shape[1:], lambda i: (i,) + zeros)

    return pl.pallas_call(
        kernel,
        out_shape=[pltpu.HBM(shape, jnp.bfloat16) for shape in shapes],
        grid=(coeffs // per_step,),
        in_specs=[whole(field.shape), pl.BlockSpec(pick.shape, lambda i: (0, 0))],
        out_specs=[whole(shape) for shape in shapes],
        compiler_params=pltpu.CompilerParams(vmem_limit_bytes=24 * MIB),
        name="cut_faces",
    )(field, jnp.asarray(pick.astype(jnp.bfloat16)))


def own_table(field, eye):
    coeffs, cells_x, cells_y, cells_z = field.shape
    plane = cells_y * cells_z

    def kernel(field, eye, out, spread):
        fill_rows(
            lambda c, h: field[c, 0, :, h * LANES : (h + 1) * LANES],
            spread,
            coeffs,
            cells_y,
            cells_z,
        )

        def put(y, block):
            out[y * cells_z : (y + 1) * cells_z, :] = block

        turn_rows(spread, eye, coeffs, cells_y, cells_z, put)

    return pl.pallas_call(
        kernel,
        out_shape=pltpu.HBM((cells_x * plane, LANES), jnp.float32),
        grid=(cells_x,),
        in_specs=[
            pl.BlockSpec((coeffs, 1, cells_y, cells_z), lambda x: (0, x, 0, 0)),
            pl.BlockSpec((cells_z, cells_z), lambda x: (0, 0)),
        ],
        out_specs=pl.BlockSpec((plane, LANES), lambda x: (x, 0)),
        scratch_shapes=[spread_shape(coeffs, cells_y, cells_z)],
        compiler_params=pltpu.CompilerParams(vmem_limit_bytes=16 * MIB),
        cost_estimate=pl.CostEstimate(
            flops=2 * 10**10, transcendentals=0, bytes_accessed=2 * 10**7
        ),
        name="own_table",
    )(field, eye)


def full_table(own, xlo, xhi, ylo, yhi, corners, eye, total_rows):
    coeffs, _, cells_y, cells_z = xlo.shape
    count = 2 * HALO + 3
    own_rows = own.shape[0]
    lines = own_rows // cells_z + count * cells_y

    def kernel(own, xlo, xhi, ylo, yhi, c0, c1, c2, c3, eye, table, zhi, zlo, *scratch):
        buf, sems, small, small_sems, spread, done = scratch
        inherit = pltpu.make_async_copy(own, table.at[pl.ds(0, own_rows), :], done)
        sources = [xlo.at[:, 0], xlo.at[:, 1], xhi.at[:, 0], xhi.at[:, 1], ylo, yhi]
        for p, source in enumerate(sources):
            pltpu.make_async_copy(source, buf.at[p], sems.at[p]).start()
        pieces = [
            pltpu.make_async_copy(corner, small.at[q], small_sems.at[q])
            for q, corner in enumerate((c0, c1, c2, c3))
        ]
        for piece in pieces:
            piece.start()
        inherit.start()

        def turn(p):
            def put(y, block):
                at = pl.multiple_of(own_rows + (p * cells_y + y) * cells_z, 8)
                table[pl.ds(at, cells_z), :] = block

            turn_rows(spread, eye, coeffs, cells_y, cells_z, put)

        def one(p, _):
            pltpu.make_async_copy(ylo, buf.at[p], sems.at[p]).wait()
            fill_rows(
                lambda c, h: buf[p, c, :, h * LANES : (h + 1) * LANES],
                spread,
                coeffs,
                cells_y,
                cells_z,
            )
            turn(p)
            return 0

        lax.fori_loop(0, count - 1, one, 0)
        for piece in pieces:
            piece.wait()
        fill_rows(
            lambda c, h: jnp.concatenate(
                [
                    small[q, c, :, h * LANES : (h + 1) * LANES].astype(jnp.float32)
                    for q in range(4)
                ],
                axis=0,
            ),
            spread,
            coeffs,
            cells_y,
            cells_z,
        )
        turn(count - 1)
        inherit.wait()
        for out, start in ((zhi, 0), (zlo, cells_z - HALO)):
            for j in range(HALO):
                for line in range(0, lines, 16):
                    parts = [
                        table[pl.ds((line + i) * cells_z + start + j, 8, stride=cells_z), :]
                        for i in (0, 8)
                    ]
                    out[j * lines + line : j * lines + line + 16, :] = jnp.concatenate(
                        parts, axis=0
                    ).astype(jnp.bfloat16)

    edge = jax.ShapeDtypeStruct((HALO * lines, LANES), jnp.bfloat16)
    vmem = pl.BlockSpec(memory_space=pltpu.VMEM)
    hbm = pl.BlockSpec(memory_space=pl.ANY)
    return pl.pallas_call(
        kernel,
        out_shape=(pltpu.VMEM((total_rows, LANES), jnp.float32), edge, edge),
        in_specs=[hbm] * 9 + [vmem],
        out_specs=(vmem, vmem, vmem),
        scratch_shapes=[
            pltpu.VMEM((count - 1, coeffs, cells_y, cells_z), jnp.bfloat16),
            pltpu.SemaphoreType.DMA((count - 1,)),
            pltpu.VMEM((4, coeffs, HALO * HALO, cells_z), jnp.bfloat16),
            pltpu.SemaphoreType.DMA((4,)),
            spread_shape(coeffs, cells_y, cells_z),
            pltpu.SemaphoreType.DMA(()),
        ],
        compiler_params=pltpu.CompilerParams(vmem_limit_bytes=24 * MIB),
        cost_estimate=pl.CostEstimate(
            flops=2 * 10**10, transcendentals=0, bytes_accessed=2 * 10**7
        ),
        name="full_table",
    )(own, xlo, xhi, ylo, yhi, *corners, eye)


GROUP = 8
PARTS = 3


def prepare(samples, weights, slot, origin, cells, total):
    count = slot.shape[0]
    cells_x, cells_y, cells_z = cells
    own_lines = cells_x * cells_y
    lines = own_lines + (2 * HALO + 3) * cells_y
    rows = lines * cells_z
    block = 256
    burst = 32
    kinds = (2 + PARTS) * SAMPLES

    def locate(near_x, near_y, near_z):
        own_x = (near_x >= HALO) & (near_x < HALO + cells_x)
        own_y = (near_y >= HALO) & (near_y < HALO + cells_y)
        low_y = near_y < HALO
        side_x = jnp.where(near_x < HALO, near_x, near_x - cells_x)
        side_y = jnp.where(low_y, near_y, near_y - HALO - cells_y)
        line_own = jnp.where(own_x, near_x - HALO, cells_x + side_x) * cells_y + near_y - HALO
        line_y = (
            (cells_x + 2 * HALO) * cells_y
            + jnp.where(low_y, 0, cells_y)
            + (near_x - HALO) * HALO
            + side_y
        )
        line_corner = (
            (cells_x + 2 * HALO + 2) * cells_y
            + jnp.where(low_y, 0, 2 * HALO * HALO)
            + side_x * HALO
            + side_y
        )
        line = jnp.where(own_y, line_own, jnp.where(own_x, line_y, line_corner))
        inside = line * cells_z + near_z - HALO
        below = rows + near_z * lines + line
        above = rows + (near_z - cells_z) * lines + line
        return jnp.where(near_z < HALO, below, jnp.where(near_z < HALO + cells_z, inside, above))

    def kernel(origin, slot, samples, weights, eye, join, index, ordered, natural):
        def turn(j, _):
            at = pl.multiple_of(j * block, block)
            near = []
            for d in range(3):
                shift = samples[d, :, pl.ds(at, block)] - origin[d] + HALO
                shift = jnp.where(shift < 0, shift + total[d], shift)
                near.append(jnp.where(shift >= total[d], shift - total[d], shift))
            row = locate(*near)
            pieces = [(row >> 8).astype(jnp.float32), (row & 255).astype(jnp.float32)]
            rest = weights[:, pl.ds(at, block)]
            for _ in range(PARTS):
                piece = rest.astype(jnp.bfloat16).astype(jnp.float32)
                pieces.append(piece)
                rest = rest - piece
            pieces.append(jnp.zeros((LANES - kinds, block), jnp.float32))
            natural[pl.ds(at, block), :] = lax.dot_general(
                eye[...],
                jnp.concatenate(pieces, axis=0).astype(jnp.bfloat16),
                (((1,), (1,)), ((), ())),
                preferred_element_type=jnp.float32,
            )
            return 0

        lax.fori_loop(0, count // block, turn, 0)

        def scatter(j, _):
            at = pl.multiple_of(j * burst, burst)
            mine = slot.at[pl.ds(at, burst)]
            for g in range(0, burst, GROUP):
                tile = natural[pl.ds(at + g, GROUP), :]
                for k in range(GROUP):
                    ordered[pl.ds(mine[g + k], 1), :] = tile[k : k + 1, :]
            return 0

        lax.fori_loop(0, count // burst, scatter, 0)

        def collect(j, _):
            at = pl.multiple_of(j * 4 * LANES, 4 * LANES)
            wide = lax.dot_general(
                join[...],
                ordered[pl.ds(at, 4 * LANES), :].astype(jnp.bfloat16),
                (((1,), (1,)), ((), ())),
                preferred_element_type=jnp.float32,
            ).astype(jnp.int32)
            for i in range(4):
                to = pl.multiple_of((j * 4 + i) * SAMPLES, SAMPLES)
                index[pl.ds(to, SAMPLES), :] = wide[:SAMPLES, i * LANES : (i + 1) * LANES]
            return 0

        lax.fori_loop(0, count // (4 * LANES), collect, 0)

    join = np.zeros((16, LANES), np.float32)
    for s in range(SAMPLES):
        join[s, s] = 256.0
        join[s, SAMPLES + s] = 1.0
    vmem = pl.BlockSpec(memory_space=pltpu.VMEM)
    smem = pl.BlockSpec(memory_space=pltpu.SMEM)
    return pl.pallas_call(
        kernel,
        out_shape=(
            jax.ShapeDtypeStruct((count * SAMPLES // LANES, LANES), jnp.int32),
            jax.ShapeDtypeStruct((count, LANES), jnp.float32),
        ),
        in_specs=[smem, smem, vmem, vmem, vmem, vmem],
        out_specs=(vmem, vmem),
        scratch_shapes=[pltpu.VMEM((count, LANES), jnp.float32)],
        compiler_params=pltpu.CompilerParams(vmem_limit_bytes=12 * MIB),
        cost_estimate=pl.CostEstimate(
            flops=2 * 10**10, transcendentals=0, bytes_accessed=3 * 10**6
        ),
        name="prepare",
    )(
        origin,
        slot,
        samples,
        weights,
        jnp.asarray(np.eye(block, dtype=np.float32).astype(jnp.bfloat16)),
        jnp.asarray(join.astype(jnp.bfloat16)),
    )


def spread_weights(ordered):
    count = ordered.shape[0]
    block = 512

    def kernel(ordered, ones, wide):
        rows = ordered[...].astype(jnp.bfloat16)
        for h in range(0, SAMPLES, 2):
            both = jnp.dot(
                rows, ones[:, h * LANES : (h + 2) * LANES], preferred_element_type=jnp.float32
            )
            for s in range(2):
                for g in range(block // GROUP):
                    to = (g * SAMPLES + h + s) * GROUP
                    wide[to : to + GROUP, :] = both[
                        g * GROUP : (g + 1) * GROUP, s * LANES : (s + 1) * LANES
                    ]

    ones = np.zeros((LANES, SAMPLES * LANES), np.float32)
    for s in range(SAMPLES):
        for p in range(PARTS):
            ones[(2 + p) * SAMPLES + s, s * LANES : (s + 1) * LANES] = 1.0
    return pl.pallas_call(
        kernel,
        out_shape=pltpu.HBM((count * SAMPLES, LANES), jnp.float32),
        grid=(count // block,),
        in_specs=[
            pl.BlockSpec((block, LANES), lambda i: (i, 0)),
            pl.BlockSpec(ones.shape, lambda i: (0, 0)),
        ],
        out_specs=pl.BlockSpec((block * SAMPLES, LANES), lambda i: (i, 0)),
        compiler_params=pltpu.CompilerParams(vmem_limit_bytes=12 * MIB),
        cost_estimate=pl.CostEstimate(
            flops=10**10, transcendentals=0, bytes_accessed=3 * 10**6
        ),
        name="spread_weights",
    )(ordered, jnp.asarray(ones.astype(jnp.bfloat16)))


RING = 2
CHUNK = 1024


def gather_rows(index, wide, table, zlo, zhi, first_edge, count, coeffs):
    edges = zlo.shape[0]
    chunks = index.shape[0] // CHUNK
    per_chunk = CHUNK // SAMPLES
    groups = per_chunk // GROUP
    pairs = count // 32
    half = LANES // 2

    def kernel(index, zlo, zhi, pick, wide, table_in, table, out, *scratch):
        local, sems, near, near_sems, rows = scratch
        table[pl.ds(first_edge, edges), :] = zlo[...].astype(jnp.float32)
        table[pl.ds(first_edge + edges, edges), :] = zhi[...].astype(jnp.float32)
        sublane = lax.broadcasted_iota(jnp.int32, (GROUP, LANES), 0)
        masks = [sublane == k for k in range(GROUP)]
        used = lax.broadcasted_iota(jnp.int32, (GROUP, LANES), 1) < coeffs

        def fetch(n, slot):
            return pltpu.make_async_copy(
                index.at[pl.ds(pl.multiple_of(n * CHUNK, CHUNK), CHUNK)],
                local.at[slot],
                sems.at[slot],
            )

        def stream(n, slot):
            return pltpu.make_async_copy(
                wide.at[pl.ds(pl.multiple_of(n * CHUNK, CHUNK), CHUNK), :],
                near.at[slot],
                near_sems.at[slot],
            )

        for b in range(RING - 1):
            fetch(b, b).start()
            stream(b, b).start()

        def body(i, _):
            for b in range(RING):
                n = i * RING + b
                fetch(n, b).wait()
                stream(n, b).wait()
                ahead = n + RING - 1

                @pl.when(ahead < chunks)
                def _():
                    fetch(ahead, (b + RING - 1) % RING).start()
                    stream(ahead, (b + RING - 1) % RING).start()

                for q in range(groups):
                    total = None
                    for s in range(SAMPLES):
                        merged = None
                        for k in range(GROUP):
                            place = s * per_chunk + q * GROUP + k
                            row = table[pl.ds(local[b, place], GROUP, stride=0), :]
                            merged = row if merged is None else jnp.where(masks[k], row, merged)
                        at = (q * SAMPLES + s) * GROUP
                        term = merged * near[b, at : at + GROUP, :]
                        total = term if total is None else total + term
                    to = pl.multiple_of((n * (groups // 4) + q // 4) * GROUP, GROUP)
                    rows[q % 4, pl.ds(to, GROUP), :] = jnp.where(used, total, 0.0)
            return 0

        lax.fori_loop(0, chunks // RING, body, 0)

        def pack(i, _):
            at = pl.multiple_of(i * 128, 128)
            part = [rows[q, pl.ds(at, 128), :].astype(jnp.bfloat16) for q in range(4)]
            outer = [jnp.concatenate([part[0], part[2]], axis=1)]
            outer.append(jnp.concatenate([part[1], part[3]], axis=1))
            first = jnp.dot(outer[0], pick[0], preferred_element_type=jnp.float32)
            second = jnp.dot(outer[1], pick[0], preferred_element_type=jnp.float32)
            third = jnp.dot(outer[0], pick[1], preferred_element_type=jnp.float32)
            third += jnp.dot(outer[1], pick[2], preferred_element_type=jnp.float32)
            for d in range(128 // GROUP):
                here = slice(d * GROUP, (d + 1) * GROUP)
                out[i * (128 // GROUP) + d, :16, :] = jnp.concatenate(
                    [first[here], second[here]], axis=0
                ).astype(jnp.bfloat16)
                out[i * (128 // GROUP) + d, 16:, :] = third[here].astype(jnp.bfloat16)
            return 0

        lax.fori_loop(0, pairs * GROUP // 128, pack, 0)

    pick = np.zeros((3, 2 * LANES, LANES), np.float32)
    for c in range(half):
        pick[0, c, c] = 1.0
        pick[0, LANES + c, half + c] = 1.0
    for c in range(32):
        pick[1, half + c, c] = 1.0
        pick[1, LANES + half + c, 64 + c] = 1.0
        pick[2, half + c, 32 + c] = 1.0
        pick[2, LANES + half + c, 96 + c] = 1.0
    vmem = pl.BlockSpec(memory_space=pltpu.VMEM)
    return pl.pallas_call(
        kernel,
        out_shape=(
            pltpu.VMEM(table.shape, jnp.float32),
            jax.ShapeDtypeStruct((pairs, 24, LANES), jnp.bfloat16),
        ),
        in_specs=[vmem] * 4 + [pl.BlockSpec(memory_space=pl.ANY), vmem],
        out_specs=(vmem, vmem),
        scratch_shapes=[
            pltpu.SMEM((RING, CHUNK), jnp.int32),
            pltpu.SemaphoreType.DMA((RING,)),
            pltpu.VMEM((RING, CHUNK, LANES), jnp.float32),
            pltpu.SemaphoreType.DMA((RING,)),
            pltpu.VMEM((4, pairs * GROUP, LANES), jnp.float32),
        ],
        input_output_aliases={5: 0},
        compiler_params=pltpu.CompilerParams(vmem_limit_bytes=24 * MIB),
        cost_estimate=pl.CostEstimate(
            flops=4 * 10**10, transcendentals=0, bytes_accessed=2 * 10**7
        ),
        name="gather_rows",
    )(index, zlo, zhi, jnp.asarray(pick.astype(jnp.bfloat16)), wide, table)[1]


def relight(transfer, routed, basis, projector):
    coeffs, count = transfer.shape
    sources, packed, _ = routed.shape
    per_pair = count // sources
    block = 512
    step = block // per_pair

    def kernel(transfer, routed, basis, wide, projector, out):
        low = lax.broadcasted_iota(jnp.int32, (GROUP, LANES), 1) < 64
        parts = []
        for i in range(step):
            head = routed[i, :16, :].astype(jnp.float32)
            first, second = head[:GROUP], head[GROUP:]
            third = routed[i, 16:, :].astype(jnp.float32)
            parts += [
                jnp.where(low, first, pltpu.roll(third, 64, 1)),
                jnp.where(low, second, pltpu.roll(third, 32, 1)),
                jnp.where(low, pltpu.roll(first, 64, 1), third),
                jnp.where(low, pltpu.roll(second, 64, 1), pltpu.roll(third, 96, 1)),
            ]
        rows = jnp.concatenate(parts, axis=0).astype(jnp.bfloat16)
        lit = jnp.dot(basis[...], transfer[...], preferred_element_type=jnp.float32)
        shade = lax.dot_general(
            wide[...], rows, (((1,), (1,)), ((), ())), preferred_element_type=jnp.float32
        )
        product = (lit * shade).astype(jnp.bfloat16)
        out[...] = jnp.dot(projector[...], product, preferred_element_type=jnp.float32).astype(
            jnp.bfloat16
        )

    directions = basis.shape[0]
    wide = np.zeros((directions, LANES), jnp.bfloat16)
    wide[:, :coeffs] = basis
    return pl.pallas_call(
        kernel,
        out_shape=jax.ShapeDtypeStruct((coeffs, count), jnp.bfloat16),
        grid=(count // block,),
        in_specs=[
            pl.BlockSpec((coeffs, block), lambda i: (0, i)),
            pl.BlockSpec((step, packed, LANES), lambda i: (i, 0, 0)),
            pl.BlockSpec((directions, coeffs), lambda i: (0, 0)),
            pl.BlockSpec((directions, LANES), lambda i: (0, 0)),
            pl.BlockSpec((coeffs, directions), lambda i: (0, 0)),
        ],
        out_specs=pl.BlockSpec((coeffs, block), lambda i: (0, i)),
        compiler_params=pltpu.CompilerParams(vmem_limit_bytes=40 * MIB),
        name="relight",
    )(transfer, routed, jnp.asarray(basis), jnp.asarray(wide), jnp.asarray(projector))


def moves(sizes, steps):
    pairs = []
    for x in range(sizes[0]):
        for y in range(sizes[1]):
            to_x, to_y = (x + steps[0]) % sizes[0], (y + steps[1]) % sizes[1]
            pairs.append((x * sizes[1] + y, to_x * sizes[1] + to_y))
    return pairs


def halo_step(field, samples, weights, destination, transfer):
    basis, projector = direction_tables()
    coeffs, cells_x, cells_y, cells_z = field.shape
    count = transfer.shape[1]
    along = tuple(lax.axis_size(axis) for axis in ("gx", "gy", "gz"))
    ups = [moves((n, 1), (1, 0)) for n in along]
    downs = [moves((n, 1), (-1, 0)) for n in along]

    last, first, top, bottom, *pieces = cut_faces(field)
    xlo = lax.ppermute(last, "gx", ups[0])
    xhi = lax.ppermute(first, "gx", downs[0])
    ylo = lax.ppermute(top, "gy", ups[1])
    yhi = lax.ppermute(bottom, "gy", downs[1])
    corners = []
    for piece, step in zip(pieces, ((1, 1), (-1, 1), (1, -1), (-1, -1))):
        corners.append(lax.ppermute(piece, ("gx", "gy"), moves(along[:2], step)))

    lines = cells_x * cells_y + (2 * HALO + 3) * cells_y
    rows = lines * cells_z
    cells = (cells_x, cells_y, cells_z)
    total = tuple(c * n for c, n in zip(cells, along))
    origin = jnp.stack(
        [lax.axis_index(axis) * c for axis, c in zip(("gx", "gy", "gz"), cells)]
    ).astype(jnp.int32)
    devices = math.prod(along)
    per_pair = count // devices
    slot = destination[0] * per_pair + destination[1]

    eye = jnp.asarray(np.eye(cells_z, dtype=np.float32).astype(jnp.bfloat16))
    own = own_table(field, eye)
    index, ordered = prepare(samples, weights, slot, origin, cells, total)
    wide = spread_weights(ordered)
    own, index, wide = lax.optimization_barrier((own, index, wide))
    table, edge_lo, edge_hi = full_table(
        own, xlo, xhi, ylo, yhi, corners, eye, rows + 2 * HALO * lines
    )
    zhi = lax.ppermute(edge_lo, "gz", downs[2])
    zlo = lax.ppermute(edge_hi, "gz", ups[2])
    outgoing = gather_rows(index.reshape(-1), wide, table, zlo, zhi, rows, count, coeffs)
    routed = lax.all_to_all(
        outgoing, ("gx", "gy", "gz"), split_axis=0, concat_axis=0, tiled=True
    )
    return relight(transfer, routed, basis, projector)


def solution(mesh):
    placed = (
        P(None, "gx", "gy", "gz"),
        P(None, None, ("gx", "gy", "gz")),
        P(None, ("gx", "gy", "gz")),
        P(None, ("gx", "gy", "gz")),
        P(None, ("gx", "gy", "gz")),
    )
    return jax.shard_map(
        halo_step,
        mesh=mesh,
        in_specs=placed,
        out_specs=P(None, ("gx", "gy", "gz")),
        check_vma=False,
    )
```

```python
import math

import jax
import jax.numpy as jnp
import numpy as np
from jax import lax
from jax.experimental import pallas as pl
from jax.experimental.pallas import tpu as pltpu
from jax.sharding import PartitionSpec as P


HALO = 2
SAMPLES = 8
DEGREES = 9
POLAR = 32
AZIMUTH = 32
LANES = 128
MIB = 1024 * 1024


def harmonic_values():
    polar = (np.arange(POLAR, dtype=np.float64) + 0.5) * (2.0 / POLAR) - 1.0
    beside = (np.arange(AZIMUTH, dtype=np.float64) + 0.5) * (2.0 * math.pi / AZIMUTH)
    cosines = np.repeat(polar, AZIMUTH)
    angles = np.tile(beside, POLAR)
    sines = np.sqrt(np.maximum(1.0 - cosines * cosines, 0.0))
    entries = {}
    for m in range(DEGREES):
        diagonal = (-1.0) ** m * float(math.prod(range(1, 2 * m, 2))) * sines**m
        legendre = {m: diagonal}
        if m + 1 < DEGREES:
            legendre[m + 1] = cosines * (2 * m + 1) * diagonal
        for l in range(m + 2, DEGREES):
            legendre[l] = (
                (2 * l - 1) * cosines * legendre[l - 1] - (l + m - 1) * legendre[l - 2]
            ) / (l - m)
        for l in range(m, DEGREES):
            factor = math.sqrt(
                (2 * l + 1) / (4.0 * math.pi) * math.factorial(l - m) / math.factorial(l + m)
            )
            if m == 0:
                entries[l, 0] = factor * legendre[l]
            else:
                entries[l, m] = math.sqrt(2.0) * factor * np.cos(m * angles) * legendre[l]
                entries[l, -m] = math.sqrt(2.0) * factor * np.sin(m * angles) * legendre[l]
    return np.stack([entries[l, m] for l in range(DEGREES) for m in range(-l, l + 1)])


def direction_tables():
    values = harmonic_values()
    basis = values.T.astype(np.float32).astype(jnp.bfloat16)
    projector = (values * (4.0 * math.pi / (POLAR * AZIMUTH))).astype(np.float32)
    return basis, projector.astype(jnp.bfloat16)


def fill_rows(get, spread, coeffs, rows_y, cells_z):
    halves = cells_z // LANES
    for c in range(coeffs):
        for h in range(halves):
            block = get(c, h).astype(jnp.float32)
            spread[h, pl.ds(c, rows_y, stride=coeffs), :] = block


def turn_rows(spread, eye, coeffs, rows_y, cells_z, put):
    halves = cells_z // LANES
    keep = -(-coeffs // 16) * 16
    zeros = jnp.zeros((LANES - keep, cells_z), jnp.bfloat16)
    for y in range(0, rows_y, 2):
        parts = []
        for i in (y, y + 1):
            rows = jnp.concatenate(
                [spread[h, i * coeffs : i * coeffs + keep, :] for h in range(halves)], axis=1
            )
            parts += [rows.astype(jnp.bfloat16), zeros]
        both = lax.dot_general(
            eye[...],
            jnp.concatenate(parts, axis=0),
            (((1,), (1,)), ((), ())),
            preferred_element_type=jnp.float32,
        )
        put(y, both[:, :LANES])
        put(y + 1, both[:, LANES:])


def spread_shape(coeffs, cells_y, cells_z):
    return pltpu.VMEM((cells_z // LANES, cells_y * coeffs + 16, LANES), jnp.float32)


def cut_faces(field):
    coeffs, cells_x, cells_y, cells_z = field.shape
    per_step = 9
    rows = cells_x * HALO

    def kernel(field, pick, last, first, top, bottom):
        for c in range(per_step):
            last[c] = field[c, cells_x - HALO :]
            first[c] = field[c, :HALO]
            chosen = jnp.dot(
                pick[...],
                field[c].reshape(cells_x * cells_y, cells_z),
                preferred_element_type=jnp.float32,
            ).astype(jnp.bfloat16)
            top[c] = chosen[:rows]
            bottom[c] = chosen[rows:]

    pick = np.zeros((2 * rows, cells_x * cells_y), np.float32)
    for x in range(cells_x):
        for j in range(HALO):
            pick[x * HALO + j, x * cells_y + cells_y - HALO + j] = 1.0
            pick[rows + x * HALO + j, x * cells_y + j] = 1.0
    shapes = [(coeffs, HALO, cells_y, cells_z)] * 2
    shapes += [(coeffs, rows, cells_z)] * 2

    def whole(shape):
        zeros = (0,) * (len(shape) - 1)
        return pl.BlockSpec((per_step,) + shape[1:], lambda i: (i,) + zeros)

    return pl.pallas_call(
        kernel,
        out_shape=[pltpu.HBM(shape, jnp.bfloat16) for shape in shapes],
        grid=(coeffs // per_step,),
        in_specs=[whole(field.shape), pl.BlockSpec(pick.shape, lambda i: (0, 0))],
        out_specs=[whole(shape) for shape in shapes],
        compiler_params=pltpu.CompilerParams(vmem_limit_bytes=24 * MIB),
        name="cut_faces",
    )(field, jnp.asarray(pick.astype(jnp.bfloat16)))


def cut_corners(ylo, yhi):
    coeffs, rows, cells_z = ylo.shape
    per_step = 27
    corner = HALO * HALO

    def kernel(ylo, yhi, pick, up, down):
        for c in range(per_step):
            chosen = jnp.dot(
                pick[...],
                jnp.concatenate([ylo[c], yhi[c]], axis=0),
                preferred_element_type=jnp.float32,
            )
            up[c] = chosen[: 2 * corner].astype(jnp.bfloat16)
            down[c] = chosen[2 * corner :].astype(jnp.bfloat16)

    pick = np.zeros((4 * corner, 2 * rows), np.float32)
    for side in range(2):
        for i in range(corner):
            pick[side * corner + i, side * rows + rows - corner + i] = 1.0
            pick[2 * corner + side * corner + i, side * rows + i] = 1.0
    shape = (coeffs, 2 * corner, cells_z)
    face = pl.BlockSpec((per_step, rows, cells_z), lambda i: (i, 0, 0))
    piece = pl.BlockSpec((per_step,) + shape[1:], lambda i: (i, 0, 0))
    return pl.pallas_call(
        kernel,
        out_shape=[pltpu.HBM(shape, jnp.bfloat16)] * 2,
        grid=(coeffs // per_step,),
        in_specs=[face, face, pl.BlockSpec(pick.shape, lambda i: (0, 0))],
        out_specs=[piece, piece],
        compiler_params=pltpu.CompilerParams(vmem_limit_bytes=24 * MIB),
        name="cut_corners",
    )(ylo, yhi, jnp.asarray(pick.astype(jnp.bfloat16)))


def own_table(field, eye):
    coeffs, cells_x, cells_y, cells_z = field.shape
    plane = cells_y * cells_z

    def kernel(field, eye, out, spread):
        fill_rows(
            lambda c, h: field[c, 0, :, h * LANES : (h + 1) * LANES],
            spread,
            coeffs,
            cells_y,
            cells_z,
        )

        def put(y, block):
            out[y * cells_z : (y + 1) * cells_z, :] = block

        turn_rows(spread, eye, coeffs, cells_y, cells_z, put)

    return pl.pallas_call(
        kernel,
        out_shape=pltpu.HBM((cells_x * plane, LANES), jnp.float32),
        grid=(cells_x,),
        in_specs=[
            pl.BlockSpec((coeffs, 1, cells_y, cells_z), lambda x: (0, x, 0, 0)),
            pl.BlockSpec((cells_z, cells_z), lambda x: (0, 0)),
        ],
        out_specs=pl.BlockSpec((plane, LANES), lambda x: (x, 0)),
        scratch_shapes=[spread_shape(coeffs, cells_y, cells_z)],
        compiler_params=pltpu.CompilerParams(vmem_limit_bytes=16 * MIB),
        cost_estimate=pl.CostEstimate(
            flops=2 * 10**10, transcendentals=0, bytes_accessed=2 * 10**7
        ),
        name="own_table",
    )(field, eye)


def full_table(own, xlo, xhi, ylo, yhi, corners, eye, total_rows):
    coeffs, _, cells_y, cells_z = xlo.shape
    count = 2 * HALO + 3
    own_rows = own.shape[0]
    lines = own_rows // cells_z + count * cells_y

    def kernel(own, xlo, xhi, ylo, yhi, clo, chi, eye, table, zhi, zlo, *scratch):
        buf, sems, small, small_sems, spread, done = scratch
        inherit = pltpu.make_async_copy(own, table.at[pl.ds(0, own_rows), :], done)
        sources = [xlo.at[:, 0], xlo.at[:, 1], xhi.at[:, 0], xhi.at[:, 1], ylo, yhi]
        for p, source in enumerate(sources):
            pltpu.make_async_copy(source, buf.at[p], sems.at[p]).start()
        pieces = [
            pltpu.make_async_copy(corner, small.at[q], small_sems.at[q])
            for q, corner in enumerate((clo, chi))
        ]
        for piece in pieces:
            piece.start()
        inherit.start()

        def turn(p):
            def put(y, block):
                at = pl.multiple_of(own_rows + (p * cells_y + y) * cells_z, 8)
                table[pl.ds(at, cells_z), :] = block

            turn_rows(spread, eye, coeffs, cells_y, cells_z, put)

        def one(p, _):
            pltpu.make_async_copy(ylo, buf.at[p], sems.at[p]).wait()
            fill_rows(
                lambda c, h: buf[p, c, :, h * LANES : (h + 1) * LANES],
                spread,
                coeffs,
                cells_y,
                cells_z,
            )
            turn(p)
            return 0

        lax.fori_loop(0, count - 1, one, 0)
        for piece in pieces:
            piece.wait()
        fill_rows(
            lambda c, h: jnp.concatenate(
                [
                    small[q, c, :, h * LANES : (h + 1) * LANES].astype(jnp.float32)
                    for q in range(2)
                ],
                axis=0,
            ),
            spread,
            coeffs,
            cells_y,
            cells_z,
        )
        turn(count - 1)
        inherit.wait()
        for out, start in ((zhi, 0), (zlo, cells_z - HALO)):
            for j in range(HALO):
                for line in range(0, lines, 16):
                    parts = [
                        table[pl.ds((line + i) * cells_z + start + j, 8, stride=cells_z), :]
                        for i in (0, 8)
                    ]
                    out[j * lines + line : j * lines + line + 16, :] = jnp.concatenate(
                        parts, axis=0
                    ).astype(jnp.bfloat16)

    edge = jax.ShapeDtypeStruct((HALO * lines, LANES), jnp.bfloat16)
    vmem = pl.BlockSpec(memory_space=pltpu.VMEM)
    hbm = pl.BlockSpec(memory_space=pl.ANY)
    return pl.pallas_call(
        kernel,
        out_shape=(pltpu.VMEM((total_rows, LANES), jnp.float32), edge, edge),
        in_specs=[hbm] * 7 + [vmem],
        out_specs=(vmem, vmem, vmem),
        scratch_shapes=[
            pltpu.VMEM((count - 1, coeffs, cells_y, cells_z), jnp.bfloat16),
            pltpu.SemaphoreType.DMA((count - 1,)),
            pltpu.VMEM((2, coeffs, 2 * HALO * HALO, cells_z), jnp.bfloat16),
            pltpu.SemaphoreType.DMA((2,)),
            spread_shape(coeffs, cells_y, cells_z),
            pltpu.SemaphoreType.DMA(()),
        ],
        compiler_params=pltpu.CompilerParams(vmem_limit_bytes=24 * MIB),
        cost_estimate=pl.CostEstimate(
            flops=2 * 10**10, transcendentals=0, bytes_accessed=2 * 10**7
        ),
        name="full_table",
    )(own, xlo, xhi, ylo, yhi, *corners, eye)


GROUP = 8
PARTS = 3


def prepare(samples, weights, slot, origin, cells, total):
    count = slot.shape[0]
    cells_x, cells_y, cells_z = cells
    own_lines = cells_x * cells_y
    lines = own_lines + (2 * HALO + 3) * cells_y
    rows = lines * cells_z
    block = 256
    burst = 32
    kinds = (2 + PARTS) * SAMPLES

    def locate(near_x, near_y, near_z):
        own_x = (near_x >= HALO) & (near_x < HALO + cells_x)
        own_y = (near_y >= HALO) & (near_y < HALO + cells_y)
        low_y = near_y < HALO
        side_x = jnp.where(near_x < HALO, near_x, near_x - cells_x)
        side_y = jnp.where(low_y, near_y, near_y - HALO - cells_y)
        line_own = jnp.where(own_x, near_x - HALO, cells_x + side_x) * cells_y + near_y - HALO
        line_y = (
            (cells_x + 2 * HALO) * cells_y
            + jnp.where(low_y, 0, cells_y)
            + (near_x - HALO) * HALO
            + side_y
        )
        line_corner = (
            (cells_x + 2 * HALO + 2) * cells_y
            + jnp.where(near_x < HALO, 0, HALO * HALO)
            + jnp.where(low_y, 0, HALO * HALO)
            + side_x * HALO
            + side_y
        )
        line = jnp.where(own_y, line_own, jnp.where(own_x, line_y, line_corner))
        inside = line * cells_z + near_z - HALO
        below = rows + near_z * lines + line
        above = rows + (near_z - cells_z) * lines + line
        return jnp.where(near_z < HALO, below, jnp.where(near_z < HALO + cells_z, inside, above))

    def kernel(origin, slot, samples, weights, eye, join, index, ordered, natural):
        def turn(j, _):
            at = pl.multiple_of(j * block, block)
            near = []
            for d in range(3):
                shift = samples[d, :, pl.ds(at, block)] - origin[d] + HALO
                shift = jnp.where(shift < 0, shift + total[d], shift)
                near.append(jnp.where(shift >= total[d], shift - total[d], shift))
            row = locate(*near)
            pieces = [(row >> 8).astype(jnp.float32), (row & 255).astype(jnp.float32)]
            rest = weights[:, pl.ds(at, block)]
            for _ in range(PARTS):
                piece = rest.astype(jnp.bfloat16).astype(jnp.float32)
                pieces.append(piece)
                rest = rest - piece
            pieces.append(jnp.zeros((LANES - kinds, block), jnp.float32))
            natural[pl.ds(at, block), :] = lax.dot_general(
                eye[...],
                jnp.concatenate(pieces, axis=0).astype(jnp.bfloat16),
                (((1,), (1,)), ((), ())),
                preferred_element_type=jnp.float32,
            )
            return 0

        lax.fori_loop(0, count // block, turn, 0)

        def scatter(j, _):
            at = pl.multiple_of(j * burst, burst)
            mine = slot.at[pl.ds(at, burst)]
            for g in range(0, burst, GROUP):
                tile = natural[pl.ds(at + g, GROUP), :]
                for k in range(GROUP):
                    ordered[pl.ds(mine[g + k], 1), :] = tile[k : k + 1, :]
            return 0

        lax.fori_loop(0, count // burst, scatter, 0)

        def collect(j, _):
            at = pl.multiple_of(j * 4 * LANES, 4 * LANES)
            wide = lax.dot_general(
                join[...],
                ordered[pl.ds(at, 4 * LANES), :].astype(jnp.bfloat16),
                (((1,), (1,)), ((), ())),
                preferred_element_type=jnp.float32,
            ).astype(jnp.int32)
            for i in range(4):
                to = pl.multiple_of((j * 4 + i) * SAMPLES, SAMPLES)
                index[pl.ds(to, SAMPLES), :] = wide[:SAMPLES, i * LANES : (i + 1) * LANES]
            return 0

        lax.fori_loop(0, count // (4 * LANES), collect, 0)

    join = np.zeros((16, LANES), np.float32)
    for s in range(SAMPLES):
        join[s, s] = 256.0
        join[s, SAMPLES + s] = 1.0
    vmem = pl.BlockSpec(memory_space=pltpu.VMEM)
    smem = pl.BlockSpec(memory_space=pltpu.SMEM)
    return pl.pallas_call(
        kernel,
        out_shape=(
            jax.ShapeDtypeStruct((count * SAMPLES // LANES, LANES), jnp.int32),
            jax.ShapeDtypeStruct((count, LANES), jnp.float32),
        ),
        in_specs=[smem, smem, vmem, vmem, vmem, vmem],
        out_specs=(vmem, vmem),
        scratch_shapes=[pltpu.VMEM((count, LANES), jnp.float32)],
        compiler_params=pltpu.CompilerParams(vmem_limit_bytes=12 * MIB),
        cost_estimate=pl.CostEstimate(
            flops=2 * 10**10, transcendentals=0, bytes_accessed=3 * 10**6
        ),
        name="prepare",
    )(
        origin,
        slot,
        samples,
        weights,
        jnp.asarray(np.eye(block, dtype=np.float32).astype(jnp.bfloat16)),
        jnp.asarray(join.astype(jnp.bfloat16)),
    )


def spread_weights(ordered):
    count = ordered.shape[0]
    block = 512

    def kernel(ordered, ones, wide):
        rows = ordered[...].astype(jnp.bfloat16)
        for h in range(0, SAMPLES, 2):
            both = jnp.dot(
                rows, ones[:, h * LANES : (h + 2) * LANES], preferred_element_type=jnp.float32
            )
            for s in range(2):
                for g in range(block // GROUP):
                    to = (g * SAMPLES + h + s) * GROUP
                    wide[to : to + GROUP, :] = both[
                        g * GROUP : (g + 1) * GROUP, s * LANES : (s + 1) * LANES
                    ]

    ones = np.zeros((LANES, SAMPLES * LANES), np.float32)
    for s in range(SAMPLES):
        for p in range(PARTS):
            ones[(2 + p) * SAMPLES + s, s * LANES : (s + 1) * LANES] = 1.0
    return pl.pallas_call(
        kernel,
        out_shape=pltpu.HBM((count * SAMPLES, LANES), jnp.float32),
        grid=(count // block,),
        in_specs=[
            pl.BlockSpec((block, LANES), lambda i: (i, 0)),
            pl.BlockSpec(ones.shape, lambda i: (0, 0)),
        ],
        out_specs=pl.BlockSpec((block * SAMPLES, LANES), lambda i: (i, 0)),
        compiler_params=pltpu.CompilerParams(vmem_limit_bytes=12 * MIB),
        cost_estimate=pl.CostEstimate(
            flops=10**10, transcendentals=0, bytes_accessed=3 * 10**6
        ),
        name="spread_weights",
    )(ordered, jnp.asarray(ones.astype(jnp.bfloat16)))


RING = 2
STREAM = 8
CHUNK = 1024


def gather_rows(index, wide, table, zlo, zhi, first_edge, count, coeffs):
    edges = zlo.shape[0]
    chunks = index.shape[0] // CHUNK
    per_chunk = CHUNK // SAMPLES
    groups = per_chunk // GROUP
    pairs = count // 32
    half = LANES // 2

    def kernel(index, zlo, zhi, pick, wide, table_in, table, out, *scratch):
        local, sems, near, near_sems, rows = scratch
        table[pl.ds(first_edge, edges), :] = zlo[...].astype(jnp.float32)
        table[pl.ds(first_edge + edges, edges), :] = zhi[...].astype(jnp.float32)
        sublane = lax.broadcasted_iota(jnp.int32, (GROUP, LANES), 0)
        masks = [sublane == k for k in range(GROUP)]
        used = lax.broadcasted_iota(jnp.int32, (GROUP, LANES), 1) < coeffs

        def fetch(n, slot):
            return pltpu.make_async_copy(
                index.at[pl.ds(pl.multiple_of(n * CHUNK, CHUNK), CHUNK)],
                local.at[slot],
                sems.at[slot],
            )

        def stream(n, slot):
            return pltpu.make_async_copy(
                wide.at[pl.ds(pl.multiple_of(n * CHUNK, CHUNK), CHUNK), :],
                near.at[slot],
                near_sems.at[slot],
            )

        for b in range(RING - 1):
            fetch(b, b).start()
        for b in range(STREAM - 1):
            stream(b, b).start()

        def body(i, _):
            for b in range(RING):
                n = i * RING + b
                slot = n % STREAM
                fetch(n, b).wait()
                stream(n, slot).wait()
                ahead = n + RING - 1
                later = n + STREAM - 1

                @pl.when(ahead < chunks)
                def _():
                    fetch(ahead, (b + RING - 1) % RING).start()

                @pl.when(later < chunks)
                def _():
                    stream(later, later % STREAM).start()

                for q in range(groups):
                    total = None
                    for s in range(SAMPLES):
                        merged = None
                        for k in range(GROUP):
                            place = s * per_chunk + q * GROUP + k
                            row = table[pl.ds(local[b, place], GROUP, stride=0), :]
                            merged = row if merged is None else jnp.where(masks[k], row, merged)
                        at = (q * SAMPLES + s) * GROUP
                        term = merged * near[slot, at : at + GROUP, :]
                        total = term if total is None else total + term
                    to = pl.multiple_of((n * (groups // 4) + q // 4) * GROUP, GROUP)
                    rows[q % 4, pl.ds(to, GROUP), :] = jnp.where(used, total, 0.0)
            return 0

        lax.fori_loop(0, chunks // RING, body, 0)

        def pack(i, _):
            at = pl.multiple_of(i * 128, 128)
            part = [rows[q, pl.ds(at, 128), :].astype(jnp.bfloat16) for q in range(4)]
            outer = [jnp.concatenate([part[0], part[2]], axis=1)]
            outer.append(jnp.concatenate([part[1], part[3]], axis=1))
            first = jnp.dot(outer[0], pick[0], preferred_element_type=jnp.float32)
            second = jnp.dot(outer[1], pick[0], preferred_element_type=jnp.float32)
            third = jnp.dot(outer[0], pick[1], preferred_element_type=jnp.float32)
            third += jnp.dot(outer[1], pick[2], preferred_element_type=jnp.float32)
            for d in range(128 // GROUP):
                here = slice(d * GROUP, (d + 1) * GROUP)
                out[i * (128 // GROUP) + d, :16, :] = jnp.concatenate(
                    [first[here], second[here]], axis=0
                ).astype(jnp.bfloat16)
                out[i * (128 // GROUP) + d, 16:, :] = third[here].astype(jnp.bfloat16)
            return 0

        lax.fori_loop(0, pairs * GROUP // 128, pack, 0)

    pick = np.zeros((3, 2 * LANES, LANES), np.float32)
    for c in range(half):
        pick[0, c, c] = 1.0
        pick[0, LANES + c, half + c] = 1.0
    for c in range(32):
        pick[1, half + c, c] = 1.0
        pick[1, LANES + half + c, 64 + c] = 1.0
        pick[2, half + c, 32 + c] = 1.0
        pick[2, LANES + half + c, 96 + c] = 1.0
    vmem = pl.BlockSpec(memory_space=pltpu.VMEM)
    return pl.pallas_call(
        kernel,
        out_shape=(
            pltpu.VMEM(table.shape, jnp.float32),
            jax.ShapeDtypeStruct((pairs, 24, LANES), jnp.bfloat16),
        ),
        in_specs=[vmem] * 4 + [pl.BlockSpec(memory_space=pl.ANY), vmem],
        out_specs=(vmem, vmem),
        scratch_shapes=[
            pltpu.SMEM((RING, CHUNK), jnp.int32),
            pltpu.SemaphoreType.DMA((RING,)),
            pltpu.VMEM((STREAM, CHUNK, LANES), jnp.float32),
            pltpu.SemaphoreType.DMA((STREAM,)),
            pltpu.VMEM((4, pairs * GROUP, LANES), jnp.float32),
        ],
        input_output_aliases={5: 0},
        compiler_params=pltpu.CompilerParams(vmem_limit_bytes=24 * MIB),
        cost_estimate=pl.CostEstimate(
            flops=4 * 10**10, transcendentals=0, bytes_accessed=2 * 10**7
        ),
        name="gather_rows",
    )(index, zlo, zhi, jnp.asarray(pick.astype(jnp.bfloat16)), wide, table)[1]


def relight(transfer, routed, basis, projector):
    coeffs, count = transfer.shape
    sources, packed, _ = routed.shape
    per_pair = count // sources
    block = 512
    step = block // per_pair

    def kernel(transfer, routed, basis, wide, projector, out):
        low = lax.broadcasted_iota(jnp.int32, (GROUP, LANES), 1) < 64
        parts = []
        for i in range(step):
            head = routed[i, :16, :].astype(jnp.float32)
            first, second = head[:GROUP], head[GROUP:]
            third = routed[i, 16:, :].astype(jnp.float32)
            parts += [
                jnp.where(low, first, pltpu.roll(third, 64, 1)),
                jnp.where(low, second, pltpu.roll(third, 32, 1)),
                jnp.where(low, pltpu.roll(first, 64, 1), third),
                jnp.where(low, pltpu.roll(second, 64, 1), pltpu.roll(third, 96, 1)),
            ]
        rows = jnp.concatenate(parts, axis=0).astype(jnp.bfloat16)
        lit = jnp.dot(basis[...], transfer[...], preferred_element_type=jnp.float32)
        shade = lax.dot_general(
            wide[...], rows, (((1,), (1,)), ((), ())), preferred_element_type=jnp.float32
        )
        product = (lit * shade).astype(jnp.bfloat16)
        out[...] = jnp.dot(projector[...], product, preferred_element_type=jnp.float32).astype(
            jnp.bfloat16
        )

    directions = basis.shape[0]
    wide = np.zeros((directions, LANES), jnp.bfloat16)
    wide[:, :coeffs] = basis
    return pl.pallas_call(
        kernel,
        out_shape=jax.ShapeDtypeStruct((coeffs, count), jnp.bfloat16),
        grid=(count // block,),
        in_specs=[
            pl.BlockSpec((coeffs, block), lambda i: (0, i)),
            pl.BlockSpec((step, packed, LANES), lambda i: (i, 0, 0)),
            pl.BlockSpec((directions, coeffs), lambda i: (0, 0)),
            pl.BlockSpec((directions, LANES), lambda i: (0, 0)),
            pl.BlockSpec((coeffs, directions), lambda i: (0, 0)),
        ],
        out_specs=pl.BlockSpec((coeffs, block), lambda i: (0, i)),
        compiler_params=pltpu.CompilerParams(vmem_limit_bytes=40 * MIB),
        name="relight",
    )(transfer, routed, jnp.asarray(basis), jnp.asarray(wide), jnp.asarray(projector))


def moves(sizes, steps):
    pairs = []
    for x in range(sizes[0]):
        for y in range(sizes[1]):
            to_x, to_y = (x + steps[0]) % sizes[0], (y + steps[1]) % sizes[1]
            pairs.append((x * sizes[1] + y, to_x * sizes[1] + to_y))
    return pairs


def halo_step(field, samples, weights, destination, transfer):
    basis, projector = direction_tables()
    coeffs, cells_x, cells_y, cells_z = field.shape
    count = transfer.shape[1]
    along = tuple(lax.axis_size(axis) for axis in ("gx", "gy", "gz"))
    ups = [moves((n, 1), (1, 0)) for n in along]
    downs = [moves((n, 1), (-1, 0)) for n in along]

    field = pltpu.with_memory_space_constraint(field, pltpu.HBM)
    last, first, top, bottom = cut_faces(field)
    ylo = lax.ppermute(top, "gy", ups[1])
    yhi = lax.ppermute(bottom, "gy", downs[1])
    xlo = lax.ppermute(last, "gx", ups[0])
    xhi = lax.ppermute(first, "gx", downs[0])
    eye = jnp.asarray(np.eye(cells_z, dtype=np.float32).astype(jnp.bfloat16))
    own = own_table(field, eye)
    ylo, yhi, own = lax.optimization_barrier((ylo, yhi, own))
    ends = cut_corners(ylo, yhi)
    corners = [lax.ppermute(ends[0], "gx", ups[0]), lax.ppermute(ends[1], "gx", downs[0])]

    lines = cells_x * cells_y + (2 * HALO + 3) * cells_y
    rows = lines * cells_z
    cells = (cells_x, cells_y, cells_z)
    total = tuple(c * n for c, n in zip(cells, along))
    origin = jnp.stack(
        [lax.axis_index(axis) * c for axis, c in zip(("gx", "gy", "gz"), cells)]
    ).astype(jnp.int32)
    devices = math.prod(along)
    per_pair = count // devices
    slot = destination[0] * per_pair + destination[1]

    index, ordered = prepare(samples, weights, slot, origin, cells, total)
    wide = spread_weights(ordered)
    own, index, wide = lax.optimization_barrier((own, index, wide))
    table, edge_lo, edge_hi = full_table(
        own, xlo, xhi, ylo, yhi, corners, eye, rows + 2 * HALO * lines
    )
    zhi = lax.ppermute(edge_lo, "gz", downs[2])
    zlo = lax.ppermute(edge_hi, "gz", ups[2])
    outgoing = gather_rows(index.reshape(-1), wide, table, zlo, zhi, rows, count, coeffs)
    routed = lax.all_to_all(
        outgoing, ("gx", "gy", "gz"), split_axis=0, concat_axis=0, tiled=True
    )
    return relight(transfer, routed, basis, projector)


def solution(mesh):
    placed = (
        P(None, "gx", "gy", "gz"),
        P(None, None, ("gx", "gy", "gz")),
        P(None, ("gx", "gy", "gz")),
        P(None, ("gx", "gy", "gz")),
        P(None, ("gx", "gy", "gz")),
    )
    return jax.shard_map(
        halo_step,
        mesh=mesh,
        in_specs=placed,
        out_specs=P(None, ("gx", "gy", "gz")),
        check_vma=False,
    )
```

```python
import math

import jax
import jax.numpy as jnp
import numpy as np
from jax import lax
from jax.experimental import pallas as pl
from jax.experimental.pallas import tpu as pltpu
from jax.sharding import PartitionSpec as P


HALO = 2
SAMPLES = 8
DEGREES = 9
POLAR = 32
AZIMUTH = 32
LANES = 128
MIB = 1024 * 1024


def harmonic_values():
    polar = (np.arange(POLAR, dtype=np.float64) + 0.5) * (2.0 / POLAR) - 1.0
    beside = (np.arange(AZIMUTH, dtype=np.float64) + 0.5) * (2.0 * math.pi / AZIMUTH)
    cosines = np.repeat(polar, AZIMUTH)
    angles = np.tile(beside, POLAR)
    sines = np.sqrt(np.maximum(1.0 - cosines * cosines, 0.0))
    entries = {}
    for m in range(DEGREES):
        diagonal = (-1.0) ** m * float(math.prod(range(1, 2 * m, 2))) * sines**m
        legendre = {m: diagonal}
        if m + 1 < DEGREES:
            legendre[m + 1] = cosines * (2 * m + 1) * diagonal
        for l in range(m + 2, DEGREES):
            legendre[l] = (
                (2 * l - 1) * cosines * legendre[l - 1] - (l + m - 1) * legendre[l - 2]
            ) / (l - m)
        for l in range(m, DEGREES):
            factor = math.sqrt(
                (2 * l + 1) / (4.0 * math.pi) * math.factorial(l - m) / math.factorial(l + m)
            )
            if m == 0:
                entries[l, 0] = factor * legendre[l]
            else:
                entries[l, m] = math.sqrt(2.0) * factor * np.cos(m * angles) * legendre[l]
                entries[l, -m] = math.sqrt(2.0) * factor * np.sin(m * angles) * legendre[l]
    return np.stack([entries[l, m] for l in range(DEGREES) for m in range(-l, l + 1)])


def direction_tables():
    values = harmonic_values()
    basis = values.T.astype(np.float32).astype(jnp.bfloat16)
    projector = (values * (4.0 * math.pi / (POLAR * AZIMUTH))).astype(np.float32)
    return basis, projector.astype(jnp.bfloat16)


def fill_rows(get, spread, coeffs, rows_y, cells_z):
    halves = cells_z // LANES
    for c in range(coeffs):
        for h in range(halves):
            block = get(c, h).astype(jnp.float32)
            spread[h, pl.ds(c, rows_y, stride=coeffs), :] = block


def turn_rows(spread, eye, coeffs, rows_y, cells_z, put):
    halves = cells_z // LANES
    keep = -(-coeffs // 16) * 16
    zeros = jnp.zeros((LANES - keep, cells_z), jnp.bfloat16)
    for y in range(0, rows_y, 2):
        parts = []
        for i in (y, y + 1):
            rows = jnp.concatenate(
                [spread[h, i * coeffs : i * coeffs + keep, :] for h in range(halves)], axis=1
            )
            parts += [rows.astype(jnp.bfloat16), zeros]
        both = lax.dot_general(
            eye[...],
            jnp.concatenate(parts, axis=0),
            (((1,), (1,)), ((), ())),
            preferred_element_type=jnp.float32,
        )
        put(y, both[:, :LANES])
        put(y + 1, both[:, LANES:])


def spread_shape(coeffs, cells_y, cells_z):
    return pltpu.VMEM((cells_z // LANES, cells_y * coeffs + 16, LANES), jnp.float32)


def cut_x(field):
    coeffs, cells_x, cells_y, cells_z = field.shape

    def kernel(field, last, first, sems):
        copies = [
            pltpu.make_async_copy(field.at[:, pl.ds(cells_x - HALO, HALO)], last, sems.at[0]),
            pltpu.make_async_copy(field.at[:, pl.ds(0, HALO)], first, sems.at[1]),
        ]
        for copy in copies:
            copy.start()
        for copy in copies:
            copy.wait()

    hbm = pl.BlockSpec(memory_space=pl.ANY)
    return pl.pallas_call(
        kernel,
        out_shape=[pltpu.HBM((coeffs, HALO, cells_y, cells_z), jnp.bfloat16)] * 2,
        in_specs=[hbm],
        out_specs=[hbm, hbm],
        scratch_shapes=[pltpu.SemaphoreType.DMA((2,))],
        compiler_params=pltpu.CompilerParams(vmem_limit_bytes=4 * MIB),
        name="cut_x",
    )(field)


def cut_y(field):
    coeffs, cells_x, cells_y, cells_z = field.shape
    per_step = 9
    rows = cells_x * HALO

    def kernel(field, pick, top, bottom):
        for c in range(per_step):
            chosen = jnp.dot(
                pick[...],
                field[c].reshape(cells_x * cells_y, cells_z),
                preferred_element_type=jnp.float32,
            ).astype(jnp.bfloat16)
            top[c] = chosen[:rows]
            bottom[c] = chosen[rows:]

    pick = np.zeros((2 * rows, cells_x * cells_y), np.float32)
    for x in range(cells_x):
        for j in range(HALO):
            pick[x * HALO + j, x * cells_y + cells_y - HALO + j] = 1.0
            pick[rows + x * HALO + j, x * cells_y + j] = 1.0
    face = pl.BlockSpec((per_step, rows, cells_z), lambda i: (i, 0, 0))
    return pl.pallas_call(
        kernel,
        out_shape=[pltpu.HBM((coeffs, rows, cells_z), jnp.bfloat16)] * 2,
        grid=(coeffs // per_step,),
        in_specs=[
            pl.BlockSpec((per_step, cells_x, cells_y, cells_z), lambda i: (i, 0, 0, 0)),
            pl.BlockSpec(pick.shape, lambda i: (0, 0)),
        ],
        out_specs=[face, face],
        compiler_params=pltpu.CompilerParams(vmem_limit_bytes=16 * MIB),
        name="cut_y",
    )(field, jnp.asarray(pick.astype(jnp.bfloat16)))


def cut_corners(ylo, yhi):
    coeffs, rows, cells_z = ylo.shape
    per_step = 27
    corner = HALO * HALO

    def kernel(ylo, yhi, pick, up, down):
        for c in range(per_step):
            chosen = jnp.dot(
                pick[...],
                jnp.concatenate([ylo[c], yhi[c]], axis=0),
                preferred_element_type=jnp.float32,
            )
            up[c] = chosen[: 2 * corner].astype(jnp.bfloat16)
            down[c] = chosen[2 * corner :].astype(jnp.bfloat16)

    pick = np.zeros((4 * corner, 2 * rows), np.float32)
    for side in range(2):
        for i in range(corner):
            pick[side * corner + i, side * rows + rows - corner + i] = 1.0
            pick[2 * corner + side * corner + i, side * rows + i] = 1.0
    shape = (coeffs, 2 * corner, cells_z)
    face = pl.BlockSpec((per_step, rows, cells_z), lambda i: (i, 0, 0))
    piece = pl.BlockSpec((per_step,) + shape[1:], lambda i: (i, 0, 0))
    return pl.pallas_call(
        kernel,
        out_shape=[pltpu.HBM(shape, jnp.bfloat16)] * 2,
        grid=(coeffs // per_step,),
        in_specs=[face, face, pl.BlockSpec(pick.shape, lambda i: (0, 0))],
        out_specs=[piece, piece],
        compiler_params=pltpu.CompilerParams(vmem_limit_bytes=16 * MIB),
        name="cut_corners",
    )(ylo, yhi, jnp.asarray(pick.astype(jnp.bfloat16)))


def add_planes(table, planes, halves, eye, first_plane, total_rows, edge_lines):
    source = planes[0][0]
    coeffs, cells_y, cells_z = source.shape[0], source.shape[-2], source.shape[-1]
    count = len(planes)
    arrays = []
    for array, _ in planes:
        if not any(array is other for other in arrays):
            arrays.append(array)
    places = [next(i for i, o in enumerate(arrays) if o is array) for array, _ in planes]
    new = table is None

    def kernel(*refs):
        refs = list(refs)
        if not new:
            refs.pop(0)
        inputs = [refs.pop(0) for _ in arrays]
        shared = [refs.pop(0) for _ in halves]
        eye = refs.pop(0)
        table = refs.pop(0)
        edges = [refs.pop(0) for _ in range(2)] if edge_lines else []
        buf, sems, spread = refs[:3]
        copies = []
        for p, ((_, at), place) in enumerate(zip(planes, places)):
            ref = inputs[place] if at is None else inputs[place].at[:, at]
            copies.append(pltpu.make_async_copy(ref, buf.at[p], sems.at[p]))
        for q, piece in enumerate(shared):
            copies.append(pltpu.make_async_copy(piece, refs[3].at[q], refs[4].at[q]))
        for copy in copies:
            copy.start()

        def turn(p):
            def put(y, block):
                at = pl.multiple_of(((first_plane + p) * cells_y + y) * cells_z, 8)
                table[pl.ds(at, cells_z), :] = block

            turn_rows(spread, eye, coeffs, cells_y, cells_z, put)

        def one(p, _):
            first = inputs[0] if planes[0][1] is None else inputs[0].at[:, 0]
            pltpu.make_async_copy(first, buf.at[p], sems.at[p]).wait()
            fill_rows(
                lambda c, h: buf[p, c, :, h * LANES : (h + 1) * LANES],
                spread,
                coeffs,
                cells_y,
                cells_z,
            )
            turn(p)
            return 0

        lax.fori_loop(0, count, one, 0)
        if halves:
            for copy in copies[count:]:
                copy.wait()
            fill_rows(
                lambda c, h: jnp.concatenate(
                    [
                        refs[3][q, c, :, h * LANES : (h + 1) * LANES].astype(jnp.float32)
                        for q in range(2)
                    ],
                    axis=0,
                ),
                spread,
                coeffs,
                cells_y,
                cells_z,
            )
            turn(count)
        for out, start in zip(edges, (0, cells_z - HALO)):
            for j in range(HALO):
                for line in range(0, edge_lines, 16):
                    parts = [
                        table[pl.ds((line + i) * cells_z + start + j, 8, stride=cells_z), :]
                        for i in (0, 8)
                    ]
                    at = j * edge_lines + line
                    out[at : at + 16, :] = jnp.concatenate(parts, axis=0).astype(jnp.bfloat16)

    vmem = pl.BlockSpec(memory_space=pltpu.VMEM)
    hbm = pl.BlockSpec(memory_space=pl.ANY)
    shapes = [pltpu.VMEM((total_rows, LANES), jnp.float32)]
    if edge_lines:
        shapes += [jax.ShapeDtypeStruct((HALO * edge_lines, LANES), jnp.bfloat16)] * 2
    scratch = [
        pltpu.VMEM((count, coeffs, cells_y, cells_z), jnp.bfloat16),
        pltpu.SemaphoreType.DMA((count,)),
        spread_shape(coeffs, cells_y, cells_z),
    ]
    if halves:
        scratch += [
            pltpu.VMEM((2, coeffs, cells_y // 2, cells_z), jnp.bfloat16),
            pltpu.SemaphoreType.DMA((2,)),
        ]
    held = [] if new else [table]
    return pl.pallas_call(
        kernel,
        out_shape=shapes,
        in_specs=[vmem] * len(held) + [hbm] * (len(arrays) + len(halves)) + [vmem],
        out_specs=[vmem] * len(shapes),
        scratch_shapes=scratch,
        input_output_aliases={} if new else {0: 0},
        compiler_params=pltpu.CompilerParams(vmem_limit_bytes=TABLE_LIMIT * MIB),
        cost_estimate=pl.CostEstimate(
            flops=2 * 10**10, transcendentals=0, bytes_accessed=2 * 10**7
        ),
    )(*held, *arrays, *halves, eye)


def cut_ends(zlo, zhi, lines, cells_x, cells_y):
    own = cells_x * cells_y
    half = HALO * cells_y + 2 * HALO * HALO
    rows = 2 * HALO * half

    def kernel(zlo, zhi, pick, up, down):
        both = jnp.concatenate([zlo[...], zhi[...]], axis=0)
        chosen = jnp.dot(pick[...], both, preferred_element_type=jnp.float32)
        up[...] = chosen[:rows].astype(jnp.bfloat16)
        down[...] = chosen[rows:].astype(jnp.bfloat16)

    pick = np.zeros((2 * rows, 2 * HALO * lines), np.float32)
    for side in range(2):
        x = cells_x - HALO if side == 0 else 0
        places = [x * cells_y + i for i in range(HALO * cells_y)]
        for face in range(2):
            at = own + face * cells_y + x * HALO
            places += [at + i for i in range(HALO * HALO)]
        for z in range(2 * HALO):
            for i, place in enumerate(places):
                pick[side * rows + z * half + i, z * lines + place] = 1.0
    vmem = pl.BlockSpec(memory_space=pltpu.VMEM)
    return pl.pallas_call(
        kernel,
        out_shape=[jax.ShapeDtypeStruct((rows, LANES), jnp.bfloat16)] * 2,
        in_specs=[vmem] * 3,
        out_specs=[vmem] * 2,
        compiler_params=pltpu.CompilerParams(vmem_limit_bytes=8 * MIB),
        name="cut_ends",
    )(zlo, zhi, jnp.asarray(pick.astype(jnp.bfloat16)))


TABLE_LIMIT = 24
GROUP = 8
PARTS = 3


def prepare(samples, weights, slot, origin, cells, total):
    count = slot.shape[0]
    cells_x, cells_y, cells_z = cells
    own_lines = cells_x * cells_y
    early = own_lines + 2 * cells_y
    rows = (early + (2 * HALO + 1) * cells_y) * cells_z
    block = 256
    burst = 32
    kinds = (2 + PARTS) * SAMPLES
    corner = HALO * HALO
    end = HALO * cells_y + 2 * corner

    def locate(near_x, near_y, near_z):
        own_x = (near_x >= HALO) & (near_x < HALO + cells_x)
        own_y = (near_y >= HALO) & (near_y < HALO + cells_y)
        low_x = near_x < HALO
        low_y = near_y < HALO
        side_x = jnp.where(low_x, near_x, near_x - HALO - cells_x)
        side_y = jnp.where(low_y, near_y, near_y - HALO - cells_y)
        line_own = (near_x - HALO) * cells_y + near_y - HALO
        line_y = own_lines + jnp.where(low_y, 0, cells_y) + (near_x - HALO) * HALO + side_y
        line_early = jnp.where(own_y, line_own, line_y)
        in_face = side_x * cells_y + near_y - HALO
        in_corner = jnp.where(low_y, 0, corner) + side_x * HALO + side_y
        line_late = early + jnp.where(
            own_y,
            jnp.where(low_x, 0, HALO * cells_y) + in_face,
            2 * HALO * cells_y + jnp.where(low_x, 0, 2 * corner) + in_corner,
        )
        line = jnp.where(own_x, line_early, line_late)
        edge = jnp.where(near_z < HALO, near_z, near_z - cells_z)
        at_end = jnp.where(own_y, in_face, HALO * cells_y + in_corner)
        beyond = jnp.where(
            own_x,
            edge * early + line_early,
            2 * HALO * early + jnp.where(low_x, 0, 2 * HALO * end) + edge * end + at_end,
        )
        inside = (near_z >= HALO) & (near_z < HALO + cells_z)
        return jnp.where(inside, line * cells_z + near_z - HALO, rows + beyond)

    def kernel(origin, slot, samples, weights, eye, join, index, ordered, natural):
        def turn(j, _):
            at = pl.multiple_of(j * block, block)
            near = []
            for d in range(3):
                shift = samples[d, :, pl.ds(at, block)] - origin[d] + HALO
                shift = jnp.where(shift < 0, shift + total[d], shift)
                near.append(jnp.where(shift >= total[d], shift - total[d], shift))
            row = locate(*near)
            pieces = [(row >> 8).astype(jnp.float32), (row & 255).astype(jnp.float32)]
            rest = weights[:, pl.ds(at, block)]
            for _ in range(PARTS):
                piece = rest.astype(jnp.bfloat16).astype(jnp.float32)
                pieces.append(piece)
                rest = rest - piece
            pieces.append(jnp.zeros((LANES - kinds, block), jnp.float32))
            natural[pl.ds(at, block), :] = lax.dot_general(
                eye[...],
                jnp.concatenate(pieces, axis=0).astype(jnp.bfloat16),
                (((1,), (1,)), ((), ())),
                preferred_element_type=jnp.float32,
            )
            return 0

        lax.fori_loop(0, count // block, turn, 0)

        def scatter(j, _):
            at = pl.multiple_of(j * burst, burst)
            mine = slot.at[pl.ds(at, burst)]
            for g in range(0, burst, GROUP):
                tile = natural[pl.ds(at + g, GROUP), :]
                for k in range(GROUP):
                    ordered[pl.ds(mine[g + k], 1), :] = tile[k : k + 1, :]
            return 0

        lax.fori_loop(0, count // burst, scatter, 0)

        def collect(j, _):
            at = pl.multiple_of(j * 4 * LANES, 4 * LANES)
            wide = lax.dot_general(
                join[...],
                ordered[pl.ds(at, 4 * LANES), :].astype(jnp.bfloat16),
                (((1,), (1,)), ((), ())),
                preferred_element_type=jnp.float32,
            ).astype(jnp.int32)
            for i in range(4):
                to = pl.multiple_of((j * 4 + i) * SAMPLES, SAMPLES)
                index[pl.ds(to, SAMPLES), :] = wide[:SAMPLES, i * LANES : (i + 1) * LANES]
            return 0

        lax.fori_loop(0, count // (4 * LANES), collect, 0)

    join = np.zeros((16, LANES), np.float32)
    for s in range(SAMPLES):
        join[s, s] = 256.0
        join[s, SAMPLES + s] = 1.0
    vmem = pl.BlockSpec(memory_space=pltpu.VMEM)
    smem = pl.BlockSpec(memory_space=pltpu.SMEM)
    return pl.pallas_call(
        kernel,
        out_shape=(
            jax.ShapeDtypeStruct((count * SAMPLES // LANES, LANES), jnp.int32),
            jax.ShapeDtypeStruct((count, LANES), jnp.float32),
        ),
        in_specs=[smem, smem, vmem, vmem, vmem, vmem],
        out_specs=(vmem, vmem),
        scratch_shapes=[pltpu.VMEM((count, LANES), jnp.float32)],
        compiler_params=pltpu.CompilerParams(vmem_limit_bytes=12 * MIB),
        cost_estimate=pl.CostEstimate(
            flops=2 * 10**10, transcendentals=0, bytes_accessed=3 * 10**6
        ),
        name="prepare",
    )(
        origin,
        slot,
        samples,
        weights,
        jnp.asarray(np.eye(block, dtype=np.float32).astype(jnp.bfloat16)),
        jnp.asarray(join.astype(jnp.bfloat16)),
    )


RING = 2
CHUNK = 1024


def gather_rows(index, ordered, table, edges, first_edge, coeffs):
    count = ordered.shape[0]
    chunks = index.shape[0] // CHUNK
    per_chunk = CHUNK // SAMPLES
    groups = per_chunk // GROUP
    pairs = count // 32
    half = LANES // 2

    def kernel(index, ordered, ones, pick, *refs):
        table, out, local, sems, near, rows = refs[len(edges) + 1 :]
        at = first_edge
        for edge in refs[: len(edges)]:
            table[pl.ds(at, edge.shape[0]), :] = edge[...].astype(jnp.float32)
            at += edge.shape[0]
        sublane = lax.broadcasted_iota(jnp.int32, (GROUP, LANES), 0)
        masks = [sublane == k for k in range(GROUP)]
        used = lax.broadcasted_iota(jnp.int32, (GROUP, LANES), 1) < coeffs

        def fetch(n, slot):
            return pltpu.make_async_copy(
                index.at[pl.ds(pl.multiple_of(n * CHUNK, CHUNK), CHUNK)],
                local.at[slot],
                sems.at[slot],
            )

        def spread(n, slot):
            at = pl.multiple_of(n * per_chunk, per_chunk)
            parts = ordered[pl.ds(at, per_chunk), :].astype(jnp.bfloat16)
            for h in range(0, SAMPLES, 2):
                both = jnp.dot(
                    parts, ones[:, h * LANES : (h + 2) * LANES], preferred_element_type=jnp.float32
                )
                for s in range(2):
                    for q in range(groups):
                        to = (q * SAMPLES + h + s) * GROUP
                        near[slot, to : to + GROUP, :] = both[
                            q * GROUP : (q + 1) * GROUP, s * LANES : (s + 1) * LANES
                        ]

        for b in range(RING - 1):
            fetch(b, b).start()
        spread(0, 0)

        def body(i, _):
            for b in range(RING):
                n = i * RING + b
                fetch(n, b).wait()
                ahead = n + RING - 1

                @pl.when(ahead < chunks)
                def _():
                    fetch(ahead, (b + RING - 1) % RING).start()

                spread(jnp.minimum(n + 1, chunks - 1), 1 - b)

                for q in range(groups):
                    total = None
                    for s in range(SAMPLES):
                        merged = None
                        for k in range(GROUP):
                            place = s * per_chunk + q * GROUP + k
                            row = table[pl.ds(local[b, place], GROUP, stride=0), :]
                            merged = row if merged is None else jnp.where(masks[k], row, merged)
                        at = (q * SAMPLES + s) * GROUP
                        term = merged * near[b, at : at + GROUP, :]
                        total = term if total is None else total + term
                    to = pl.multiple_of((n * (groups // 4) + q // 4) * GROUP, GROUP)
                    rows[q % 4, pl.ds(to, GROUP), :] = jnp.where(used, total, 0.0)
            return 0

        lax.fori_loop(0, chunks // RING, body, 0)

        def pack(i, _):
            at = pl.multiple_of(i * 128, 128)
            part = [rows[q, pl.ds(at, 128), :].astype(jnp.bfloat16) for q in range(4)]
            outer = [jnp.concatenate([part[0], part[2]], axis=1)]
            outer.append(jnp.concatenate([part[1], part[3]], axis=1))
            first = jnp.dot(outer[0], pick[0], preferred_element_type=jnp.float32)
            second = jnp.dot(outer[1], pick[0], preferred_element_type=jnp.float32)
            third = jnp.dot(outer[0], pick[1], preferred_element_type=jnp.float32)
            third += jnp.dot(outer[1], pick[2], preferred_element_type=jnp.float32)
            for d in range(128 // GROUP):
                here = slice(d * GROUP, (d + 1) * GROUP)
                out[i * (128 // GROUP) + d, :16, :] = jnp.concatenate(
                    [first[here], second[here]], axis=0
                ).astype(jnp.bfloat16)
                out[i * (128 // GROUP) + d, 16:, :] = third[here].astype(jnp.bfloat16)
            return 0

        lax.fori_loop(0, pairs * GROUP // 128, pack, 0)

    ones = np.zeros((LANES, SAMPLES * LANES), np.float32)
    for s in range(SAMPLES):
        for p in range(PARTS):
            ones[(2 + p) * SAMPLES + s, s * LANES : (s + 1) * LANES] = 1.0
    pick = np.zeros((3, 2 * LANES, LANES), np.float32)
    for c in range(half):
        pick[0, c, c] = 1.0
        pick[0, LANES + c, half + c] = 1.0
    for c in range(32):
        pick[1, half + c, c] = 1.0
        pick[1, LANES + half + c, 64 + c] = 1.0
        pick[2, half + c, 32 + c] = 1.0
        pick[2, LANES + half + c, 96 + c] = 1.0
    vmem = pl.BlockSpec(memory_space=pltpu.VMEM)
    return pl.pallas_call(
        kernel,
        out_shape=(
            pltpu.VMEM(table.shape, jnp.float32),
            jax.ShapeDtypeStruct((pairs, 24, LANES), jnp.bfloat16),
        ),
        in_specs=[vmem] * (5 + len(edges)),
        out_specs=(vmem, vmem),
        scratch_shapes=[
            pltpu.SMEM((RING, CHUNK), jnp.int32),
            pltpu.SemaphoreType.DMA((RING,)),
            pltpu.VMEM((RING, CHUNK, LANES), jnp.float32),
            pltpu.VMEM((4, pairs * GROUP, LANES), jnp.float32),
        ],
        input_output_aliases={4 + len(edges): 0},
        compiler_params=pltpu.CompilerParams(vmem_limit_bytes=24 * MIB),
        cost_estimate=pl.CostEstimate(
            flops=4 * 10**10, transcendentals=0, bytes_accessed=2 * 10**7
        ),
        name="gather_rows",
    )(
        index,
        ordered,
        jnp.asarray(ones.astype(jnp.bfloat16)),
        jnp.asarray(pick.astype(jnp.bfloat16)),
        *edges,
        table,
    )[1]


def relight(transfer, routed, basis, projector):
    coeffs, count = transfer.shape
    sources, packed, _ = routed.shape
    per_pair = count // sources
    block = 512
    step = block // per_pair

    def kernel(transfer, routed, basis, wide, projector, out):
        low = lax.broadcasted_iota(jnp.int32, (GROUP, LANES), 1) < 64
        parts = []
        for i in range(step):
            head = routed[i, :16, :].astype(jnp.float32)
            first, second = head[:GROUP], head[GROUP:]
            third = routed[i, 16:, :].astype(jnp.float32)
            parts += [
                jnp.where(low, first, pltpu.roll(third, 64, 1)),
                jnp.where(low, second, pltpu.roll(third, 32, 1)),
                jnp.where(low, pltpu.roll(first, 64, 1), third),
                jnp.where(low, pltpu.roll(second, 64, 1), pltpu.roll(third, 96, 1)),
            ]
        rows = jnp.concatenate(parts, axis=0).astype(jnp.bfloat16)
        lit = jnp.dot(basis[...], transfer[...], preferred_element_type=jnp.float32)
        shade = lax.dot_general(
            wide[...], rows, (((1,), (1,)), ((), ())), preferred_element_type=jnp.float32
        )
        product = (lit * shade).astype(jnp.bfloat16)
        out[...] = jnp.dot(projector[...], product, preferred_element_type=jnp.float32).astype(
            jnp.bfloat16
        )

    directions = basis.shape[0]
    wide = np.zeros((directions, LANES), jnp.bfloat16)
    wide[:, :coeffs] = basis
    return pl.pallas_call(
        kernel,
        out_shape=jax.ShapeDtypeStruct((coeffs, count), jnp.bfloat16),
        grid=(count // block,),
        in_specs=[
            pl.BlockSpec((coeffs, block), lambda i: (0, i)),
            pl.BlockSpec((step, packed, LANES), lambda i: (i, 0, 0)),
            pl.BlockSpec((directions, coeffs), lambda i: (0, 0)),
            pl.BlockSpec((directions, LANES), lambda i: (0, 0)),
            pl.BlockSpec((coeffs, directions), lambda i: (0, 0)),
        ],
        out_specs=pl.BlockSpec((coeffs, block), lambda i: (0, i)),
        compiler_params=pltpu.CompilerParams(vmem_limit_bytes=40 * MIB),
        name="relight",
    )(transfer, routed, jnp.asarray(basis), jnp.asarray(wide), jnp.asarray(projector))


def moves(sizes, steps):
    pairs = []
    for x in range(sizes[0]):
        for y in range(sizes[1]):
            to_x, to_y = (x + steps[0]) % sizes[0], (y + steps[1]) % sizes[1]
            pairs.append((x * sizes[1] + y, to_x * sizes[1] + to_y))
    return pairs


def halo_step(field, samples, weights, destination, transfer):
    basis, projector = direction_tables()
    coeffs, cells_x, cells_y, cells_z = field.shape
    count = transfer.shape[1]
    along = tuple(lax.axis_size(axis) for axis in ("gx", "gy", "gz"))
    ups = [moves((n, 1), (1, 0)) for n in along]
    downs = [moves((n, 1), (-1, 0)) for n in along]

    cells = (cells_x, cells_y, cells_z)
    total = tuple(c * n for c, n in zip(cells, along))
    origin = jnp.stack(
        [lax.axis_index(axis) * c for axis, c in zip(("gx", "gy", "gz"), cells)]
    ).astype(jnp.int32)
    devices = math.prod(along)
    per_pair = count // devices
    slot = destination[0] * per_pair + destination[1]

    field = pltpu.with_memory_space_constraint(field, pltpu.HBM)
    last, first = cut_x(field)
    xlo = lax.ppermute(last, "gx", ups[0])
    xhi = lax.ppermute(first, "gx", downs[0])
    top, bottom = cut_y(field)
    ylo = lax.ppermute(top, "gy", ups[1])
    yhi = lax.ppermute(bottom, "gy", downs[1])
    field, slot, origin = lax.optimization_barrier((field, slot, origin))

    eye = jnp.asarray(np.eye(cells_z, dtype=np.float32).astype(jnp.bfloat16))
    early = (cells_x + 2) * cells_y
    rows = (early + (2 * HALO + 1) * cells_y) * cells_z
    ends = HALO * cells_y + 2 * HALO * HALO
    total_rows = rows + 2 * HALO * (early + 2 * ends)
    own = [(field, x) for x in range(cells_x)]
    table = add_planes(None, own, (), eye, 0, total_rows, 0)[0]
    index, ordered = prepare(samples, weights, slot, origin, cells, total)
    table, index, ordered, ylo, yhi = lax.optimization_barrier((table, index, ordered, ylo, yhi))
    up, down = cut_corners(ylo, yhi)
    clo = lax.ppermute(up, "gx", ups[0])
    chi = lax.ppermute(down, "gx", downs[0])
    table, bottoms, tops = add_planes(
        table, [(ylo, None), (yhi, None)], (), eye, cells_x, total_rows, early
    )
    zhi = lax.ppermute(bottoms, "gz", downs[2])
    zlo = lax.ppermute(tops, "gz", ups[2])
    up, down = cut_ends(zlo, zhi, early, cells_x, cells_y)
    elo = lax.ppermute(up, "gx", ups[0])
    ehi = lax.ppermute(down, "gx", downs[0])
    sides = [(xlo, 0), (xlo, 1), (xhi, 0), (xhi, 1)]
    table = add_planes(table, sides, (clo, chi), eye, cells_x + 2, total_rows, 0)[0]
    outgoing = gather_rows(
        index.reshape(-1), ordered, table, (zlo, zhi, elo, ehi), rows, coeffs
    )
    routed = lax.all_to_all(
        outgoing, ("gx", "gy", "gz"), split_axis=0, concat_axis=0, tiled=True
    )
    return relight(transfer, routed, basis, projector)


def solution(mesh):
    placed = (
        P(None, "gx", "gy", "gz"),
        P(None, None, ("gx", "gy", "gz")),
        P(None, ("gx", "gy", "gz")),
        P(None, ("gx", "gy", "gz")),
        P(None, ("gx", "gy", "gz")),
    )
    return jax.shard_map(
        halo_step,
        mesh=mesh,
        in_specs=placed,
        out_specs=P(None, ("gx", "gy", "gz")),
        check_vma=False,
    )
```

```python
import math

import jax
import jax.numpy as jnp
import numpy as np
from jax import lax
from jax.experimental import pallas as pl
from jax.experimental.pallas import tpu as pltpu
from jax.sharding import PartitionSpec as P


HALO = 2
SAMPLES = 8
DEGREES = 9
POLAR = 32
AZIMUTH = 32
LANES = 128
MIB = 1024 * 1024


def harmonic_values():
    polar = (np.arange(POLAR, dtype=np.float64) + 0.5) * (2.0 / POLAR) - 1.0
    beside = (np.arange(AZIMUTH, dtype=np.float64) + 0.5) * (2.0 * math.pi / AZIMUTH)
    cosines = np.repeat(polar, AZIMUTH)
    angles = np.tile(beside, POLAR)
    sines = np.sqrt(np.maximum(1.0 - cosines * cosines, 0.0))
    entries = {}
    for m in range(DEGREES):
        diagonal = (-1.0) ** m * float(math.prod(range(1, 2 * m, 2))) * sines**m
        legendre = {m: diagonal}
        if m + 1 < DEGREES:
            legendre[m + 1] = cosines * (2 * m + 1) * diagonal
        for l in range(m + 2, DEGREES):
            legendre[l] = (
                (2 * l - 1) * cosines * legendre[l - 1] - (l + m - 1) * legendre[l - 2]
            ) / (l - m)
        for l in range(m, DEGREES):
            factor = math.sqrt(
                (2 * l + 1) / (4.0 * math.pi) * math.factorial(l - m) / math.factorial(l + m)
            )
            if m == 0:
                entries[l, 0] = factor * legendre[l]
            else:
                entries[l, m] = math.sqrt(2.0) * factor * np.cos(m * angles) * legendre[l]
                entries[l, -m] = math.sqrt(2.0) * factor * np.sin(m * angles) * legendre[l]
    return np.stack([entries[l, m] for l in range(DEGREES) for m in range(-l, l + 1)])


def direction_tables():
    values = harmonic_values()
    basis = values.T.astype(np.float32).astype(jnp.bfloat16)
    projector = (values * (4.0 * math.pi / (POLAR * AZIMUTH))).astype(np.float32)
    return basis, projector.astype(jnp.bfloat16)


def fill_rows(get, spread, coeffs, rows_y, cells_z):
    halves = cells_z // LANES
    for c in range(coeffs):
        for h in range(halves):
            block = get(c, h).astype(jnp.float32)
            spread[h, pl.ds(c, rows_y, stride=coeffs), :] = block


def turn_rows(spread, eye, coeffs, rows_y, cells_z, put):
    halves = cells_z // LANES
    keep = -(-coeffs // 16) * 16
    zeros = jnp.zeros((LANES - keep, cells_z), jnp.bfloat16)
    for y in range(0, rows_y, 2):
        parts = []
        for i in (y, y + 1):
            rows = jnp.concatenate(
                [spread[h, i * coeffs : i * coeffs + keep, :] for h in range(halves)], axis=1
            )
            parts += [rows.astype(jnp.bfloat16), zeros]
        both = lax.dot_general(
            eye[...],
            jnp.concatenate(parts, axis=0),
            (((1,), (1,)), ((), ())),
            preferred_element_type=jnp.float32,
        )
        put(y, both[:, :LANES])
        put(y + 1, both[:, LANES:])


def spread_shape(coeffs, cells_y, cells_z):
    return pltpu.VMEM((cells_z // LANES, cells_y * coeffs + 16, LANES), jnp.float32)


def cut_faces(field):
    coeffs, cells_x, cells_y, cells_z = field.shape
    per_step = 9
    rows = cells_x * HALO

    def kernel(field, pick, last, first, top, bottom):
        for c in range(per_step):
            last[c] = field[c, cells_x - HALO :]
            first[c] = field[c, :HALO]
            chosen = jnp.dot(
                pick[...],
                field[c].reshape(cells_x * cells_y, cells_z),
                preferred_element_type=jnp.float32,
            ).astype(jnp.bfloat16)
            top[c] = chosen[:rows]
            bottom[c] = chosen[rows:]

    pick = np.zeros((2 * rows, cells_x * cells_y), np.float32)
    for x in range(cells_x):
        for j in range(HALO):
            pick[x * HALO + j, x * cells_y + cells_y - HALO + j] = 1.0
            pick[rows + x * HALO + j, x * cells_y + j] = 1.0
    shapes = [(coeffs, HALO, cells_y, cells_z)] * 2
    shapes += [(coeffs, rows, cells_z)] * 2

    def whole(shape):
        zeros = (0,) * (len(shape) - 1)
        return pl.BlockSpec((per_step,) + shape[1:], lambda i: (i,) + zeros)

    return pl.pallas_call(
        kernel,
        out_shape=[pltpu.HBM(shape, jnp.bfloat16) for shape in shapes],
        grid=(coeffs // per_step,),
        in_specs=[whole(field.shape), pl.BlockSpec(pick.shape, lambda i: (0, 0))],
        out_specs=[whole(shape) for shape in shapes],
        compiler_params=pltpu.CompilerParams(vmem_limit_bytes=24 * MIB),
        name="cut_faces",
    )(field, jnp.asarray(pick.astype(jnp.bfloat16)))


def cut_corners(ylo, yhi):
    coeffs, rows, cells_z = ylo.shape
    per_step = 27
    corner = HALO * HALO

    def kernel(ylo, yhi, pick, up, down):
        for c in range(per_step):
            chosen = jnp.dot(
                pick[...],
                jnp.concatenate([ylo[c], yhi[c]], axis=0),
                preferred_element_type=jnp.float32,
            )
            up[c] = chosen[: 2 * corner].astype(jnp.bfloat16)
            down[c] = chosen[2 * corner :].astype(jnp.bfloat16)

    pick = np.zeros((4 * corner, 2 * rows), np.float32)
    for side in range(2):
        for i in range(corner):
            pick[side * corner + i, side * rows + rows - corner + i] = 1.0
            pick[2 * corner + side * corner + i, side * rows + i] = 1.0
    shape = (coeffs, 2 * corner, cells_z)
    face = pl.BlockSpec((per_step, rows, cells_z), lambda i: (i, 0, 0))
    piece = pl.BlockSpec((per_step,) + shape[1:], lambda i: (i, 0, 0))
    return pl.pallas_call(
        kernel,
        out_shape=[pltpu.HBM(shape, jnp.bfloat16)] * 2,
        grid=(coeffs // per_step,),
        in_specs=[face, face, pl.BlockSpec(pick.shape, lambda i: (0, 0))],
        out_specs=[piece, piece],
        compiler_params=pltpu.CompilerParams(vmem_limit_bytes=16 * MIB),
        name="cut_corners",
    )(ylo, yhi, jnp.asarray(pick.astype(jnp.bfloat16)))


def add_planes(table, planes, halves, eye, first_plane, total_rows, edge_lines):
    source = planes[0][0]
    coeffs, cells_y, cells_z = source.shape[0], source.shape[-2], source.shape[-1]
    count = len(planes)
    arrays = []
    for array, _ in planes:
        if not any(array is other for other in arrays):
            arrays.append(array)
    places = [next(i for i, o in enumerate(arrays) if o is array) for array, _ in planes]
    new = table is None

    def kernel(*refs):
        refs = list(refs)
        if not new:
            refs.pop(0)
        inputs = [refs.pop(0) for _ in arrays]
        shared = [refs.pop(0) for _ in halves]
        eye = refs.pop(0)
        table = refs.pop(0)
        edges = [refs.pop(0) for _ in range(2)] if edge_lines else []
        buf, sems, spread = refs[:3]
        copies = []
        for p, ((_, at), place) in enumerate(zip(planes, places)):
            ref = inputs[place] if at is None else inputs[place].at[:, at]
            copies.append(pltpu.make_async_copy(ref, buf.at[p], sems.at[p]))
        for q, piece in enumerate(shared):
            copies.append(pltpu.make_async_copy(piece, refs[3].at[q], refs[4].at[q]))
        for copy in copies:
            copy.start()

        def turn(p):
            def put(y, block):
                at = pl.multiple_of(((first_plane + p) * cells_y + y) * cells_z, 8)
                table[pl.ds(at, cells_z), :] = block

            turn_rows(spread, eye, coeffs, cells_y, cells_z, put)

        def one(p, _):
            first = inputs[0] if planes[0][1] is None else inputs[0].at[:, 0]
            pltpu.make_async_copy(first, buf.at[p], sems.at[p]).wait()
            fill_rows(
                lambda c, h: buf[p, c, :, h * LANES : (h + 1) * LANES],
                spread,
                coeffs,
                cells_y,
                cells_z,
            )
            turn(p)
            return 0

        lax.fori_loop(0, count, one, 0)
        if halves:
            for copy in copies[count:]:
                copy.wait()
            fill_rows(
                lambda c, h: jnp.concatenate(
                    [
                        refs[3][q, c, :, h * LANES : (h + 1) * LANES].astype(jnp.float32)
                        for q in range(2)
                    ],
                    axis=0,
                ),
                spread,
                coeffs,
                cells_y,
                cells_z,
            )
            turn(count)
        for out, start in zip(edges, (0, cells_z - HALO)):
            for j in range(HALO):
                for line in range(0, edge_lines, 16):
                    parts = [
                        table[pl.ds((line + i) * cells_z + start + j, 8, stride=cells_z), :]
                        for i in (0, 8)
                    ]
                    at = j * edge_lines + line
                    out[at : at + 16, :] = jnp.concatenate(parts, axis=0).astype(jnp.bfloat16)

    vmem = pl.BlockSpec(memory_space=pltpu.VMEM)
    hbm = pl.BlockSpec(memory_space=pl.ANY)
    shapes = [pltpu.VMEM((total_rows, LANES), jnp.float32)]
    if edge_lines:
        shapes += [jax.ShapeDtypeStruct((HALO * edge_lines, LANES), jnp.bfloat16)] * 2
    scratch = [
        pltpu.VMEM((count, coeffs, cells_y, cells_z), jnp.bfloat16),
        pltpu.SemaphoreType.DMA((count,)),
        spread_shape(coeffs, cells_y, cells_z),
    ]
    if halves:
        scratch += [
            pltpu.VMEM((2, coeffs, cells_y // 2, cells_z), jnp.bfloat16),
            pltpu.SemaphoreType.DMA((2,)),
        ]
    held = [] if new else [table]
    return pl.pallas_call(
        kernel,
        out_shape=shapes,
        in_specs=[vmem] * len(held) + [hbm] * (len(arrays) + len(halves)) + [vmem],
        out_specs=[vmem] * len(shapes),
        scratch_shapes=scratch,
        input_output_aliases={} if new else {0: 0},
        compiler_params=pltpu.CompilerParams(vmem_limit_bytes=TABLE_LIMIT * MIB),
        cost_estimate=pl.CostEstimate(
            flops=2 * 10**10, transcendentals=0, bytes_accessed=2 * 10**7
        ),
    )(*held, *arrays, *halves, eye)


def cut_ends(zlo, zhi, lines, cells_x, cells_y):
    own = cells_x * cells_y
    half = HALO * cells_y + 2 * HALO * HALO
    rows = 2 * HALO * half

    def kernel(zlo, zhi, pick, up, down):
        both = jnp.concatenate([zlo[...], zhi[...]], axis=0)
        chosen = jnp.dot(pick[...], both, preferred_element_type=jnp.float32)
        up[...] = chosen[:rows].astype(jnp.bfloat16)
        down[...] = chosen[rows:].astype(jnp.bfloat16)

    pick = np.zeros((2 * rows, 2 * HALO * lines), np.float32)
    for side in range(2):
        x = cells_x - HALO if side == 0 else 0
        places = [x * cells_y + i for i in range(HALO * cells_y)]
        for face in range(2):
            at = own + face * cells_y + x * HALO
            places += [at + i for i in range(HALO * HALO)]
        for z in range(2 * HALO):
            for i, place in enumerate(places):
                pick[side * rows + z * half + i, z * lines + place] = 1.0
    vmem = pl.BlockSpec(memory_space=pltpu.VMEM)
    return pl.pallas_call(
        kernel,
        out_shape=[jax.ShapeDtypeStruct((rows, LANES), jnp.bfloat16)] * 2,
        in_specs=[vmem] * 3,
        out_specs=[vmem] * 2,
        compiler_params=pltpu.CompilerParams(vmem_limit_bytes=8 * MIB),
        name="cut_ends",
    )(zlo, zhi, jnp.asarray(pick.astype(jnp.bfloat16)))


TABLE_LIMIT = 24
GROUP = 8
PARTS = 3


def prepare(samples, weights, slot, origin, cells, total):
    count = slot.shape[0]
    cells_x, cells_y, cells_z = cells
    own_lines = cells_x * cells_y
    early = own_lines + 2 * cells_y
    rows = (early + (2 * HALO + 1) * cells_y) * cells_z
    block = 256
    burst = 32
    kinds = (2 + PARTS) * SAMPLES
    corner = HALO * HALO
    end = HALO * cells_y + 2 * corner

    def locate(near_x, near_y, near_z):
        own_x = (near_x >= HALO) & (near_x < HALO + cells_x)
        own_y = (near_y >= HALO) & (near_y < HALO + cells_y)
        low_x = near_x < HALO
        low_y = near_y < HALO
        side_x = jnp.where(low_x, near_x, near_x - HALO - cells_x)
        side_y = jnp.where(low_y, near_y, near_y - HALO - cells_y)
        line_own = (near_x - HALO) * cells_y + near_y - HALO
        line_y = own_lines + jnp.where(low_y, 0, cells_y) + (near_x - HALO) * HALO + side_y
        line_early = jnp.where(own_y, line_own, line_y)
        in_face = side_x * cells_y + near_y - HALO
        in_corner = jnp.where(low_y, 0, corner) + side_x * HALO + side_y
        line_late = early + jnp.where(
            own_y,
            jnp.where(low_x, 0, HALO * cells_y) + in_face,
            2 * HALO * cells_y + jnp.where(low_x, 0, 2 * corner) + in_corner,
        )
        line = jnp.where(own_x, line_early, line_late)
        edge = jnp.where(near_z < HALO, near_z, near_z - cells_z)
        at_end = jnp.where(own_y, in_face, HALO * cells_y + in_corner)
        beyond = jnp.where(
            own_x,
            edge * early + line_early,
            2 * HALO * early + jnp.where(low_x, 0, 2 * HALO * end) + edge * end + at_end,
        )
        inside = (near_z >= HALO) & (near_z < HALO + cells_z)
        return jnp.where(inside, line * cells_z + near_z - HALO, rows + beyond)

    def kernel(origin, slot, samples, weights, eye, join, index, ordered, natural):
        def turn(j, _):
            at = pl.multiple_of(j * block, block)
            near = []
            for d in range(3):
                shift = samples[d, :, pl.ds(at, block)] - origin[d] + HALO
                shift = jnp.where(shift < 0, shift + total[d], shift)
                near.append(jnp.where(shift >= total[d], shift - total[d], shift))
            row = locate(*near)
            pieces = [(row >> 8).astype(jnp.float32), (row & 255).astype(jnp.float32)]
            rest = weights[:, pl.ds(at, block)]
            for _ in range(PARTS):
                piece = rest.astype(jnp.bfloat16).astype(jnp.float32)
                pieces.append(piece)
                rest = rest - piece
            pieces.append(jnp.zeros((LANES - kinds, block), jnp.float32))
            natural[pl.ds(at, block), :] = lax.dot_general(
                eye[...],
                jnp.concatenate(pieces, axis=0).astype(jnp.bfloat16),
                (((1,), (1,)), ((), ())),
                preferred_element_type=jnp.float32,
            )
            return 0

        lax.fori_loop(0, count // block, turn, 0)

        def scatter(j, _):
            at = pl.multiple_of(j * burst, burst)
            mine = slot.at[pl.ds(at, burst)]
            for g in range(0, burst, GROUP):
                tile = natural[pl.ds(at + g, GROUP), :]
                for k in range(GROUP):
                    ordered[pl.ds(mine[g + k], 1), :] = tile[k : k + 1, :]
            return 0

        lax.fori_loop(0, count // burst, scatter, 0)

        def collect(j, _):
            at = pl.multiple_of(j * 4 * LANES, 4 * LANES)
            wide = lax.dot_general(
                join[...],
                ordered[pl.ds(at, 4 * LANES), :].astype(jnp.bfloat16),
                (((1,), (1,)), ((), ())),
                preferred_element_type=jnp.float32,
            ).astype(jnp.int32)
            for i in range(4):
                to = pl.multiple_of((j * 4 + i) * SAMPLES, SAMPLES)
                index[pl.ds(to, SAMPLES), :] = wide[:SAMPLES, i * LANES : (i + 1) * LANES]
            return 0

        lax.fori_loop(0, count // (4 * LANES), collect, 0)

    join = np.zeros((16, LANES), np.float32)
    for s in range(SAMPLES):
        join[s, s] = 256.0
        join[s, SAMPLES + s] = 1.0
    vmem = pl.BlockSpec(memory_space=pltpu.VMEM)
    smem = pl.BlockSpec(memory_space=pltpu.SMEM)
    return pl.pallas_call(
        kernel,
        out_shape=(
            jax.ShapeDtypeStruct((count * SAMPLES // LANES, LANES), jnp.int32),
            jax.ShapeDtypeStruct((count, LANES), jnp.float32),
        ),
        in_specs=[smem, smem, vmem, vmem, vmem, vmem],
        out_specs=(vmem, vmem),
        scratch_shapes=[pltpu.VMEM((count, LANES), jnp.float32)],
        compiler_params=pltpu.CompilerParams(vmem_limit_bytes=12 * MIB),
        cost_estimate=pl.CostEstimate(
            flops=2 * 10**10, transcendentals=0, bytes_accessed=3 * 10**6
        ),
        name="prepare",
    )(
        origin,
        slot,
        samples,
        weights,
        jnp.asarray(np.eye(block, dtype=np.float32).astype(jnp.bfloat16)),
        jnp.asarray(join.astype(jnp.bfloat16)),
    )


def spread_weights(ordered):
    count = ordered.shape[0]
    block = 512

    def kernel(ordered, ones, wide):
        rows = ordered[...].astype(jnp.bfloat16)
        for h in range(0, SAMPLES, 2):
            both = jnp.dot(
                rows, ones[:, h * LANES : (h + 2) * LANES], preferred_element_type=jnp.float32
            )
            for s in range(2):
                for g in range(block // GROUP):
                    to = (g * SAMPLES + h + s) * GROUP
                    wide[to : to + GROUP, :] = both[
                        g * GROUP : (g + 1) * GROUP, s * LANES : (s + 1) * LANES
                    ]

    ones = np.zeros((LANES, SAMPLES * LANES), np.float32)
    for s in range(SAMPLES):
        for p in range(PARTS):
            ones[(2 + p) * SAMPLES + s, s * LANES : (s + 1) * LANES] = 1.0
    return pl.pallas_call(
        kernel,
        out_shape=pltpu.HBM((count * SAMPLES, LANES), jnp.float32),
        grid=(count // block,),
        in_specs=[
            pl.BlockSpec((block, LANES), lambda i: (i, 0)),
            pl.BlockSpec(ones.shape, lambda i: (0, 0)),
        ],
        out_specs=pl.BlockSpec((block * SAMPLES, LANES), lambda i: (i, 0)),
        compiler_params=pltpu.CompilerParams(vmem_limit_bytes=12 * MIB),
        cost_estimate=pl.CostEstimate(
            flops=10**10, transcendentals=0, bytes_accessed=3 * 10**6
        ),
        name="spread_weights",
    )(ordered, jnp.asarray(ones.astype(jnp.bfloat16)))


RING = 2
STREAM = 8
CHUNK = 1024


def gather_rows(index, wide, table, edges, first_edge, coeffs):
    count = wide.shape[0] // SAMPLES
    chunks = index.shape[0] // CHUNK
    per_chunk = CHUNK // SAMPLES
    groups = per_chunk // GROUP
    pairs = count // 32
    half = LANES // 2

    def kernel(index, wide, pick, *refs):
        table, out, local, sems, near, near_sems, rows = refs[len(edges) + 1 :]
        at = first_edge
        for edge in refs[: len(edges)]:
            table[pl.ds(at, edge.shape[0]), :] = edge[...].astype(jnp.float32)
            at += edge.shape[0]
        sublane = lax.broadcasted_iota(jnp.int32, (GROUP, LANES), 0)
        masks = [sublane == k for k in range(GROUP)]
        used = lax.broadcasted_iota(jnp.int32, (GROUP, LANES), 1) < coeffs

        def fetch(n, slot):
            return pltpu.make_async_copy(
                index.at[pl.ds(pl.multiple_of(n * CHUNK, CHUNK), CHUNK)],
                local.at[slot],
                sems.at[slot],
            )

        def stream(n, slot):
            return pltpu.make_async_copy(
                wide.at[pl.ds(pl.multiple_of(n * CHUNK, CHUNK), CHUNK), :],
                near.at[slot],
                near_sems.at[slot],
            )

        for b in range(RING - 1):
            fetch(b, b).start()
        for b in range(STREAM - 1):
            stream(b, b).start()

        def body(i, _):
            for b in range(RING):
                n = i * RING + b
                slot = n % STREAM
                fetch(n, b).wait()
                stream(n, slot).wait()
                ahead = n + RING - 1
                later = n + STREAM - 1

                @pl.when(ahead < chunks)
                def _():
                    fetch(ahead, (b + RING - 1) % RING).start()

                @pl.when(later < chunks)
                def _():
                    stream(later, later % STREAM).start()

                for q in range(groups):
                    total = None
                    for s in range(SAMPLES):
                        merged = None
                        for k in range(GROUP):
                            place = s * per_chunk + q * GROUP + k
                            row = table[pl.ds(local[b, place], GROUP, stride=0), :]
                            merged = row if merged is None else jnp.where(masks[k], row, merged)
                        at = (q * SAMPLES + s) * GROUP
                        term = merged * near[slot, at : at + GROUP, :]
                        total = term if total is None else total + term
                    to = pl.multiple_of((n * (groups // 4) + q // 4) * GROUP, GROUP)
                    rows[q % 4, pl.ds(to, GROUP), :] = jnp.where(used, total, 0.0)
            return 0

        lax.fori_loop(0, chunks // RING, body, 0)

        def pack(i, _):
            at = pl.multiple_of(i * 128, 128)
            part = [rows[q, pl.ds(at, 128), :].astype(jnp.bfloat16) for q in range(4)]
            outer = [jnp.concatenate([part[0], part[2]], axis=1)]
            outer.append(jnp.concatenate([part[1], part[3]], axis=1))
            first = jnp.dot(outer[0], pick[0], preferred_element_type=jnp.float32)
            second = jnp.dot(outer[1], pick[0], preferred_element_type=jnp.float32)
            third = jnp.dot(outer[0], pick[1], preferred_element_type=jnp.float32)
            third += jnp.dot(outer[1], pick[2], preferred_element_type=jnp.float32)
            for d in range(128 // GROUP):
                here = slice(d * GROUP, (d + 1) * GROUP)
                out[i * (128 // GROUP) + d, :16, :] = jnp.concatenate(
                    [first[here], second[here]], axis=0
                ).astype(jnp.bfloat16)
                out[i * (128 // GROUP) + d, 16:, :] = third[here].astype(jnp.bfloat16)
            return 0

        lax.fori_loop(0, pairs * GROUP // 128, pack, 0)

    pick = np.zeros((3, 2 * LANES, LANES), np.float32)
    for c in range(half):
        pick[0, c, c] = 1.0
        pick[0, LANES + c, half + c] = 1.0
    for c in range(32):
        pick[1, half + c, c] = 1.0
        pick[1, LANES + half + c, 64 + c] = 1.0
        pick[2, half + c, 32 + c] = 1.0
        pick[2, LANES + half + c, 96 + c] = 1.0
    vmem = pl.BlockSpec(memory_space=pltpu.VMEM)
    return pl.pallas_call(
        kernel,
        out_shape=(
            pltpu.VMEM(table.shape, jnp.float32),
            jax.ShapeDtypeStruct((pairs, 24, LANES), jnp.bfloat16),
        ),
        in_specs=[vmem, pl.BlockSpec(memory_space=pl.ANY)] + [vmem] * (2 + len(edges)),
        out_specs=(vmem, vmem),
        scratch_shapes=[
            pltpu.SMEM((RING, CHUNK), jnp.int32),
            pltpu.SemaphoreType.DMA((RING,)),
            pltpu.VMEM((STREAM, CHUNK, LANES), jnp.float32),
            pltpu.SemaphoreType.DMA((STREAM,)),
            pltpu.VMEM((4, pairs * GROUP, LANES), jnp.float32),
        ],
        input_output_aliases={3 + len(edges): 0},
        compiler_params=pltpu.CompilerParams(vmem_limit_bytes=24 * MIB),
        cost_estimate=pl.CostEstimate(
            flops=4 * 10**10, transcendentals=0, bytes_accessed=2 * 10**7
        ),
        name="gather_rows",
    )(index, wide, jnp.asarray(pick.astype(jnp.bfloat16)), *edges, table)[1]


def relight(transfer, routed, basis, projector):
    coeffs, count = transfer.shape
    sources, packed, _ = routed.shape
    per_pair = count // sources
    block = 512
    step = block // per_pair

    def kernel(transfer, routed, basis, wide, projector, out):
        low = lax.broadcasted_iota(jnp.int32, (GROUP, LANES), 1) < 64
        parts = []
        for i in range(step):
            head = routed[i, :16, :].astype(jnp.float32)
            first, second = head[:GROUP], head[GROUP:]
            third = routed[i, 16:, :].astype(jnp.float32)
            parts += [
                jnp.where(low, first, pltpu.roll(third, 64, 1)),
                jnp.where(low, second, pltpu.roll(third, 32, 1)),
                jnp.where(low, pltpu.roll(first, 64, 1), third),
                jnp.where(low, pltpu.roll(second, 64, 1), pltpu.roll(third, 96, 1)),
            ]
        rows = jnp.concatenate(parts, axis=0).astype(jnp.bfloat16)
        lit = jnp.dot(basis[...], transfer[...], preferred_element_type=jnp.float32)
        shade = lax.dot_general(
            wide[...], rows, (((1,), (1,)), ((), ())), preferred_element_type=jnp.float32
        )
        product = (lit * shade).astype(jnp.bfloat16)
        out[...] = jnp.dot(projector[...], product, preferred_element_type=jnp.float32).astype(
            jnp.bfloat16
        )

    directions = basis.shape[0]
    wide = np.zeros((directions, LANES), jnp.bfloat16)
    wide[:, :coeffs] = basis
    return pl.pallas_call(
        kernel,
        out_shape=jax.ShapeDtypeStruct((coeffs, count), jnp.bfloat16),
        grid=(count // block,),
        in_specs=[
            pl.BlockSpec((coeffs, block), lambda i: (0, i)),
            pl.BlockSpec((step, packed, LANES), lambda i: (i, 0, 0)),
            pl.BlockSpec((directions, coeffs), lambda i: (0, 0)),
            pl.BlockSpec((directions, LANES), lambda i: (0, 0)),
            pl.BlockSpec((coeffs, directions), lambda i: (0, 0)),
        ],
        out_specs=pl.BlockSpec((coeffs, block), lambda i: (0, i)),
        compiler_params=pltpu.CompilerParams(vmem_limit_bytes=40 * MIB),
        name="relight",
    )(transfer, routed, jnp.asarray(basis), jnp.asarray(wide), jnp.asarray(projector))


def moves(sizes, steps):
    pairs = []
    for x in range(sizes[0]):
        for y in range(sizes[1]):
            to_x, to_y = (x + steps[0]) % sizes[0], (y + steps[1]) % sizes[1]
            pairs.append((x * sizes[1] + y, to_x * sizes[1] + to_y))
    return pairs


def halo_step(field, samples, weights, destination, transfer):
    basis, projector = direction_tables()
    coeffs, cells_x, cells_y, cells_z = field.shape
    count = transfer.shape[1]
    along = tuple(lax.axis_size(axis) for axis in ("gx", "gy", "gz"))
    ups = [moves((n, 1), (1, 0)) for n in along]
    downs = [moves((n, 1), (-1, 0)) for n in along]

    cells = (cells_x, cells_y, cells_z)
    total = tuple(c * n for c, n in zip(cells, along))
    origin = jnp.stack(
        [lax.axis_index(axis) * c for axis, c in zip(("gx", "gy", "gz"), cells)]
    ).astype(jnp.int32)
    devices = math.prod(along)
    per_pair = count // devices
    slot = destination[0] * per_pair + destination[1]

    field = pltpu.with_memory_space_constraint(field, pltpu.HBM)
    last, first, top, bottom = cut_faces(field)
    ylo = lax.ppermute(top, "gy", ups[1])
    yhi = lax.ppermute(bottom, "gy", downs[1])
    xlo = lax.ppermute(last, "gx", ups[0])
    xhi = lax.ppermute(first, "gx", downs[0])
    field, slot, origin = lax.optimization_barrier((field, slot, origin))

    eye = jnp.asarray(np.eye(cells_z, dtype=np.float32).astype(jnp.bfloat16))
    early = (cells_x + 2) * cells_y
    rows = (early + (2 * HALO + 1) * cells_y) * cells_z
    ends = HALO * cells_y + 2 * HALO * HALO
    total_rows = rows + 2 * HALO * (early + 2 * ends)
    own = [(field, x) for x in range(cells_x)]
    table = add_planes(None, own, (), eye, 0, total_rows, 0)[0]
    index, ordered = prepare(samples, weights, slot, origin, cells, total)
    table, index, ordered, ylo, yhi = lax.optimization_barrier((table, index, ordered, ylo, yhi))
    up, down = cut_corners(ylo, yhi)
    clo = lax.ppermute(up, "gx", ups[0])
    chi = lax.ppermute(down, "gx", downs[0])
    table, bottoms, tops = add_planes(
        table, [(ylo, None), (yhi, None)], (), eye, cells_x, total_rows, early
    )
    zhi = lax.ppermute(bottoms, "gz", downs[2])
    zlo = lax.ppermute(tops, "gz", ups[2])
    up, down = cut_ends(zlo, zhi, early, cells_x, cells_y)
    up, down, ordered = lax.optimization_barrier((up, down, ordered))
    elo = lax.ppermute(up, "gx", ups[0])
    ehi = lax.ppermute(down, "gx", downs[0])
    wide = spread_weights(ordered)
    table, wide = lax.optimization_barrier((table, wide))
    sides = [(xlo, 0), (xlo, 1), (xhi, 0), (xhi, 1)]
    table = add_planes(table, sides, (clo, chi), eye, cells_x + 2, total_rows, 0)[0]
    outgoing = gather_rows(
        index.reshape(-1), wide, table, (zlo, zhi, elo, ehi), rows, coeffs
    )
    routed = lax.all_to_all(
        outgoing, ("gx", "gy", "gz"), split_axis=0, concat_axis=0, tiled=True
    )
    return relight(transfer, routed, basis, projector)


def solution(mesh):
    placed = (
        P(None, "gx", "gy", "gz"),
        P(None, None, ("gx", "gy", "gz")),
        P(None, ("gx", "gy", "gz")),
        P(None, ("gx", "gy", "gz")),
        P(None, ("gx", "gy", "gz")),
    )
    return jax.shard_map(
        halo_step,
        mesh=mesh,
        in_specs=placed,
        out_specs=P(None, ("gx", "gy", "gz")),
        check_vma=False,
    )
```

```python
import math

import jax
import jax.numpy as jnp
import numpy as np
from jax import lax
from jax.experimental import pallas as pl
from jax.experimental.pallas import tpu as pltpu
from jax.sharding import PartitionSpec as P


HALO = 2
SAMPLES = 8
DEGREES = 9
POLAR = 32
AZIMUTH = 32
LANES = 128
MIB = 1024 * 1024


def harmonic_values():
    polar = (np.arange(POLAR, dtype=np.float64) + 0.5) * (2.0 / POLAR) - 1.0
    beside = (np.arange(AZIMUTH, dtype=np.float64) + 0.5) * (2.0 * math.pi / AZIMUTH)
    cosines = np.repeat(polar, AZIMUTH)
    angles = np.tile(beside, POLAR)
    sines = np.sqrt(np.maximum(1.0 - cosines * cosines, 0.0))
    entries = {}
    for m in range(DEGREES):
        diagonal = (-1.0) ** m * float(math.prod(range(1, 2 * m, 2))) * sines**m
        legendre = {m: diagonal}
        if m + 1 < DEGREES:
            legendre[m + 1] = cosines * (2 * m + 1) * diagonal
        for l in range(m + 2, DEGREES):
            legendre[l] = (
                (2 * l - 1) * cosines * legendre[l - 1] - (l + m - 1) * legendre[l - 2]
            ) / (l - m)
        for l in range(m, DEGREES):
            factor = math.sqrt(
                (2 * l + 1) / (4.0 * math.pi) * math.factorial(l - m) / math.factorial(l + m)
            )
            if m == 0:
                entries[l, 0] = factor * legendre[l]
            else:
                entries[l, m] = math.sqrt(2.0) * factor * np.cos(m * angles) * legendre[l]
                entries[l, -m] = math.sqrt(2.0) * factor * np.sin(m * angles) * legendre[l]
    return np.stack([entries[l, m] for l in range(DEGREES) for m in range(-l, l + 1)])


def direction_tables():
    values = harmonic_values()
    basis = values.T.astype(np.float32).astype(jnp.bfloat16)
    projector = (values * (4.0 * math.pi / (POLAR * AZIMUTH))).astype(np.float32)
    return basis, projector.astype(jnp.bfloat16)


def fill_rows(get, spread, coeffs, rows_y, cells_z):
    halves = cells_z // LANES
    for c in range(coeffs):
        for h in range(halves):
            block = get(c, h).astype(jnp.float32)
            spread[h, pl.ds(c, rows_y, stride=coeffs), :] = block


def turn_rows(spread, eye, coeffs, rows_y, cells_z, put):
    halves = cells_z // LANES
    keep = -(-coeffs // 16) * 16
    zeros = jnp.zeros((LANES - keep, cells_z), jnp.bfloat16)
    for y in range(0, rows_y, 2):
        parts = []
        for i in (y, y + 1):
            rows = jnp.concatenate(
                [spread[h, i * coeffs : i * coeffs + keep, :] for h in range(halves)], axis=1
            )
            parts += [rows.astype(jnp.bfloat16), zeros]
        both = lax.dot_general(
            eye[...],
            jnp.concatenate(parts, axis=0),
            (((1,), (1,)), ((), ())),
            preferred_element_type=jnp.float32,
        )
        put(y, both[:, :LANES])
        put(y + 1, both[:, LANES:])


def spread_shape(coeffs, cells_y, cells_z):
    return pltpu.VMEM((cells_z // LANES, cells_y * coeffs + 16, LANES), jnp.float32)


def cut_faces(field):
    coeffs, cells_x, cells_y, cells_z = field.shape
    parts = 9
    per_part = coeffs // parts
    rows = cells_x * HALO

    def kernel(field, pick, last, first, top, bottom, buf, high, low, sems, out_sems):
        def load(i):
            here = pl.ds(i * per_part, per_part)
            return pltpu.make_async_copy(field.at[here], buf.at[here], sems.at[i])

        def saves(i):
            here = pl.ds(i * per_part, per_part)
            return [
                pltpu.make_async_copy(high.at[here], top.at[here], out_sems.at[0, i]),
                pltpu.make_async_copy(low.at[here], bottom.at[here], out_sems.at[1, i]),
                pltpu.make_async_copy(
                    buf.at[here, pl.ds(cells_x - HALO, HALO)], last.at[here], out_sems.at[2, i]
                ),
                pltpu.make_async_copy(
                    buf.at[here, pl.ds(0, HALO)], first.at[here], out_sems.at[3, i]
                ),
            ]

        for i in range(parts):
            load(i).start()

        def body(i, _):
            load(i).wait()
            for k in range(per_part):
                c = i * per_part + k
                chosen = jnp.dot(
                    pick[...],
                    buf[c].reshape(cells_x * cells_y, cells_z),
                    preferred_element_type=jnp.float32,
                ).astype(jnp.bfloat16)
                high[c] = chosen[:rows]
                low[c] = chosen[rows:]
            for save in saves(i):
                save.start()
            return 0

        lax.fori_loop(0, parts, body, 0)
        for i in range(parts):
            for save in saves(i):
                save.wait()

    pick = np.zeros((2 * rows, cells_x * cells_y), np.float32)
    for x in range(cells_x):
        for j in range(HALO):
            pick[x * HALO + j, x * cells_y + cells_y - HALO + j] = 1.0
            pick[rows + x * HALO + j, x * cells_y + j] = 1.0
    shapes = [(coeffs, HALO, cells_y, cells_z)] * 2 + [(coeffs, rows, cells_z)] * 2
    hbm = pl.BlockSpec(memory_space=pl.ANY)
    return pl.pallas_call(
        kernel,
        out_shape=[pltpu.HBM(shape, jnp.bfloat16) for shape in shapes],
        in_specs=[hbm, pl.BlockSpec(memory_space=pltpu.VMEM)],
        out_specs=[hbm] * 4,
        scratch_shapes=[
            pltpu.VMEM(field.shape, jnp.bfloat16),
            pltpu.VMEM((coeffs, rows, cells_z), jnp.bfloat16),
            pltpu.VMEM((coeffs, rows, cells_z), jnp.bfloat16),
            pltpu.SemaphoreType.DMA((parts,)),
            pltpu.SemaphoreType.DMA((4, parts)),
        ],
        compiler_params=pltpu.CompilerParams(vmem_limit_bytes=16 * MIB),
        name="cut_faces",
    )(field, jnp.asarray(pick.astype(jnp.bfloat16)))


def cut_corners(ylo, yhi):
    coeffs, rows, cells_z = ylo.shape
    per_step = 27
    corner = HALO * HALO

    def kernel(ylo, yhi, pick, up, down):
        for c in range(per_step):
            chosen = jnp.dot(
                pick[...],
                jnp.concatenate([ylo[c], yhi[c]], axis=0),
                preferred_element_type=jnp.float32,
            )
            up[c] = chosen[: 2 * corner].astype(jnp.bfloat16)
            down[c] = chosen[2 * corner :].astype(jnp.bfloat16)

    pick = np.zeros((4 * corner, 2 * rows), np.float32)
    for side in range(2):
        for i in range(corner):
            pick[side * corner + i, side * rows + rows - corner + i] = 1.0
            pick[2 * corner + side * corner + i, side * rows + i] = 1.0
    shape = (coeffs, 2 * corner, cells_z)
    face = pl.BlockSpec((per_step, rows, cells_z), lambda i: (i, 0, 0))
    piece = pl.BlockSpec((per_step,) + shape[1:], lambda i: (i, 0, 0))
    return pl.pallas_call(
        kernel,
        out_shape=[pltpu.HBM(shape, jnp.bfloat16)] * 2,
        grid=(coeffs // per_step,),
        in_specs=[face, face, pl.BlockSpec(pick.shape, lambda i: (0, 0))],
        out_specs=[piece, piece],
        compiler_params=pltpu.CompilerParams(vmem_limit_bytes=16 * MIB),
        name="cut_corners",
    )(ylo, yhi, jnp.asarray(pick.astype(jnp.bfloat16)))


def add_planes(table, planes, halves, eye, first_plane, total_rows, edge_lines):
    source = planes[0][0]
    coeffs, cells_y, cells_z = source.shape[0], source.shape[-2], source.shape[-1]
    count = len(planes)
    arrays = []
    for array, _ in planes:
        if not any(array is other for other in arrays):
            arrays.append(array)
    places = [next(i for i, o in enumerate(arrays) if o is array) for array, _ in planes]
    new = table is None

    def kernel(*refs):
        refs = list(refs)
        if not new:
            refs.pop(0)
        inputs = [refs.pop(0) for _ in arrays]
        shared = [refs.pop(0) for _ in halves]
        eye = refs.pop(0)
        table = refs.pop(0)
        edges = [refs.pop(0) for _ in range(2)] if edge_lines else []
        buf, sems, spread = refs[:3]
        copies = []
        for p, ((_, at), place) in enumerate(zip(planes, places)):
            ref = inputs[place] if at is None else inputs[place].at[:, at]
            copies.append(pltpu.make_async_copy(ref, buf.at[p], sems.at[p]))
        for q, piece in enumerate(shared):
            copies.append(pltpu.make_async_copy(piece, refs[3].at[q], refs[4].at[q]))
        for copy in copies:
            copy.start()

        def turn(p):
            def put(y, block):
                at = pl.multiple_of(((first_plane + p) * cells_y + y) * cells_z, 8)
                table[pl.ds(at, cells_z), :] = block

            turn_rows(spread, eye, coeffs, cells_y, cells_z, put)

        def one(p, _):
            first = inputs[0] if planes[0][1] is None else inputs[0].at[:, 0]
            pltpu.make_async_copy(first, buf.at[p], sems.at[p]).wait()
            fill_rows(
                lambda c, h: buf[p, c, :, h * LANES : (h + 1) * LANES],
                spread,
                coeffs,
                cells_y,
                cells_z,
            )
            turn(p)
            return 0

        lax.fori_loop(0, count, one, 0)
        if halves:
            for copy in copies[count:]:
                copy.wait()
            fill_rows(
                lambda c, h: jnp.concatenate(
                    [
                        refs[3][q, c, :, h * LANES : (h + 1) * LANES].astype(jnp.float32)
                        for q in range(2)
                    ],
                    axis=0,
                ),
                spread,
                coeffs,
                cells_y,
                cells_z,
            )
            turn(count)
        for out, start in zip(edges, (0, cells_z - HALO)):
            for j in range(HALO):
                for line in range(0, edge_lines, 16):
                    parts = [
                        table[pl.ds((line + i) * cells_z + start + j, 8, stride=cells_z), :]
                        for i in (0, 8)
                    ]
                    at = j * edge_lines + line
                    out[at : at + 16, :] = jnp.concatenate(parts, axis=0).astype(jnp.bfloat16)

    vmem = pl.BlockSpec(memory_space=pltpu.VMEM)
    hbm = pl.BlockSpec(memory_space=pl.ANY)
    shapes = [pltpu.VMEM((total_rows, LANES), jnp.float32)]
    if edge_lines:
        shapes += [jax.ShapeDtypeStruct((HALO * edge_lines, LANES), jnp.bfloat16)] * 2
    scratch = [
        pltpu.VMEM((count, coeffs, cells_y, cells_z), jnp.bfloat16),
        pltpu.SemaphoreType.DMA((count,)),
        spread_shape(coeffs, cells_y, cells_z),
    ]
    if halves:
        scratch += [
            pltpu.VMEM((2, coeffs, cells_y // 2, cells_z), jnp.bfloat16),
            pltpu.SemaphoreType.DMA((2,)),
        ]
    held = [] if new else [table]
    return pl.pallas_call(
        kernel,
        out_shape=shapes,
        in_specs=[vmem] * len(held) + [hbm] * (len(arrays) + len(halves)) + [vmem],
        out_specs=[vmem] * len(shapes),
        scratch_shapes=scratch,
        input_output_aliases={} if new else {0: 0},
        compiler_params=pltpu.CompilerParams(vmem_limit_bytes=TABLE_LIMIT * MIB),
        cost_estimate=pl.CostEstimate(
            flops=2 * 10**10, transcendentals=0, bytes_accessed=2 * 10**7
        ),
    )(*held, *arrays, *halves, eye)


def cut_ends(zlo, zhi, lines, cells_x, cells_y):
    own = cells_x * cells_y
    half = HALO * cells_y + 2 * HALO * HALO
    rows = 2 * HALO * half

    def kernel(zlo, zhi, pick, up, down):
        both = jnp.concatenate([zlo[...], zhi[...]], axis=0)
        chosen = jnp.dot(pick[...], both, preferred_element_type=jnp.float32)
        up[...] = chosen[:rows].astype(jnp.bfloat16)
        down[...] = chosen[rows:].astype(jnp.bfloat16)

    pick = np.zeros((2 * rows, 2 * HALO * lines), np.float32)
    for side in range(2):
        x = cells_x - HALO if side == 0 else 0
        places = [x * cells_y + i for i in range(HALO * cells_y)]
        for face in range(2):
            at = own + face * cells_y + x * HALO
            places += [at + i for i in range(HALO * HALO)]
        for z in range(2 * HALO):
            for i, place in enumerate(places):
                pick[side * rows + z * half + i, z * lines + place] = 1.0
    vmem = pl.BlockSpec(memory_space=pltpu.VMEM)
    return pl.pallas_call(
        kernel,
        out_shape=[jax.ShapeDtypeStruct((rows, LANES), jnp.bfloat16)] * 2,
        in_specs=[vmem] * 3,
        out_specs=[vmem] * 2,
        compiler_params=pltpu.CompilerParams(vmem_limit_bytes=8 * MIB),
        name="cut_ends",
    )(zlo, zhi, jnp.asarray(pick.astype(jnp.bfloat16)))


TABLE_LIMIT = 24
GROUP = 8
PARTS = 3


def prepare(samples, weights, slot, origin, cells, total):
    count = slot.shape[0]
    cells_x, cells_y, cells_z = cells
    own_lines = cells_x * cells_y
    early = own_lines + 2 * cells_y
    rows = (early + (2 * HALO + 1) * cells_y) * cells_z
    block = 256
    burst = 32
    kinds = (2 + PARTS) * SAMPLES
    corner = HALO * HALO
    end = HALO * cells_y + 2 * corner

    def locate(near_x, near_y, near_z):
        own_x = (near_x >= HALO) & (near_x < HALO + cells_x)
        own_y = (near_y >= HALO) & (near_y < HALO + cells_y)
        low_x = near_x < HALO
        low_y = near_y < HALO
        side_x = jnp.where(low_x, near_x, near_x - HALO - cells_x)
        side_y = jnp.where(low_y, near_y, near_y - HALO - cells_y)
        line_own = (near_x - HALO) * cells_y + near_y - HALO
        line_y = own_lines + jnp.where(low_y, 0, cells_y) + (near_x - HALO) * HALO + side_y
        line_early = jnp.where(own_y, line_own, line_y)
        in_face = side_x * cells_y + near_y - HALO
        in_corner = jnp.where(low_y, 0, corner) + side_x * HALO + side_y
        line_late = early + jnp.where(
            own_y,
            jnp.where(low_x, 0, HALO * cells_y) + in_face,
            2 * HALO * cells_y + jnp.where(low_x, 0, 2 * corner) + in_corner,
        )
        line = jnp.where(own_x, line_early, line_late)
        edge = jnp.where(near_z < HALO, near_z, near_z - cells_z)
        at_end = jnp.where(own_y, in_face, HALO * cells_y + in_corner)
        beyond = jnp.where(
            own_x,
            edge * early + line_early,
            2 * HALO * early + jnp.where(low_x, 0, 2 * HALO * end) + edge * end + at_end,
        )
        inside = (near_z >= HALO) & (near_z < HALO + cells_z)
        return jnp.where(inside, line * cells_z + near_z - HALO, rows + beyond)

    def kernel(origin, slot, samples, weights, eye, join, index, ordered, natural):
        def turn(j, _):
            at = pl.multiple_of(j * block, block)
            near = []
            for d in range(3):
                shift = samples[d, :, pl.ds(at, block)] - origin[d] + HALO
                shift = jnp.where(shift < 0, shift + total[d], shift)
                near.append(jnp.where(shift >= total[d], shift - total[d], shift))
            row = locate(*near)
            pieces = [(row >> 8).astype(jnp.float32), (row & 255).astype(jnp.float32)]
            rest = weights[:, pl.ds(at, block)]
            for _ in range(PARTS):
                piece = rest.astype(jnp.bfloat16).astype(jnp.float32)
                pieces.append(piece)
                rest = rest - piece
            pieces.append(jnp.zeros((LANES - kinds, block), jnp.float32))
            natural[pl.ds(at, block), :] = lax.dot_general(
                eye[...],
                jnp.concatenate(pieces, axis=0).astype(jnp.bfloat16),
                (((1,), (1,)), ((), ())),
                preferred_element_type=jnp.float32,
            )
            return 0

        lax.fori_loop(0, count // block, turn, 0)

        def scatter(j, _):
            at = pl.multiple_of(j * burst, burst)
            mine = slot.at[pl.ds(at, burst)]
            for g in range(0, burst, GROUP):
                tile = natural[pl.ds(at + g, GROUP), :]
                for k in range(GROUP):
                    ordered[pl.ds(mine[g + k], 1), :] = tile[k : k + 1, :]
            return 0

        lax.fori_loop(0, count // burst, scatter, 0)

        def collect(j, _):
            at = pl.multiple_of(j * 4 * LANES, 4 * LANES)
            wide = lax.dot_general(
                join[...],
                ordered[pl.ds(at, 4 * LANES), :].astype(jnp.bfloat16),
                (((1,), (1,)), ((), ())),
                preferred_element_type=jnp.float32,
            ).astype(jnp.int32)
            for i in range(4):
                to = pl.multiple_of((j * 4 + i) * SAMPLES, SAMPLES)
                index[pl.ds(to, SAMPLES), :] = wide[:SAMPLES, i * LANES : (i + 1) * LANES]
            return 0

        lax.fori_loop(0, count // (4 * LANES), collect, 0)

    join = np.zeros((16, LANES), np.float32)
    for s in range(SAMPLES):
        join[s, s] = 256.0
        join[s, SAMPLES + s] = 1.0
    vmem = pl.BlockSpec(memory_space=pltpu.VMEM)
    smem = pl.BlockSpec(memory_space=pltpu.SMEM)
    return pl.pallas_call(
        kernel,
        out_shape=(
            jax.ShapeDtypeStruct((count * SAMPLES // LANES, LANES), jnp.int32),
            jax.ShapeDtypeStruct((count, LANES), jnp.float32),
        ),
        in_specs=[smem, smem, vmem, vmem, vmem, vmem],
        out_specs=(vmem, vmem),
        scratch_shapes=[pltpu.VMEM((count, LANES), jnp.float32)],
        compiler_params=pltpu.CompilerParams(vmem_limit_bytes=12 * MIB),
        cost_estimate=pl.CostEstimate(
            flops=2 * 10**10, transcendentals=0, bytes_accessed=3 * 10**6
        ),
        name="prepare",
    )(
        origin,
        slot,
        samples,
        weights,
        jnp.asarray(np.eye(block, dtype=np.float32).astype(jnp.bfloat16)),
        jnp.asarray(join.astype(jnp.bfloat16)),
    )


def spread_weights(ordered):
    count = ordered.shape[0]
    block = 512

    def kernel(ordered, ones, wide):
        rows = ordered[...].astype(jnp.bfloat16)
        for h in range(0, SAMPLES, 2):
            both = jnp.dot(
                rows, ones[:, h * LANES : (h + 2) * LANES], preferred_element_type=jnp.float32
            )
            for s in range(2):
                for g in range(block // GROUP):
                    to = (g * SAMPLES + h + s) * GROUP
                    wide[to : to + GROUP, :] = both[
                        g * GROUP : (g + 1) * GROUP, s * LANES : (s + 1) * LANES
                    ]

    ones = np.zeros((LANES, SAMPLES * LANES), np.float32)
    for s in range(SAMPLES):
        for p in range(PARTS):
            ones[(2 + p) * SAMPLES + s, s * LANES : (s + 1) * LANES] = 1.0
    return pl.pallas_call(
        kernel,
        out_shape=pltpu.HBM((count * SAMPLES, LANES), jnp.float32),
        grid=(count // block,),
        in_specs=[
            pl.BlockSpec((block, LANES), lambda i: (i, 0)),
            pl.BlockSpec(ones.shape, lambda i: (0, 0)),
        ],
        out_specs=pl.BlockSpec((block * SAMPLES, LANES), lambda i: (i, 0)),
        compiler_params=pltpu.CompilerParams(vmem_limit_bytes=12 * MIB),
        cost_estimate=pl.CostEstimate(
            flops=10**10, transcendentals=0, bytes_accessed=3 * 10**6
        ),
        name="spread_weights",
    )(ordered, jnp.asarray(ones.astype(jnp.bfloat16)))


RING = 4
STREAM = 8
CHUNK = 1024


def gather_rows(index, wide, table, edges, first_edge, coeffs):
    count = wide.shape[0] // SAMPLES
    chunks = index.shape[0] // CHUNK
    per_chunk = CHUNK // SAMPLES
    groups = per_chunk // GROUP
    pairs = count // 32
    half = LANES // 2

    def kernel(index, wide, pick, *refs):
        table, out, local, sems, near, near_sems, rows = refs[len(edges) + 1 :]
        sublane = lax.broadcasted_iota(jnp.int32, (GROUP, LANES), 0)
        masks = [sublane == k for k in range(GROUP)]
        used = lax.broadcasted_iota(jnp.int32, (GROUP, LANES), 1) < coeffs

        def fetch(n, slot):
            return pltpu.make_async_copy(
                index.at[pl.ds(pl.multiple_of(n * CHUNK, CHUNK), CHUNK)],
                local.at[slot],
                sems.at[slot],
            )

        def stream(n, slot):
            return pltpu.make_async_copy(
                wide.at[pl.ds(pl.multiple_of(n * CHUNK, CHUNK), CHUNK), :],
                near.at[slot],
                near_sems.at[slot],
            )

        for b in range(RING - 1):
            fetch(b, b).start()
        for b in range(STREAM - 1):
            stream(b, b).start()

        at = first_edge
        for edge in refs[: len(edges)]:
            table[pl.ds(at, edge.shape[0]), :] = edge[...].astype(jnp.float32)
            at += edge.shape[0]

        def body(i, _):
            for b in range(RING):
                n = i * RING + b
                slot = n % STREAM
                fetch(n, b).wait()
                stream(n, slot).wait()
                ahead = n + RING - 1
                later = n + STREAM - 1

                @pl.when(ahead < chunks)
                def _():
                    fetch(ahead, (b + RING - 1) % RING).start()

                @pl.when(later < chunks)
                def _():
                    stream(later, later % STREAM).start()

                for q in range(groups):
                    total = None
                    for s in range(SAMPLES):
                        merged = None
                        for k in range(GROUP):
                            place = s * per_chunk + q * GROUP + k
                            row = table[pl.ds(local[b, place], GROUP, stride=0), :]
                            merged = row if merged is None else jnp.where(masks[k], row, merged)
                        at = (q * SAMPLES + s) * GROUP
                        term = merged * near[slot, at : at + GROUP, :]
                        total = term if total is None else total + term
                    to = pl.multiple_of((n * (groups // 4) + q // 4) * GROUP, GROUP)
                    rows[q % 4, pl.ds(to, GROUP), :] = jnp.where(used, total, 0.0)
            return 0

        lax.fori_loop(0, chunks // RING, body, 0)

        def pack(i, _):
            at = pl.multiple_of(i * 128, 128)
            part = [rows[q, pl.ds(at, 128), :].astype(jnp.bfloat16) for q in range(4)]
            outer = [jnp.concatenate([part[0], part[2]], axis=1)]
            outer.append(jnp.concatenate([part[1], part[3]], axis=1))
            first = jnp.dot(outer[0], pick[0], preferred_element_type=jnp.float32)
            second = jnp.dot(outer[1], pick[0], preferred_element_type=jnp.float32)
            third = jnp.dot(outer[0], pick[1], preferred_element_type=jnp.float32)
            third += jnp.dot(outer[1], pick[2], preferred_element_type=jnp.float32)
            for d in range(128 // GROUP):
                here = slice(d * GROUP, (d + 1) * GROUP)
                out[i * (128 // GROUP) + d, :16, :] = jnp.concatenate(
                    [first[here], second[here]], axis=0
                ).astype(jnp.bfloat16)
                out[i * (128 // GROUP) + d, 16:, :] = third[here].astype(jnp.bfloat16)
            return 0

        lax.fori_loop(0, pairs * GROUP // 128, pack, 0)

    pick = np.zeros((3, 2 * LANES, LANES), np.float32)
    for c in range(half):
        pick[0, c, c] = 1.0
        pick[0, LANES + c, half + c] = 1.0
    for c in range(32):
        pick[1, half + c, c] = 1.0
        pick[1, LANES + half + c, 64 + c] = 1.0
        pick[2, half + c, 32 + c] = 1.0
        pick[2, LANES + half + c, 96 + c] = 1.0
    vmem = pl.BlockSpec(memory_space=pltpu.VMEM)
    return pl.pallas_call(
        kernel,
        out_shape=(
            pltpu.VMEM(table.shape, jnp.float32),
            jax.ShapeDtypeStruct((pairs, 24, LANES), jnp.bfloat16),
        ),
        in_specs=[pl.BlockSpec(memory_space=pl.ANY)] * 2 + [vmem] * (2 + len(edges)),
        out_specs=(vmem, vmem),
        scratch_shapes=[
            pltpu.SMEM((RING, CHUNK), jnp.int32),
            pltpu.SemaphoreType.DMA((RING,)),
            pltpu.VMEM((STREAM, CHUNK, LANES), jnp.float32),
            pltpu.SemaphoreType.DMA((STREAM,)),
            pltpu.VMEM((4, pairs * GROUP, LANES), jnp.float32),
        ],
        input_output_aliases={3 + len(edges): 0},
        compiler_params=pltpu.CompilerParams(vmem_limit_bytes=24 * MIB),
        cost_estimate=pl.CostEstimate(
            flops=4 * 10**10, transcendentals=0, bytes_accessed=2 * 10**7
        ),
        name="gather_rows",
    )(index, wide, jnp.asarray(pick.astype(jnp.bfloat16)), *edges, table)[1]


def relight(transfer, routed, basis, projector):
    coeffs, count = transfer.shape
    sources, packed, _ = routed.shape
    per_pair = count // sources
    block = 512
    step = block // per_pair

    def kernel(transfer, routed, basis, wide, projector, unpick, out):
        heads = [
            routed[:, i * GROUP : (i + 1) * GROUP, :].astype(jnp.float32).reshape(-1, LANES)
            for i in range(3)
        ]
        heads = [head.astype(jnp.bfloat16) for head in heads]
        pairs = [jnp.concatenate([heads[i], heads[2]], axis=1) for i in range(2)]
        quarters = [
            jnp.dot(pairs[q % 2], unpick[q], preferred_element_type=jnp.float32) for q in range(4)
        ]
        parts = []
        for i in range(step):
            parts += [quarter[i * GROUP : (i + 1) * GROUP] for quarter in quarters]
        rows = jnp.concatenate(parts, axis=0).astype(jnp.bfloat16)
        lit = jnp.dot(basis[...], transfer[...], preferred_element_type=jnp.float32)
        shade = lax.dot_general(
            wide[...], rows, (((1,), (1,)), ((), ())), preferred_element_type=jnp.float32
        )
        product = (lit * shade).astype(jnp.bfloat16)
        out[...] = jnp.dot(projector[...], product, preferred_element_type=jnp.float32).astype(
            jnp.bfloat16
        )

    directions = basis.shape[0]
    wide = np.zeros((directions, LANES), jnp.bfloat16)
    wide[:, :coeffs] = basis
    half = LANES // 2
    unpick = np.zeros((4, 2 * LANES, LANES), np.float32)
    for q in range(4):
        for c in range(half):
            unpick[q, (q // 2) * half + c, c] = 1.0
        for c in range(32):
            unpick[q, LANES + q * 32 + c, half + c] = 1.0
    return pl.pallas_call(
        kernel,
        out_shape=jax.ShapeDtypeStruct((coeffs, count), jnp.bfloat16),
        grid=(count // block,),
        in_specs=[
            pl.BlockSpec((coeffs, block), lambda i: (0, i)),
            pl.BlockSpec((step, packed, LANES), lambda i: (i, 0, 0)),
            pl.BlockSpec((directions, coeffs), lambda i: (0, 0)),
            pl.BlockSpec((directions, LANES), lambda i: (0, 0)),
            pl.BlockSpec((coeffs, directions), lambda i: (0, 0)),
            pl.BlockSpec(unpick.shape, lambda i: (0, 0, 0)),
        ],
        out_specs=pl.BlockSpec((coeffs, block), lambda i: (0, i)),
        compiler_params=pltpu.CompilerParams(vmem_limit_bytes=40 * MIB),
        name="relight",
    )(
        transfer,
        routed,
        jnp.asarray(basis),
        jnp.asarray(wide),
        jnp.asarray(projector),
        jnp.asarray(unpick.astype(jnp.bfloat16)),
    )


def moves(sizes, steps):
    pairs = []
    for x in range(sizes[0]):
        for y in range(sizes[1]):
            to_x, to_y = (x + steps[0]) % sizes[0], (y + steps[1]) % sizes[1]
            pairs.append((x * sizes[1] + y, to_x * sizes[1] + to_y))
    return pairs


def shift(array, axis, pairs):
    return pltpu.with_memory_space_constraint(lax.ppermute(array, axis, pairs), pltpu.HBM)


def halo_step(field, samples, weights, destination, transfer):
    basis, projector = direction_tables()
    coeffs, cells_x, cells_y, cells_z = field.shape
    count = transfer.shape[1]
    along = tuple(lax.axis_size(axis) for axis in ("gx", "gy", "gz"))
    ups = [moves((n, 1), (1, 0)) for n in along]
    downs = [moves((n, 1), (-1, 0)) for n in along]

    cells = (cells_x, cells_y, cells_z)
    total = tuple(c * n for c, n in zip(cells, along))
    origin = jnp.stack(
        [lax.axis_index(axis) * c for axis, c in zip(("gx", "gy", "gz"), cells)]
    ).astype(jnp.int32)
    devices = math.prod(along)
    per_pair = count // devices
    slot = destination[0] * per_pair + destination[1]

    field = pltpu.with_memory_space_constraint(field, pltpu.HBM)
    last, first, top, bottom = cut_faces(field)
    ylo = shift(top, "gy", ups[1])
    yhi = shift(bottom, "gy", downs[1])
    xlo = shift(last, "gx", ups[0])
    xhi = shift(first, "gx", downs[0])
    field, slot, origin = lax.optimization_barrier((field, slot, origin))

    eye = jnp.asarray(np.eye(cells_z, dtype=np.float32).astype(jnp.bfloat16))
    early = (cells_x + 2) * cells_y
    rows = (early + (2 * HALO + 1) * cells_y) * cells_z
    ends = HALO * cells_y + 2 * HALO * HALO
    total_rows = rows + 2 * HALO * (early + 2 * ends)
    own = [(field, x) for x in range(cells_x)]
    table = add_planes(None, own, (), eye, 0, total_rows, 0)[0]
    index, ordered = prepare(samples, weights, slot, origin, cells, total)
    table, index, ordered, ylo, yhi = lax.optimization_barrier((table, index, ordered, ylo, yhi))
    up, down = cut_corners(ylo, yhi)
    clo = shift(up, "gx", ups[0])
    chi = shift(down, "gx", downs[0])
    table, bottoms, tops = add_planes(
        table, [(ylo, None), (yhi, None)], (), eye, cells_x, total_rows, early
    )
    zhi = lax.ppermute(bottoms, "gz", downs[2])
    zlo = lax.ppermute(tops, "gz", ups[2])
    up, down = cut_ends(zlo, zhi, early, cells_x, cells_y)
    up, down, ordered = lax.optimization_barrier((up, down, ordered))
    elo = lax.ppermute(up, "gx", ups[0])
    ehi = lax.ppermute(down, "gx", downs[0])
    wide = spread_weights(ordered)
    table, wide = lax.optimization_barrier((table, wide))
    sides = [(xlo, 0), (xlo, 1), (xhi, 0), (xhi, 1)]
    table = add_planes(table, sides, (clo, chi), eye, cells_x + 2, total_rows, 0)[0]
    outgoing = gather_rows(
        index.reshape(-1), wide, table, (zlo, zhi, elo, ehi), rows, coeffs
    )
    routed = lax.all_to_all(
        outgoing, ("gx", "gy", "gz"), split_axis=0, concat_axis=0, tiled=True
    )
    return relight(transfer, routed, basis, projector)


def solution(mesh):
    placed = (
        P(None, "gx", "gy", "gz"),
        P(None, None, ("gx", "gy", "gz")),
        P(None, ("gx", "gy", "gz")),
        P(None, ("gx", "gy", "gz")),
        P(None, ("gx", "gy", "gz")),
    )
    return jax.shard_map(
        halo_step,
        mesh=mesh,
        in_specs=placed,
        out_specs=P(None, ("gx", "gy", "gz")),
        check_vma=False,
    )
```

```python
import math

import jax
import jax.numpy as jnp
import numpy as np
from jax import lax
from jax.experimental import pallas as pl
from jax.experimental.pallas import tpu as pltpu
from jax.sharding import PartitionSpec as P


HALO = 2
SAMPLES = 8
DEGREES = 9
POLAR = 32
AZIMUTH = 32
LANES = 128
MIB = 1024 * 1024


def harmonic_values():
    polar = (np.arange(POLAR, dtype=np.float64) + 0.5) * (2.0 / POLAR) - 1.0
    beside = (np.arange(AZIMUTH, dtype=np.float64) + 0.5) * (2.0 * math.pi / AZIMUTH)
    cosines = np.repeat(polar, AZIMUTH)
    angles = np.tile(beside, POLAR)
    sines = np.sqrt(np.maximum(1.0 - cosines * cosines, 0.0))
    entries = {}
    for m in range(DEGREES):
        diagonal = (-1.0) ** m * float(math.prod(range(1, 2 * m, 2))) * sines**m
        legendre = {m: diagonal}
        if m + 1 < DEGREES:
            legendre[m + 1] = cosines * (2 * m + 1) * diagonal
        for l in range(m + 2, DEGREES):
            legendre[l] = (
                (2 * l - 1) * cosines * legendre[l - 1] - (l + m - 1) * legendre[l - 2]
            ) / (l - m)
        for l in range(m, DEGREES):
            factor = math.sqrt(
                (2 * l + 1) / (4.0 * math.pi) * math.factorial(l - m) / math.factorial(l + m)
            )
            if m == 0:
                entries[l, 0] = factor * legendre[l]
            else:
                entries[l, m] = math.sqrt(2.0) * factor * np.cos(m * angles) * legendre[l]
                entries[l, -m] = math.sqrt(2.0) * factor * np.sin(m * angles) * legendre[l]
    return np.stack([entries[l, m] for l in range(DEGREES) for m in range(-l, l + 1)])


def direction_tables():
    values = harmonic_values()
    basis = values.T.astype(np.float32).astype(jnp.bfloat16)
    projector = (values * (4.0 * math.pi / (POLAR * AZIMUTH))).astype(np.float32)
    return basis, projector.astype(jnp.bfloat16)


def fill_rows(get, spread, coeffs, rows_y, cells_z):
    halves = cells_z // LANES
    for c in range(coeffs):
        for h in range(halves):
            block = get(c, h).astype(jnp.float32)
            spread[h, pl.ds(c, rows_y, stride=coeffs), :] = block


def turn_rows(spread, eye, coeffs, rows_y, cells_z, put):
    halves = cells_z // LANES
    keep = -(-coeffs // 16) * 16
    zeros = jnp.zeros((LANES - keep, cells_z), jnp.bfloat16)
    for y in range(0, rows_y, 2):
        parts = []
        for i in (y, y + 1):
            rows = jnp.concatenate(
                [spread[h, i * coeffs : i * coeffs + keep, :] for h in range(halves)], axis=1
            )
            parts += [rows.astype(jnp.bfloat16), zeros]
        both = lax.dot_general(
            eye[...],
            jnp.concatenate(parts, axis=0),
            (((1,), (1,)), ((), ())),
            preferred_element_type=jnp.float32,
        )
        put(y, both[:, :LANES])
        put(y + 1, both[:, LANES:])


def spread_shape(coeffs, cells_y, cells_z):
    return pltpu.VMEM((cells_z // LANES, cells_y * coeffs + 16, LANES), jnp.float32)


def cut_faces(field):
    coeffs, cells_x, cells_y, cells_z = field.shape
    parts = 9
    per_part = coeffs // parts
    rows = cells_x * HALO

    def kernel(field, pick, last, first, top, bottom, buf, high, low, sems, out_sems):
        def load(i):
            here = pl.ds(i * per_part, per_part)
            return pltpu.make_async_copy(field.at[here], buf.at[here], sems.at[i])

        def saves(i):
            here = pl.ds(i * per_part, per_part)
            return [
                pltpu.make_async_copy(high.at[here], top.at[here], out_sems.at[0, i]),
                pltpu.make_async_copy(low.at[here], bottom.at[here], out_sems.at[1, i]),
                pltpu.make_async_copy(
                    buf.at[here, pl.ds(cells_x - HALO, HALO)], last.at[here], out_sems.at[2, i]
                ),
                pltpu.make_async_copy(
                    buf.at[here, pl.ds(0, HALO)], first.at[here], out_sems.at[3, i]
                ),
            ]

        for i in range(parts):
            load(i).start()

        def body(i, _):
            load(i).wait()
            for k in range(per_part):
                c = i * per_part + k
                chosen = jnp.dot(
                    pick[...],
                    buf[c].reshape(cells_x * cells_y, cells_z),
                    preferred_element_type=jnp.float32,
                ).astype(jnp.bfloat16)
                high[c] = chosen[:rows]
                low[c] = chosen[rows:]
            for save in saves(i):
                save.start()
            return 0

        lax.fori_loop(0, parts, body, 0)
        for i in range(parts):
            for save in saves(i):
                save.wait()

    pick = np.zeros((2 * rows, cells_x * cells_y), np.float32)
    for x in range(cells_x):
        for j in range(HALO):
            pick[x * HALO + j, x * cells_y + cells_y - HALO + j] = 1.0
            pick[rows + x * HALO + j, x * cells_y + j] = 1.0
    shapes = [(coeffs, HALO, cells_y, cells_z)] * 2 + [(coeffs, rows, cells_z)] * 2
    hbm = pl.BlockSpec(memory_space=pl.ANY)
    return pl.pallas_call(
        kernel,
        out_shape=[pltpu.HBM(shape, jnp.bfloat16) for shape in shapes],
        in_specs=[hbm, pl.BlockSpec(memory_space=pltpu.VMEM)],
        out_specs=[hbm] * 4,
        scratch_shapes=[
            pltpu.VMEM(field.shape, jnp.bfloat16),
            pltpu.VMEM((coeffs, rows, cells_z), jnp.bfloat16),
            pltpu.VMEM((coeffs, rows, cells_z), jnp.bfloat16),
            pltpu.SemaphoreType.DMA((parts,)),
            pltpu.SemaphoreType.DMA((4, parts)),
        ],
        compiler_params=pltpu.CompilerParams(vmem_limit_bytes=16 * MIB),
        name="cut_faces",
    )(field, jnp.asarray(pick.astype(jnp.bfloat16)))


def cut_corners(ylo, yhi):
    coeffs, rows, cells_z = ylo.shape
    per_step = 27
    corner = HALO * HALO

    def kernel(ylo, yhi, pick, up, down):
        for c in range(per_step):
            chosen = jnp.dot(
                pick[...],
                jnp.concatenate([ylo[c], yhi[c]], axis=0),
                preferred_element_type=jnp.float32,
            )
            up[c] = chosen[: 2 * corner].astype(jnp.bfloat16)
            down[c] = chosen[2 * corner :].astype(jnp.bfloat16)

    pick = np.zeros((4 * corner, 2 * rows), np.float32)
    for side in range(2):
        for i in range(corner):
            pick[side * corner + i, side * rows + rows - corner + i] = 1.0
            pick[2 * corner + side * corner + i, side * rows + i] = 1.0
    shape = (coeffs, 2 * corner, cells_z)
    face = pl.BlockSpec((per_step, rows, cells_z), lambda i: (i, 0, 0))
    piece = pl.BlockSpec((per_step,) + shape[1:], lambda i: (i, 0, 0))
    return pl.pallas_call(
        kernel,
        out_shape=[pltpu.HBM(shape, jnp.bfloat16)] * 2,
        grid=(coeffs // per_step,),
        in_specs=[face, face, pl.BlockSpec(pick.shape, lambda i: (0, 0))],
        out_specs=[piece, piece],
        compiler_params=pltpu.CompilerParams(vmem_limit_bytes=16 * MIB),
        name="cut_corners",
    )(ylo, yhi, jnp.asarray(pick.astype(jnp.bfloat16)))


def add_planes(table, planes, halves, eye, first_plane, total_rows, edge_lines):
    source = planes[0][0]
    coeffs, cells_y, cells_z = source.shape[0], source.shape[-2], source.shape[-1]
    count = len(planes)
    arrays = []
    for array, _ in planes:
        if not any(array is other for other in arrays):
            arrays.append(array)
    places = [next(i for i, o in enumerate(arrays) if o is array) for array, _ in planes]
    new = table is None

    def kernel(*refs):
        refs = list(refs)
        if not new:
            refs.pop(0)
        inputs = [refs.pop(0) for _ in arrays]
        shared = [refs.pop(0) for _ in halves]
        eye = refs.pop(0)
        table = refs.pop(0)
        edges = [refs.pop(0) for _ in range(2)] if edge_lines else []
        buf, sems, spread = refs[:3]
        copies = []
        for p, ((_, at), place) in enumerate(zip(planes, places)):
            ref = inputs[place] if at is None else inputs[place].at[:, at]
            copies.append(pltpu.make_async_copy(ref, buf.at[p], sems.at[p]))
        for q, piece in enumerate(shared):
            copies.append(pltpu.make_async_copy(piece, refs[3].at[q], refs[4].at[q]))
        for copy in copies:
            copy.start()

        def turn(p):
            def put(y, block):
                at = pl.multiple_of(((first_plane + p) * cells_y + y) * cells_z, 8)
                table[pl.ds(at, cells_z), :] = block

            turn_rows(spread, eye, coeffs, cells_y, cells_z, put)

        def one(p, _):
            first = inputs[0] if planes[0][1] is None else inputs[0].at[:, 0]
            pltpu.make_async_copy(first, buf.at[p], sems.at[p]).wait()
            fill_rows(
                lambda c, h: buf[p, c, :, h * LANES : (h + 1) * LANES],
                spread,
                coeffs,
                cells_y,
                cells_z,
            )
            turn(p)
            return 0

        lax.fori_loop(0, count, one, 0)
        if halves:
            for copy in copies[count:]:
                copy.wait()
            fill_rows(
                lambda c, h: jnp.concatenate(
                    [
                        refs[3][q, c, :, h * LANES : (h + 1) * LANES].astype(jnp.float32)
                        for q in range(2)
                    ],
                    axis=0,
                ),
                spread,
                coeffs,
                cells_y,
                cells_z,
            )
            turn(count)
        for out, start in zip(edges, (0, cells_z - HALO)):
            for j in range(HALO):
                for line in range(0, edge_lines, 16):
                    parts = [
                        table[pl.ds((line + i) * cells_z + start + j, 8, stride=cells_z), :]
                        for i in (0, 8)
                    ]
                    at = j * edge_lines + line
                    out[at : at + 16, :] = jnp.concatenate(parts, axis=0).astype(jnp.bfloat16)

    vmem = pl.BlockSpec(memory_space=pltpu.VMEM)
    hbm = pl.BlockSpec(memory_space=pl.ANY)
    shapes = [pltpu.VMEM((total_rows, LANES), jnp.float32)]
    if edge_lines:
        shapes += [jax.ShapeDtypeStruct((HALO * edge_lines, LANES), jnp.bfloat16)] * 2
    scratch = [
        pltpu.VMEM((count, coeffs, cells_y, cells_z), jnp.bfloat16),
        pltpu.SemaphoreType.DMA((count,)),
        spread_shape(coeffs, cells_y, cells_z),
    ]
    if halves:
        scratch += [
            pltpu.VMEM((2, coeffs, cells_y // 2, cells_z), jnp.bfloat16),
            pltpu.SemaphoreType.DMA((2,)),
        ]
    held = [] if new else [table]
    return pl.pallas_call(
        kernel,
        out_shape=shapes,
        in_specs=[vmem] * len(held) + [hbm] * (len(arrays) + len(halves)) + [vmem],
        out_specs=[vmem] * len(shapes),
        scratch_shapes=scratch,
        input_output_aliases={} if new else {0: 0},
        compiler_params=pltpu.CompilerParams(vmem_limit_bytes=TABLE_LIMIT * MIB),
        cost_estimate=pl.CostEstimate(
            flops=2 * 10**10, transcendentals=0, bytes_accessed=2 * 10**7
        ),
    )(*held, *arrays, *halves, eye)


def cut_ends(zlo, zhi, lines, cells_x, cells_y):
    own = cells_x * cells_y
    half = HALO * cells_y + 2 * HALO * HALO
    rows = 2 * HALO * half

    def kernel(zlo, zhi, pick, up, down):
        both = jnp.concatenate([zlo[...], zhi[...]], axis=0)
        chosen = jnp.dot(pick[...], both, preferred_element_type=jnp.float32)
        up[...] = chosen[:rows].astype(jnp.bfloat16)
        down[...] = chosen[rows:].astype(jnp.bfloat16)

    pick = np.zeros((2 * rows, 2 * HALO * lines), np.float32)
    for side in range(2):
        x = cells_x - HALO if side == 0 else 0
        places = [x * cells_y + i for i in range(HALO * cells_y)]
        for face in range(2):
            at = own + face * cells_y + x * HALO
            places += [at + i for i in range(HALO * HALO)]
        for z in range(2 * HALO):
            for i, place in enumerate(places):
                pick[side * rows + z * half + i, z * lines + place] = 1.0
    vmem = pl.BlockSpec(memory_space=pltpu.VMEM)
    return pl.pallas_call(
        kernel,
        out_shape=[jax.ShapeDtypeStruct((rows, LANES), jnp.bfloat16)] * 2,
        in_specs=[vmem] * 3,
        out_specs=[vmem] * 2,
        compiler_params=pltpu.CompilerParams(vmem_limit_bytes=8 * MIB),
        name="cut_ends",
    )(zlo, zhi, jnp.asarray(pick.astype(jnp.bfloat16)))


TABLE_LIMIT = 24
GROUP = 8
PARTS = 3


def prepare(samples, weights, slot, origin, cells, total):
    count = slot.shape[0]
    cells_x, cells_y, cells_z = cells
    own_lines = cells_x * cells_y
    early = own_lines + 2 * cells_y
    rows = (early + (2 * HALO + 1) * cells_y) * cells_z
    block = 256
    burst = 32
    kinds = (2 + PARTS) * SAMPLES
    corner = HALO * HALO
    end = HALO * cells_y + 2 * corner

    def locate(near_x, near_y, near_z):
        own_x = (near_x >= HALO) & (near_x < HALO + cells_x)
        own_y = (near_y >= HALO) & (near_y < HALO + cells_y)
        low_x = near_x < HALO
        low_y = near_y < HALO
        side_x = jnp.where(low_x, near_x, near_x - HALO - cells_x)
        side_y = jnp.where(low_y, near_y, near_y - HALO - cells_y)
        line_own = (near_x - HALO) * cells_y + near_y - HALO
        line_y = own_lines + jnp.where(low_y, 0, cells_y) + (near_x - HALO) * HALO + side_y
        line_early = jnp.where(own_y, line_own, line_y)
        in_face = side_x * cells_y + near_y - HALO
        in_corner = jnp.where(low_y, 0, corner) + side_x * HALO + side_y
        line_late = early + jnp.where(
            own_y,
            jnp.where(low_x, 0, HALO * cells_y) + in_face,
            2 * HALO * cells_y + jnp.where(low_x, 0, 2 * corner) + in_corner,
        )
        line = jnp.where(own_x, line_early, line_late)
        edge = jnp.where(near_z < HALO, near_z, near_z - cells_z)
        at_end = jnp.where(own_y, in_face, HALO * cells_y + in_corner)
        beyond = jnp.where(
            own_x,
            edge * early + line_early,
            2 * HALO * early + jnp.where(low_x, 0, 2 * HALO * end) + edge * end + at_end,
        )
        inside = (near_z >= HALO) & (near_z < HALO + cells_z)
        return jnp.where(inside, line * cells_z + near_z - HALO, rows + beyond)

    def kernel(origin, slot, samples, weights, eye, join, index, ordered, natural):
        def turn(j, _):
            at = pl.multiple_of(j * block, block)
            near = []
            for d in range(3):
                shift = samples[d, :, pl.ds(at, block)] - origin[d] + HALO
                shift = jnp.where(shift < 0, shift + total[d], shift)
                near.append(jnp.where(shift >= total[d], shift - total[d], shift))
            row = locate(*near)
            pieces = [(row >> 8).astype(jnp.float32), (row & 255).astype(jnp.float32)]
            rest = weights[:, pl.ds(at, block)]
            for _ in range(PARTS):
                piece = rest.astype(jnp.bfloat16).astype(jnp.float32)
                pieces.append(piece)
                rest = rest - piece
            pieces.append(jnp.zeros((LANES - kinds, block), jnp.float32))
            natural[pl.ds(at, block), :] = lax.dot_general(
                eye[...],
                jnp.concatenate(pieces, axis=0).astype(jnp.bfloat16),
                (((1,), (1,)), ((), ())),
                preferred_element_type=jnp.float32,
            )
            return 0

        lax.fori_loop(0, count // block, turn, 0)

        def scatter(j, _):
            at = pl.multiple_of(j * burst, burst)
            mine = slot.at[pl.ds(at, burst)]
            for g in range(0, burst, GROUP):
                tile = natural[pl.ds(at + g, GROUP), :]
                for k in range(GROUP):
                    ordered[pl.ds(mine[g + k], 1), :] = tile[k : k + 1, :]
            return 0

        lax.fori_loop(0, count // burst, scatter, 0)

        def collect(j, _):
            at = pl.multiple_of(j * 4 * LANES, 4 * LANES)
            wide = lax.dot_general(
                join[...],
                ordered[pl.ds(at, 4 * LANES), :].astype(jnp.bfloat16),
                (((1,), (1,)), ((), ())),
                preferred_element_type=jnp.float32,
            ).astype(jnp.int32)
            for i in range(4):
                to = pl.multiple_of((j * 4 + i) * SAMPLES, SAMPLES)
                index[pl.ds(to, SAMPLES), :] = wide[:SAMPLES, i * LANES : (i + 1) * LANES]
            return 0

        lax.fori_loop(0, count // (4 * LANES), collect, 0)

    join = np.zeros((16, LANES), np.float32)
    for s in range(SAMPLES):
        join[s, s] = 256.0
        join[s, SAMPLES + s] = 1.0
    vmem = pl.BlockSpec(memory_space=pltpu.VMEM)
    smem = pl.BlockSpec(memory_space=pltpu.SMEM)
    return pl.pallas_call(
        kernel,
        out_shape=(
            jax.ShapeDtypeStruct((count * SAMPLES // LANES, LANES), jnp.int32),
            jax.ShapeDtypeStruct((count, LANES), jnp.float32),
        ),
        in_specs=[smem, smem, vmem, vmem, vmem, vmem],
        out_specs=(vmem, vmem),
        scratch_shapes=[pltpu.VMEM((count, LANES), jnp.float32)],
        compiler_params=pltpu.CompilerParams(vmem_limit_bytes=12 * MIB),
        cost_estimate=pl.CostEstimate(
            flops=2 * 10**10, transcendentals=0, bytes_accessed=3 * 10**6
        ),
        name="prepare",
    )(
        origin,
        slot,
        samples,
        weights,
        jnp.asarray(np.eye(block, dtype=np.float32).astype(jnp.bfloat16)),
        jnp.asarray(join.astype(jnp.bfloat16)),
    )


def spread_weights(ordered):
    count = ordered.shape[0]
    block = 512

    def kernel(ordered, ones, wide):
        rows = ordered[...].astype(jnp.bfloat16)
        for h in range(0, SAMPLES, 2):
            both = jnp.dot(
                rows, ones[:, h * LANES : (h + 2) * LANES], preferred_element_type=jnp.float32
            )
            for s in range(2):
                for g in range(block // GROUP):
                    to = (g * SAMPLES + h + s) * GROUP
                    wide[to : to + GROUP, :] = both[
                        g * GROUP : (g + 1) * GROUP, s * LANES : (s + 1) * LANES
                    ]

    ones = np.zeros((LANES, SAMPLES * LANES), np.float32)
    for s in range(SAMPLES):
        for p in range(PARTS):
            ones[(2 + p) * SAMPLES + s, s * LANES : (s + 1) * LANES] = 1.0
    return pl.pallas_call(
        kernel,
        out_shape=pltpu.HBM((count * SAMPLES, LANES), jnp.float32),
        grid=(count // block,),
        in_specs=[
            pl.BlockSpec((block, LANES), lambda i: (i, 0)),
            pl.BlockSpec(ones.shape, lambda i: (0, 0)),
        ],
        out_specs=pl.BlockSpec((block * SAMPLES, LANES), lambda i: (i, 0)),
        compiler_params=pltpu.CompilerParams(vmem_limit_bytes=12 * MIB),
        cost_estimate=pl.CostEstimate(
            flops=10**10, transcendentals=0, bytes_accessed=3 * 10**6
        ),
        name="spread_weights",
    )(ordered, jnp.asarray(ones.astype(jnp.bfloat16)))


RING = 4
STREAM = 8
CHUNK = 1024


def gather_rows(index, wide, table, edges, first_edge, coeffs):
    count = wide.shape[0] // SAMPLES
    chunks = index.shape[0] // CHUNK
    per_chunk = CHUNK // SAMPLES
    groups = per_chunk // GROUP
    pairs = count // 32
    half = LANES // 2

    def kernel(index, wide, pick, *refs):
        table, out, local, sems, near, near_sems, rows, staged, out_sems = refs[len(edges) + 1 :]
        sublane = lax.broadcasted_iota(jnp.int32, (GROUP, LANES), 0)
        masks = [sublane == k for k in range(GROUP)]
        used = lax.broadcasted_iota(jnp.int32, (GROUP, LANES), 1) < coeffs

        def fetch(n, slot):
            return pltpu.make_async_copy(
                index.at[pl.ds(pl.multiple_of(n * CHUNK, CHUNK), CHUNK)],
                local.at[slot],
                sems.at[slot],
            )

        def stream(n, slot):
            return pltpu.make_async_copy(
                wide.at[pl.ds(pl.multiple_of(n * CHUNK, CHUNK), CHUNK), :],
                near.at[slot],
                near_sems.at[slot],
            )

        dests = groups // 4

        def save(n):
            here = pl.ds(n * dests, dests)
            return pltpu.make_async_copy(staged.at[here], out.at[here], out_sems.at[n])

        def pack(n):
            span = dests * GROUP
            at = pl.multiple_of(n * span, span)
            part = [rows[q, pl.ds(at, span), :].astype(jnp.bfloat16) for q in range(4)]
            even = jnp.concatenate([part[0], part[2]], axis=1)
            odd = jnp.concatenate([part[1], part[3]], axis=1)
            first = jnp.dot(even, pick[0], preferred_element_type=jnp.float32)
            second = jnp.dot(odd, pick[0], preferred_element_type=jnp.float32)
            third = jnp.dot(even, pick[1], preferred_element_type=jnp.float32)
            third += jnp.dot(odd, pick[2], preferred_element_type=jnp.float32)
            for d in range(dests):
                here = slice(d * GROUP, (d + 1) * GROUP)
                staged[n * dests + d, :16, :] = jnp.concatenate(
                    [first[here], second[here]], axis=0
                ).astype(jnp.bfloat16)
                staged[n * dests + d, 16:, :] = third[here].astype(jnp.bfloat16)

        for b in range(RING - 1):
            fetch(b, b).start()
        for b in range(STREAM - 1):
            stream(b, b).start()

        at = first_edge
        for edge in refs[: len(edges)]:
            table[pl.ds(at, edge.shape[0]), :] = edge[...].astype(jnp.float32)
            at += edge.shape[0]

        def body(i, _):
            for b in range(RING):
                n = i * RING + b
                slot = n % STREAM
                fetch(n, b).wait()
                stream(n, slot).wait()
                ahead = n + RING - 1
                later = n + STREAM - 1

                @pl.when(ahead < chunks)
                def _():
                    fetch(ahead, (b + RING - 1) % RING).start()

                @pl.when(later < chunks)
                def _():
                    stream(later, later % STREAM).start()

                @pl.when(n > 1)
                def _():
                    save(n - 2).start()

                pack(jnp.maximum(n - 1, 0))

                for q in range(groups):
                    total = None
                    for s in range(SAMPLES):
                        merged = None
                        for k in range(GROUP):
                            place = s * per_chunk + q * GROUP + k
                            row = table[pl.ds(local[b, place], GROUP, stride=0), :]
                            merged = row if merged is None else jnp.where(masks[k], row, merged)
                        at = (q * SAMPLES + s) * GROUP
                        term = merged * near[slot, at : at + GROUP, :]
                        total = term if total is None else total + term
                    to = pl.multiple_of((n * (groups // 4) + q // 4) * GROUP, GROUP)
                    rows[q % 4, pl.ds(to, GROUP), :] = jnp.where(used, total, 0.0)
            return 0

        lax.fori_loop(0, chunks // RING, body, 0)

        save(chunks - 2).start()
        pack(chunks - 1)
        save(chunks - 1).start()
        for n in range(chunks):
            save(n).wait()

    pick = np.zeros((3, 2 * LANES, LANES), np.float32)
    for c in range(half):
        pick[0, c, c] = 1.0
        pick[0, LANES + c, half + c] = 1.0
    for c in range(32):
        pick[1, half + c, c] = 1.0
        pick[1, LANES + half + c, 64 + c] = 1.0
        pick[2, half + c, 32 + c] = 1.0
        pick[2, LANES + half + c, 96 + c] = 1.0
    vmem = pl.BlockSpec(memory_space=pltpu.VMEM)
    return pl.pallas_call(
        kernel,
        out_shape=(
            pltpu.VMEM(table.shape, jnp.float32),
            pltpu.HBM((pairs, 24, LANES), jnp.bfloat16),
        ),
        in_specs=[pl.BlockSpec(memory_space=pl.ANY)] * 2 + [vmem] * (2 + len(edges)),
        out_specs=(vmem, pl.BlockSpec(memory_space=pl.ANY)),
        scratch_shapes=[
            pltpu.SMEM((RING, CHUNK), jnp.int32),
            pltpu.SemaphoreType.DMA((RING,)),
            pltpu.VMEM((STREAM, CHUNK, LANES), jnp.float32),
            pltpu.SemaphoreType.DMA((STREAM,)),
            pltpu.VMEM((4, pairs * GROUP, LANES), jnp.float32),
            pltpu.VMEM((pairs, 24, LANES), jnp.bfloat16),
            pltpu.SemaphoreType.DMA((chunks,)),
        ],
        input_output_aliases={3 + len(edges): 0},
        compiler_params=pltpu.CompilerParams(vmem_limit_bytes=24 * MIB),
        cost_estimate=pl.CostEstimate(
            flops=4 * 10**10, transcendentals=0, bytes_accessed=2 * 10**7
        ),
        name="gather_rows",
    )(index, wide, jnp.asarray(pick.astype(jnp.bfloat16)), *edges, table)[1]


def relight(transfer, routed, basis, projector):
    coeffs, count = transfer.shape
    sources, packed, _ = routed.shape
    per_pair = count // sources
    block = 512
    step = block // per_pair

    def kernel(transfer, routed, basis, wide, projector, out):
        low = lax.broadcasted_iota(jnp.int32, (GROUP, LANES), 1) < 64
        parts = []
        for i in range(step):
            head = routed[i, :16, :].astype(jnp.float32)
            first, second = head[:GROUP], head[GROUP:]
            third = routed[i, 16:, :].astype(jnp.float32)
            parts += [
                jnp.where(low, first, pltpu.roll(third, 64, 1)),
                jnp.where(low, second, pltpu.roll(third, 32, 1)),
                jnp.where(low, pltpu.roll(first, 64, 1), third),
                jnp.where(low, pltpu.roll(second, 64, 1), pltpu.roll(third, 96, 1)),
            ]
        rows = jnp.concatenate(parts, axis=0).astype(jnp.bfloat16)
        lit = jnp.dot(basis[...], transfer[...], preferred_element_type=jnp.float32)
        shade = lax.dot_general(
            wide[...], rows, (((1,), (1,)), ((), ())), preferred_element_type=jnp.float32
        )
        product = (lit * shade).astype(jnp.bfloat16)
        out[...] = jnp.dot(projector[...], product, preferred_element_type=jnp.float32).astype(
            jnp.bfloat16
        )

    directions = basis.shape[0]
    wide = np.zeros((directions, LANES), jnp.bfloat16)
    wide[:, :coeffs] = basis
    return pl.pallas_call(
        kernel,
        out_shape=jax.ShapeDtypeStruct((coeffs, count), jnp.bfloat16),
        grid=(count // block,),
        in_specs=[
            pl.BlockSpec((coeffs, block), lambda i: (0, i)),
            pl.BlockSpec((step, packed, LANES), lambda i: (i, 0, 0)),
            pl.BlockSpec((directions, coeffs), lambda i: (0, 0)),
            pl.BlockSpec((directions, LANES), lambda i: (0, 0)),
            pl.BlockSpec((coeffs, directions), lambda i: (0, 0)),
        ],
        out_specs=pl.BlockSpec((coeffs, block), lambda i: (0, i)),
        compiler_params=pltpu.CompilerParams(vmem_limit_bytes=40 * MIB),
        name="relight",
    )(transfer, routed, jnp.asarray(basis), jnp.asarray(wide), jnp.asarray(projector))


def moves(sizes, steps):
    pairs = []
    for x in range(sizes[0]):
        for y in range(sizes[1]):
            to_x, to_y = (x + steps[0]) % sizes[0], (y + steps[1]) % sizes[1]
            pairs.append((x * sizes[1] + y, to_x * sizes[1] + to_y))
    return pairs


def shift(array, axis, pairs):
    return pltpu.with_memory_space_constraint(lax.ppermute(array, axis, pairs), pltpu.HBM)


def halo_step(field, samples, weights, destination, transfer):
    basis, projector = direction_tables()
    coeffs, cells_x, cells_y, cells_z = field.shape
    count = transfer.shape[1]
    along = tuple(lax.axis_size(axis) for axis in ("gx", "gy", "gz"))
    ups = [moves((n, 1), (1, 0)) for n in along]
    downs = [moves((n, 1), (-1, 0)) for n in along]

    cells = (cells_x, cells_y, cells_z)
    total = tuple(c * n for c, n in zip(cells, along))
    origin = jnp.stack(
        [lax.axis_index(axis) * c for axis, c in zip(("gx", "gy", "gz"), cells)]
    ).astype(jnp.int32)
    devices = math.prod(along)
    per_pair = count // devices
    slot = destination[0] * per_pair + destination[1]

    field = pltpu.with_memory_space_constraint(field, pltpu.HBM)
    last, first, top, bottom = cut_faces(field)
    ylo = shift(top, "gy", ups[1])
    yhi = shift(bottom, "gy", downs[1])
    xlo = shift(last, "gx", ups[0])
    xhi = shift(first, "gx", downs[0])
    field, slot, origin = lax.optimization_barrier((field, slot, origin))

    eye = jnp.asarray(np.eye(cells_z, dtype=np.float32).astype(jnp.bfloat16))
    early = (cells_x + 2) * cells_y
    rows = (early + (2 * HALO + 1) * cells_y) * cells_z
    ends = HALO * cells_y + 2 * HALO * HALO
    total_rows = rows + 2 * HALO * (early + 2 * ends)
    own = [(field, x) for x in range(cells_x)]
    table = add_planes(None, own, (), eye, 0, total_rows, 0)[0]
    index, ordered = prepare(samples, weights, slot, origin, cells, total)
    table, index, ordered, ylo, yhi = lax.optimization_barrier((table, index, ordered, ylo, yhi))
    up, down = cut_corners(ylo, yhi)
    up, down, table = lax.optimization_barrier((up, down, table))
    clo = shift(up, "gx", ups[0])
    chi = shift(down, "gx", downs[0])
    table, bottoms, tops = add_planes(
        table, [(ylo, None), (yhi, None)], (), eye, cells_x, total_rows, early
    )
    zhi = lax.ppermute(bottoms, "gz", downs[2])
    zlo = lax.ppermute(tops, "gz", ups[2])
    bottoms, tops, ordered = lax.optimization_barrier((bottoms, tops, ordered))
    wide = spread_weights(ordered)
    zlo, zhi, wide = lax.optimization_barrier((zlo, zhi, wide))
    up, down = cut_ends(zlo, zhi, early, cells_x, cells_y)
    elo = lax.ppermute(up, "gx", ups[0])
    ehi = lax.ppermute(down, "gx", downs[0])
    sides = [(xlo, 0), (xlo, 1), (xhi, 0), (xhi, 1)]
    table = add_planes(table, sides, (clo, chi), eye, cells_x + 2, total_rows, 0)[0]
    outgoing = gather_rows(
        index.reshape(-1), wide, table, (zlo, zhi, elo, ehi), rows, coeffs
    )
    routed = lax.all_to_all(
        outgoing, ("gx", "gy", "gz"), split_axis=0, concat_axis=0, tiled=True
    )
    return relight(transfer, routed, basis, projector)


def solution(mesh):
    placed = (
        P(None, "gx", "gy", "gz"),
        P(None, None, ("gx", "gy", "gz")),
        P(None, ("gx", "gy", "gz")),
        P(None, ("gx", "gy", "gz")),
        P(None, ("gx", "gy", "gz")),
    )
    return jax.shard_map(
        halo_step,
        mesh=mesh,
        in_specs=placed,
        out_specs=P(None, ("gx", "gy", "gz")),
        check_vma=False,
    )
```

```python
import math

import jax
import jax.numpy as jnp
import numpy as np
from jax import lax
from jax.experimental import pallas as pl
from jax.experimental.pallas import tpu as pltpu
from jax.sharding import PartitionSpec as P


HALO = 2
SAMPLES = 8
DEGREES = 9
POLAR = 32
AZIMUTH = 32
LANES = 128
MIB = 1024 * 1024


def harmonic_values():
    polar = (np.arange(POLAR, dtype=np.float64) + 0.5) * (2.0 / POLAR) - 1.0
    beside = (np.arange(AZIMUTH, dtype=np.float64) + 0.5) * (2.0 * math.pi / AZIMUTH)
    cosines = np.repeat(polar, AZIMUTH)
    angles = np.tile(beside, POLAR)
    sines = np.sqrt(np.maximum(1.0 - cosines * cosines, 0.0))
    entries = {}
    for m in range(DEGREES):
        diagonal = (-1.0) ** m * float(math.prod(range(1, 2 * m, 2))) * sines**m
        legendre = {m: diagonal}
        if m + 1 < DEGREES:
            legendre[m + 1] = cosines * (2 * m + 1) * diagonal
        for l in range(m + 2, DEGREES):
            legendre[l] = (
                (2 * l - 1) * cosines * legendre[l - 1] - (l + m - 1) * legendre[l - 2]
            ) / (l - m)
        for l in range(m, DEGREES):
            factor = math.sqrt(
                (2 * l + 1) / (4.0 * math.pi) * math.factorial(l - m) / math.factorial(l + m)
            )
            if m == 0:
                entries[l, 0] = factor * legendre[l]
            else:
                entries[l, m] = math.sqrt(2.0) * factor * np.cos(m * angles) * legendre[l]
                entries[l, -m] = math.sqrt(2.0) * factor * np.sin(m * angles) * legendre[l]
    return np.stack([entries[l, m] for l in range(DEGREES) for m in range(-l, l + 1)])


def direction_tables():
    values = harmonic_values()
    basis = values.T.astype(np.float32).astype(jnp.bfloat16)
    projector = (values * (4.0 * math.pi / (POLAR * AZIMUTH))).astype(np.float32)
    return basis, projector.astype(jnp.bfloat16)


def fill_rows(get, spread, coeffs, rows_y, cells_z):
    halves = cells_z // LANES
    for c in range(coeffs):
        for h in range(halves):
            block = get(c, h).astype(jnp.float32)
            spread[h, pl.ds(c, rows_y, stride=coeffs), :] = block


def turn_rows(spread, eye, coeffs, rows_y, cells_z, put):
    halves = cells_z // LANES
    keep = -(-coeffs // 16) * 16
    zeros = jnp.zeros((LANES - keep, cells_z), jnp.bfloat16)
    for y in range(0, rows_y, 2):
        parts = []
        for i in (y, y + 1):
            rows = jnp.concatenate(
                [spread[h, i * coeffs : i * coeffs + keep, :] for h in range(halves)], axis=1
            )
            parts += [rows.astype(jnp.bfloat16), zeros]
        both = lax.dot_general(
            eye[...],
            jnp.concatenate(parts, axis=0),
            (((1,), (1,)), ((), ())),
            preferred_element_type=jnp.float32,
        )
        put(y, both[:, :LANES])
        put(y + 1, both[:, LANES:])


def spread_shape(coeffs, cells_y, cells_z):
    return pltpu.VMEM((cells_z // LANES, cells_y * coeffs + 16, LANES), jnp.float32)


def cut_faces(field):
    coeffs, cells_x, cells_y, cells_z = field.shape
    parts = 9
    per_part = coeffs // parts
    rows = cells_x * HALO

    def kernel(field, pick, last, first, top, bottom, buf, high, low, sems, out_sems):
        def load(i):
            here = pl.ds(i * per_part, per_part)
            return pltpu.make_async_copy(field.at[here], buf.at[here], sems.at[i])

        def saves(i):
            here = pl.ds(i * per_part, per_part)
            return [
                pltpu.make_async_copy(high.at[here], top.at[here], out_sems.at[0, i]),
                pltpu.make_async_copy(low.at[here], bottom.at[here], out_sems.at[1, i]),
                pltpu.make_async_copy(
                    buf.at[here, pl.ds(cells_x - HALO, HALO)], last.at[here], out_sems.at[2, i]
                ),
                pltpu.make_async_copy(
                    buf.at[here, pl.ds(0, HALO)], first.at[here], out_sems.at[3, i]
                ),
            ]

        for i in range(parts):
            load(i).start()

        def body(i, _):
            load(i).wait()
            for k in range(per_part):
                c = i * per_part + k
                chosen = jnp.dot(
                    pick[...],
                    buf[c].reshape(cells_x * cells_y, cells_z),
                    preferred_element_type=jnp.float32,
                ).astype(jnp.bfloat16)
                high[c] = chosen[:rows]
                low[c] = chosen[rows:]
            for save in saves(i):
                save.start()
            return 0

        lax.fori_loop(0, parts, body, 0)
        for i in range(parts):
            for save in saves(i):
                save.wait()

    pick = np.zeros((2 * rows, cells_x * cells_y), np.float32)
    for x in range(cells_x):
        for j in range(HALO):
            pick[x * HALO + j, x * cells_y + cells_y - HALO + j] = 1.0
            pick[rows + x * HALO + j, x * cells_y + j] = 1.0
    shapes = [(coeffs, HALO, cells_y, cells_z)] * 2 + [(coeffs, rows, cells_z)] * 2
    hbm = pl.BlockSpec(memory_space=pl.ANY)
    return pl.pallas_call(
        kernel,
        out_shape=[pltpu.HBM(shape, jnp.bfloat16) for shape in shapes],
        in_specs=[hbm, pl.BlockSpec(memory_space=pltpu.VMEM)],
        out_specs=[hbm] * 4,
        scratch_shapes=[
            pltpu.VMEM(field.shape, jnp.bfloat16),
            pltpu.VMEM((coeffs, rows, cells_z), jnp.bfloat16),
            pltpu.VMEM((coeffs, rows, cells_z), jnp.bfloat16),
            pltpu.SemaphoreType.DMA((parts,)),
            pltpu.SemaphoreType.DMA((4, parts)),
        ],
        compiler_params=pltpu.CompilerParams(vmem_limit_bytes=16 * MIB),
        name="cut_faces",
    )(field, jnp.asarray(pick.astype(jnp.bfloat16)))


def cut_corners(ylo, yhi):
    coeffs, rows, cells_z = ylo.shape
    per_step = 27
    corner = HALO * HALO

    def kernel(ylo, yhi, pick, up, down):
        for c in range(per_step):
            chosen = jnp.dot(
                pick[...],
                jnp.concatenate([ylo[c], yhi[c]], axis=0),
                preferred_element_type=jnp.float32,
            )
            up[c] = chosen[: 2 * corner].astype(jnp.bfloat16)
            down[c] = chosen[2 * corner :].astype(jnp.bfloat16)

    pick = np.zeros((4 * corner, 2 * rows), np.float32)
    for side in range(2):
        for i in range(corner):
            pick[side * corner + i, side * rows + rows - corner + i] = 1.0
            pick[2 * corner + side * corner + i, side * rows + i] = 1.0
    shape = (coeffs, 2 * corner, cells_z)
    face = pl.BlockSpec((per_step, rows, cells_z), lambda i: (i, 0, 0))
    piece = pl.BlockSpec((per_step,) + shape[1:], lambda i: (i, 0, 0))
    return pl.pallas_call(
        kernel,
        out_shape=[pltpu.HBM(shape, jnp.bfloat16)] * 2,
        grid=(coeffs // per_step,),
        in_specs=[face, face, pl.BlockSpec(pick.shape, lambda i: (0, 0))],
        out_specs=[piece, piece],
        compiler_params=pltpu.CompilerParams(vmem_limit_bytes=16 * MIB),
        name="cut_corners",
    )(ylo, yhi, jnp.asarray(pick.astype(jnp.bfloat16)))


def add_planes(table, planes, halves, eye, first_plane, total_rows, edge_lines):
    source = planes[0][0]
    coeffs, cells_y, cells_z = source.shape[0], source.shape[-2], source.shape[-1]
    count = len(planes)
    arrays = []
    for array, _ in planes:
        if not any(array is other for other in arrays):
            arrays.append(array)
    places = [next(i for i, o in enumerate(arrays) if o is array) for array, _ in planes]
    new = table is None

    def kernel(*refs):
        refs = list(refs)
        if not new:
            refs.pop(0)
        inputs = [refs.pop(0) for _ in arrays]
        shared = [refs.pop(0) for _ in halves]
        eye_in = refs.pop(0)
        table = refs.pop(0)
        edges = [refs.pop(0) for _ in range(2)] if edge_lines else []
        eye, eye_sem, buf, sems, spread = refs[:5]
        refs = refs[2:]
        copies = []
        for p, ((_, at), place) in enumerate(zip(planes, places)):
            ref = inputs[place] if at is None else inputs[place].at[:, at]
            copies.append(pltpu.make_async_copy(ref, buf.at[p], sems.at[p]))
        for q, piece in enumerate(shared):
            copies.append(pltpu.make_async_copy(piece, refs[3].at[q], refs[4].at[q]))
        for copy in copies:
            copy.start()
        eye_copy = pltpu.make_async_copy(eye_in, eye, eye_sem)
        eye_copy.start()
        eye_copy.wait()

        def turn(p):
            def put(y, block):
                at = pl.multiple_of(((first_plane + p) * cells_y + y) * cells_z, 8)
                table[pl.ds(at, cells_z), :] = block

            turn_rows(spread, eye, coeffs, cells_y, cells_z, put)

        def one(p, _):
            first = inputs[0] if planes[0][1] is None else inputs[0].at[:, 0]
            pltpu.make_async_copy(first, buf.at[p], sems.at[p]).wait()
            fill_rows(
                lambda c, h: buf[p, c, :, h * LANES : (h + 1) * LANES],
                spread,
                coeffs,
                cells_y,
                cells_z,
            )
            turn(p)
            return 0

        lax.fori_loop(0, count, one, 0)
        if halves:
            for copy in copies[count:]:
                copy.wait()
            fill_rows(
                lambda c, h: jnp.concatenate(
                    [
                        refs[3][q, c, :, h * LANES : (h + 1) * LANES].astype(jnp.float32)
                        for q in range(2)
                    ],
                    axis=0,
                ),
                spread,
                coeffs,
                cells_y,
                cells_z,
            )
            turn(count)
        for out, start in zip(edges, (0, cells_z - HALO)):
            for j in range(HALO):
                for line in range(0, edge_lines, 16):
                    parts = [
                        table[pl.ds((line + i) * cells_z + start + j, 8, stride=cells_z), :]
                        for i in (0, 8)
                    ]
                    at = j * edge_lines + line
                    out[at : at + 16, :] = jnp.concatenate(parts, axis=0).astype(jnp.bfloat16)

    vmem = pl.BlockSpec(memory_space=pltpu.VMEM)
    hbm = pl.BlockSpec(memory_space=pl.ANY)
    shapes = [pltpu.VMEM((total_rows, LANES), jnp.float32)]
    if edge_lines:
        shapes += [jax.ShapeDtypeStruct((HALO * edge_lines, LANES), jnp.bfloat16)] * 2
    scratch = [
        pltpu.VMEM(eye.shape, eye.dtype),
        pltpu.SemaphoreType.DMA(()),
        pltpu.VMEM((count, coeffs, cells_y, cells_z), jnp.bfloat16),
        pltpu.SemaphoreType.DMA((count,)),
        spread_shape(coeffs, cells_y, cells_z),
    ]
    if halves:
        scratch += [
            pltpu.VMEM((2, coeffs, cells_y // 2, cells_z), jnp.bfloat16),
            pltpu.SemaphoreType.DMA((2,)),
        ]
    held = [] if new else [table]
    return pl.pallas_call(
        kernel,
        out_shape=shapes,
        in_specs=[vmem] * len(held) + [hbm] * (len(arrays) + len(halves) + 1),
        out_specs=[vmem] * len(shapes),
        scratch_shapes=scratch,
        input_output_aliases={} if new else {0: 0},
        compiler_params=pltpu.CompilerParams(vmem_limit_bytes=TABLE_LIMIT * MIB),
        cost_estimate=pl.CostEstimate(
            flops=2 * 10**10, transcendentals=0, bytes_accessed=2 * 10**7
        ),
    )(*held, *arrays, *halves, eye)


def cut_ends(zlo, zhi, lines, cells_x, cells_y):
    own = cells_x * cells_y
    half = HALO * cells_y + 2 * HALO * HALO
    rows = 2 * HALO * half

    def kernel(zlo, zhi, pick, up, down):
        both = jnp.concatenate([zlo[...], zhi[...]], axis=0)
        chosen = jnp.dot(pick[...], both, preferred_element_type=jnp.float32)
        up[...] = chosen[:rows].astype(jnp.bfloat16)
        down[...] = chosen[rows:].astype(jnp.bfloat16)

    pick = np.zeros((2 * rows, 2 * HALO * lines), np.float32)
    for side in range(2):
        x = cells_x - HALO if side == 0 else 0
        places = [x * cells_y + i for i in range(HALO * cells_y)]
        for face in range(2):
            at = own + face * cells_y + x * HALO
            places += [at + i for i in range(HALO * HALO)]
        for z in range(2 * HALO):
            for i, place in enumerate(places):
                pick[side * rows + z * half + i, z * lines + place] = 1.0
    vmem = pl.BlockSpec(memory_space=pltpu.VMEM)
    return pl.pallas_call(
        kernel,
        out_shape=[jax.ShapeDtypeStruct((rows, LANES), jnp.bfloat16)] * 2,
        in_specs=[vmem] * 3,
        out_specs=[vmem] * 2,
        compiler_params=pltpu.CompilerParams(vmem_limit_bytes=8 * MIB),
        name="cut_ends",
    )(zlo, zhi, jnp.asarray(pick.astype(jnp.bfloat16)))


TABLE_LIMIT = 24
GROUP = 8
PARTS = 3


def prepare(samples, weights, slot, origin, cells, total):
    count = slot.shape[0]
    cells_x, cells_y, cells_z = cells
    own_lines = cells_x * cells_y
    early = own_lines + 2 * cells_y
    rows = (early + (2 * HALO + 1) * cells_y) * cells_z
    block = 256
    burst = 32
    kinds = (2 + PARTS) * SAMPLES
    corner = HALO * HALO
    end = HALO * cells_y + 2 * corner

    def locate(near_x, near_y, near_z):
        own_x = (near_x >= HALO) & (near_x < HALO + cells_x)
        own_y = (near_y >= HALO) & (near_y < HALO + cells_y)
        low_x = near_x < HALO
        low_y = near_y < HALO
        side_x = jnp.where(low_x, near_x, near_x - HALO - cells_x)
        side_y = jnp.where(low_y, near_y, near_y - HALO - cells_y)
        line_own = (near_x - HALO) * cells_y + near_y - HALO
        line_y = own_lines + jnp.where(low_y, 0, cells_y) + (near_x - HALO) * HALO + side_y
        line_early = jnp.where(own_y, line_own, line_y)
        in_face = side_x * cells_y + near_y - HALO
        in_corner = jnp.where(low_y, 0, corner) + side_x * HALO + side_y
        line_late = early + jnp.where(
            own_y,
            jnp.where(low_x, 0, HALO * cells_y) + in_face,
            2 * HALO * cells_y + jnp.where(low_x, 0, 2 * corner) + in_corner,
        )
        line = jnp.where(own_x, line_early, line_late)
        edge = jnp.where(near_z < HALO, near_z, near_z - cells_z)
        at_end = jnp.where(own_y, in_face, HALO * cells_y + in_corner)
        beyond = jnp.where(
            own_x,
            edge * early + line_early,
            2 * HALO * early + jnp.where(low_x, 0, 2 * HALO * end) + edge * end + at_end,
        )
        inside = (near_z >= HALO) & (near_z < HALO + cells_z)
        return jnp.where(inside, line * cells_z + near_z - HALO, rows + beyond)

    def kernel(origin, slot, samples, weights, eye, join, index, ordered, natural):
        def turn(j, _):
            at = pl.multiple_of(j * block, block)
            near = []
            for d in range(3):
                shift = samples[d, :, pl.ds(at, block)] - origin[d] + HALO
                shift = jnp.where(shift < 0, shift + total[d], shift)
                near.append(jnp.where(shift >= total[d], shift - total[d], shift))
            row = locate(*near)
            pieces = [(row >> 8).astype(jnp.float32), (row & 255).astype(jnp.float32)]
            rest = weights[:, pl.ds(at, block)]
            for _ in range(PARTS):
                piece = rest.astype(jnp.bfloat16).astype(jnp.float32)
                pieces.append(piece)
                rest = rest - piece
            pieces.append(jnp.zeros((LANES - kinds, block), jnp.float32))
            natural[pl.ds(at, block), :] = lax.dot_general(
                eye[...],
                jnp.concatenate(pieces, axis=0).astype(jnp.bfloat16),
                (((1,), (1,)), ((), ())),
                preferred_element_type=jnp.float32,
            )
            return 0

        lax.fori_loop(0, count // block, turn, 0)

        def scatter(j, _):
            at = pl.multiple_of(j * burst, burst)
            mine = slot.at[pl.ds(at, burst)]
            for g in range(0, burst, GROUP):
                tile = natural[pl.ds(at + g, GROUP), :]
                for k in range(GROUP):
                    ordered[pl.ds(mine[g + k], 1), :] = tile[k : k + 1, :]
            return 0

        lax.fori_loop(0, count // burst, scatter, 0)

        def collect(j, _):
            at = pl.multiple_of(j * 4 * LANES, 4 * LANES)
            wide = lax.dot_general(
                join[...],
                ordered[pl.ds(at, 4 * LANES), :].astype(jnp.bfloat16),
                (((1,), (1,)), ((), ())),
                preferred_element_type=jnp.float32,
            ).astype(jnp.int32)
            for i in range(4):
                to = pl.multiple_of((j * 4 + i) * SAMPLES, SAMPLES)
                index[pl.ds(to, SAMPLES), :] = wide[:SAMPLES, i * LANES : (i + 1) * LANES]
            return 0

        lax.fori_loop(0, count // (4 * LANES), collect, 0)

    join = np.zeros((16, LANES), np.float32)
    for s in range(SAMPLES):
        join[s, s] = 256.0
        join[s, SAMPLES + s] = 1.0
    vmem = pl.BlockSpec(memory_space=pltpu.VMEM)
    smem = pl.BlockSpec(memory_space=pltpu.SMEM)
    return pl.pallas_call(
        kernel,
        out_shape=(
            jax.ShapeDtypeStruct((count * SAMPLES // LANES, LANES), jnp.int32),
            jax.ShapeDtypeStruct((count, LANES), jnp.float32),
        ),
        in_specs=[smem, smem, vmem, vmem, vmem, vmem],
        out_specs=(vmem, vmem),
        scratch_shapes=[pltpu.VMEM((count, LANES), jnp.float32)],
        compiler_params=pltpu.CompilerParams(vmem_limit_bytes=12 * MIB),
        cost_estimate=pl.CostEstimate(
            flops=2 * 10**10, transcendentals=0, bytes_accessed=3 * 10**6
        ),
        name="prepare",
    )(
        origin,
        slot,
        samples,
        weights,
        jnp.asarray(np.eye(block, dtype=np.float32).astype(jnp.bfloat16)),
        jnp.asarray(join.astype(jnp.bfloat16)),
    )


def spread_weights(ordered):
    count = ordered.shape[0]
    block = 512

    def kernel(ordered, ones, wide):
        rows = ordered[...].astype(jnp.bfloat16)
        for h in range(0, SAMPLES, 2):
            both = jnp.dot(
                rows, ones[:, h * LANES : (h + 2) * LANES], preferred_element_type=jnp.float32
            )
            for s in range(2):
                for g in range(block // GROUP):
                    to = (g * SAMPLES + h + s) * GROUP
                    wide[to : to + GROUP, :] = both[
                        g * GROUP : (g + 1) * GROUP, s * LANES : (s + 1) * LANES
                    ]

    ones = np.zeros((LANES, SAMPLES * LANES), np.float32)
    for s in range(SAMPLES):
        for p in range(PARTS):
            ones[(2 + p) * SAMPLES + s, s * LANES : (s + 1) * LANES] = 1.0
    return pl.pallas_call(
        kernel,
        out_shape=pltpu.HBM((count * SAMPLES, LANES), jnp.float32),
        grid=(count // block,),
        in_specs=[
            pl.BlockSpec((block, LANES), lambda i: (i, 0)),
            pl.BlockSpec(ones.shape, lambda i: (0, 0)),
        ],
        out_specs=pl.BlockSpec((block * SAMPLES, LANES), lambda i: (i, 0)),
        compiler_params=pltpu.CompilerParams(vmem_limit_bytes=12 * MIB),
        cost_estimate=pl.CostEstimate(
            flops=10**10, transcendentals=0, bytes_accessed=3 * 10**6
        ),
        name="spread_weights",
    )(ordered, jnp.asarray(ones.astype(jnp.bfloat16)))


RING = 4
STREAM = 8
CHUNK = 1024


def gather_rows(index, wide, table, edges, first_edge, coeffs):
    count = wide.shape[0] // SAMPLES
    chunks = index.shape[0] // CHUNK
    per_chunk = CHUNK // SAMPLES
    groups = per_chunk // GROUP
    pairs = count // 32
    half = LANES // 2

    def kernel(index, wide, pick_in, *refs):
        scratch = refs[len(edges) + 1 :]
        table, out, local, sems, near, near_sems, rows, staged, out_sems = scratch[:9]
        side_sems, pick, *held = scratch[9:]
        sublane = lax.broadcasted_iota(jnp.int32, (GROUP, LANES), 0)
        masks = [sublane == k for k in range(GROUP)]
        used = lax.broadcasted_iota(jnp.int32, (GROUP, LANES), 1) < coeffs

        def fetch(n, slot):
            return pltpu.make_async_copy(
                index.at[pl.ds(pl.multiple_of(n * CHUNK, CHUNK), CHUNK)],
                local.at[slot],
                sems.at[slot],
            )

        def stream(n, slot):
            return pltpu.make_async_copy(
                wide.at[pl.ds(pl.multiple_of(n * CHUNK, CHUNK), CHUNK), :],
                near.at[slot],
                near_sems.at[slot],
            )

        dests = groups // 4

        def save(n):
            here = pl.ds(n * dests, dests)
            return pltpu.make_async_copy(staged.at[here], out.at[here], out_sems.at[n])

        def pack(n):
            span = dests * GROUP
            at = pl.multiple_of(n * span, span)
            part = [rows[q, pl.ds(at, span), :].astype(jnp.bfloat16) for q in range(4)]
            even = jnp.concatenate([part[0], part[2]], axis=1)
            odd = jnp.concatenate([part[1], part[3]], axis=1)
            first = jnp.dot(even, pick[0], preferred_element_type=jnp.float32)
            second = jnp.dot(odd, pick[0], preferred_element_type=jnp.float32)
            third = jnp.dot(even, pick[1], preferred_element_type=jnp.float32)
            third += jnp.dot(odd, pick[2], preferred_element_type=jnp.float32)
            for d in range(dests):
                here = slice(d * GROUP, (d + 1) * GROUP)
                staged[n * dests + d, :16, :] = jnp.concatenate(
                    [first[here], second[here]], axis=0
                ).astype(jnp.bfloat16)
                staged[n * dests + d, 16:, :] = third[here].astype(jnp.bfloat16)

        for b in range(RING - 1):
            fetch(b, b).start()
        for b in range(STREAM - 1):
            stream(b, b).start()

        sides = [
            pltpu.make_async_copy(source, target, side_sems.at[i])
            for i, (source, target) in enumerate(zip(refs[: len(edges)], held))
        ]
        sides.append(pltpu.make_async_copy(pick_in, pick, side_sems.at[len(edges)]))
        for side in sides:
            side.start()
        for side in sides:
            side.wait()
        at = first_edge
        for edge in held:
            table[pl.ds(at, edge.shape[0]), :] = edge[...].astype(jnp.float32)
            at += edge.shape[0]

        def body(i, _):
            for b in range(RING):
                n = i * RING + b
                slot = n % STREAM
                fetch(n, b).wait()
                stream(n, slot).wait()
                ahead = n + RING - 1
                later = n + STREAM - 1

                @pl.when(ahead < chunks)
                def _():
                    fetch(ahead, (b + RING - 1) % RING).start()

                @pl.when(later < chunks)
                def _():
                    stream(later, later % STREAM).start()

                @pl.when(n > 1)
                def _():
                    save(n - 2).start()

                pack(jnp.maximum(n - 1, 0))

                for q in range(groups):
                    total = None
                    for s in range(SAMPLES):
                        merged = None
                        for k in range(GROUP):
                            place = s * per_chunk + q * GROUP + k
                            row = table[pl.ds(local[b, place], GROUP, stride=0), :]
                            merged = row if merged is None else jnp.where(masks[k], row, merged)
                        at = (q * SAMPLES + s) * GROUP
                        term = merged * near[slot, at : at + GROUP, :]
                        total = term if total is None else total + term
                    to = pl.multiple_of((n * (groups // 4) + q // 4) * GROUP, GROUP)
                    rows[q % 4, pl.ds(to, GROUP), :] = jnp.where(used, total, 0.0)
            return 0

        lax.fori_loop(0, chunks // RING, body, 0)

        save(chunks - 2).start()
        pack(chunks - 1)
        save(chunks - 1).start()
        for n in range(chunks):
            save(n).wait()

    pick = np.zeros((3, 2 * LANES, LANES), np.float32)
    for c in range(half):
        pick[0, c, c] = 1.0
        pick[0, LANES + c, half + c] = 1.0
    for c in range(32):
        pick[1, half + c, c] = 1.0
        pick[1, LANES + half + c, 64 + c] = 1.0
        pick[2, half + c, 32 + c] = 1.0
        pick[2, LANES + half + c, 96 + c] = 1.0
    vmem = pl.BlockSpec(memory_space=pltpu.VMEM)
    return pl.pallas_call(
        kernel,
        out_shape=(
            pltpu.VMEM(table.shape, jnp.float32),
            pltpu.HBM((pairs, 24, LANES), jnp.bfloat16),
        ),
        in_specs=[pl.BlockSpec(memory_space=pl.ANY)] * (3 + len(edges)) + [vmem],
        out_specs=(vmem, pl.BlockSpec(memory_space=pl.ANY)),
        scratch_shapes=[
            pltpu.SMEM((RING, CHUNK), jnp.int32),
            pltpu.SemaphoreType.DMA((RING,)),
            pltpu.VMEM((STREAM, CHUNK, LANES), jnp.float32),
            pltpu.SemaphoreType.DMA((STREAM,)),
            pltpu.VMEM((4, pairs * GROUP, LANES), jnp.float32),
            pltpu.VMEM((pairs, 24, LANES), jnp.bfloat16),
            pltpu.SemaphoreType.DMA((chunks,)),
            pltpu.SemaphoreType.DMA((len(edges) + 1,)),
            pltpu.VMEM(pick.shape, jnp.bfloat16),
            *(pltpu.VMEM(edge.shape, edge.dtype) for edge in edges),
        ],
        input_output_aliases={3 + len(edges): 0},
        compiler_params=pltpu.CompilerParams(vmem_limit_bytes=24 * MIB),
        cost_estimate=pl.CostEstimate(
            flops=4 * 10**10, transcendentals=0, bytes_accessed=2 * 10**7
        ),
        name="gather_rows",
    )(index, wide, jnp.asarray(pick.astype(jnp.bfloat16)), *edges, table)[1]


def relight(transfer, routed, basis, projector):
    coeffs, count = transfer.shape
    sources, packed, _ = routed.shape
    per_pair = count // sources
    block = 512
    step = block // per_pair

    def kernel(transfer, routed, basis, wide, projector, out):
        low = lax.broadcasted_iota(jnp.int32, (GROUP, LANES), 1) < 64
        parts = []
        for i in range(step):
            head = routed[i, :16, :].astype(jnp.float32)
            first, second = head[:GROUP], head[GROUP:]
            third = routed[i, 16:, :].astype(jnp.float32)
            parts += [
                jnp.where(low, first, pltpu.roll(third, 64, 1)),
                jnp.where(low, second, pltpu.roll(third, 32, 1)),
                jnp.where(low, pltpu.roll(first, 64, 1), third),
                jnp.where(low, pltpu.roll(second, 64, 1), pltpu.roll(third, 96, 1)),
            ]
        rows = jnp.concatenate(parts, axis=0).astype(jnp.bfloat16)
        lit = jnp.dot(basis[...], transfer[...], preferred_element_type=jnp.float32)
        shade = lax.dot_general(
            wide[...], rows, (((1,), (1,)), ((), ())), preferred_element_type=jnp.float32
        )
        product = (lit * shade).astype(jnp.bfloat16)
        out[...] = jnp.dot(projector[...], product, preferred_element_type=jnp.float32).astype(
            jnp.bfloat16
        )

    directions = basis.shape[0]
    wide = np.zeros((directions, LANES), jnp.bfloat16)
    wide[:, :coeffs] = basis
    return pl.pallas_call(
        kernel,
        out_shape=jax.ShapeDtypeStruct((coeffs, count), jnp.bfloat16),
        grid=(count // block,),
        in_specs=[
            pl.BlockSpec((coeffs, block), lambda i: (0, i)),
            pl.BlockSpec((step, packed, LANES), lambda i: (i, 0, 0)),
            pl.BlockSpec((directions, coeffs), lambda i: (0, 0)),
            pl.BlockSpec((directions, LANES), lambda i: (0, 0)),
            pl.BlockSpec((coeffs, directions), lambda i: (0, 0)),
        ],
        out_specs=pl.BlockSpec((coeffs, block), lambda i: (0, i)),
        compiler_params=pltpu.CompilerParams(vmem_limit_bytes=40 * MIB),
        name="relight",
    )(transfer, routed, jnp.asarray(basis), jnp.asarray(wide), jnp.asarray(projector))


def moves(sizes, steps):
    pairs = []
    for x in range(sizes[0]):
        for y in range(sizes[1]):
            to_x, to_y = (x + steps[0]) % sizes[0], (y + steps[1]) % sizes[1]
            pairs.append((x * sizes[1] + y, to_x * sizes[1] + to_y))
    return pairs


def shift(array, axis, pairs):
    return pltpu.with_memory_space_constraint(lax.ppermute(array, axis, pairs), pltpu.HBM)


def halo_step(field, samples, weights, destination, transfer):
    basis, projector = direction_tables()
    coeffs, cells_x, cells_y, cells_z = field.shape
    count = transfer.shape[1]
    along = tuple(lax.axis_size(axis) for axis in ("gx", "gy", "gz"))
    ups = [moves((n, 1), (1, 0)) for n in along]
    downs = [moves((n, 1), (-1, 0)) for n in along]

    cells = (cells_x, cells_y, cells_z)
    total = tuple(c * n for c, n in zip(cells, along))
    origin = jnp.stack(
        [lax.axis_index(axis) * c for axis, c in zip(("gx", "gy", "gz"), cells)]
    ).astype(jnp.int32)
    devices = math.prod(along)
    per_pair = count // devices
    slot = destination[0] * per_pair + destination[1]

    field = pltpu.with_memory_space_constraint(field, pltpu.HBM)
    last, first, top, bottom = cut_faces(field)
    ylo = shift(top, "gy", ups[1])
    yhi = shift(bottom, "gy", downs[1])
    xlo = shift(last, "gx", ups[0])
    xhi = shift(first, "gx", downs[0])
    field, slot, origin = lax.optimization_barrier((field, slot, origin))

    eye = jnp.asarray(np.eye(cells_z, dtype=np.float32).astype(jnp.bfloat16))
    early = (cells_x + 2) * cells_y
    rows = (early + (2 * HALO + 1) * cells_y) * cells_z
    ends = HALO * cells_y + 2 * HALO * HALO
    total_rows = rows + 2 * HALO * (early + 2 * ends)
    own = [(field, x) for x in range(cells_x)]
    table = add_planes(None, own, (), eye, 0, total_rows, 0)[0]
    index, ordered = prepare(samples, weights, slot, origin, cells, total)
    table, index, ordered, ylo, yhi = lax.optimization_barrier((table, index, ordered, ylo, yhi))
    up, down = cut_corners(ylo, yhi)
    up, down, table = lax.optimization_barrier((up, down, table))
    clo = shift(up, "gx", ups[0])
    chi = shift(down, "gx", downs[0])
    table, bottoms, tops = add_planes(
        table, [(ylo, None), (yhi, None)], (), eye, cells_x, total_rows, early
    )
    zhi = lax.ppermute(bottoms, "gz", downs[2])
    zlo = lax.ppermute(tops, "gz", ups[2])
    bottoms, tops, ordered = lax.optimization_barrier((bottoms, tops, ordered))
    wide = spread_weights(ordered)
    zlo, zhi, wide = lax.optimization_barrier((zlo, zhi, wide))
    up, down = cut_ends(zlo, zhi, early, cells_x, cells_y)
    elo = lax.ppermute(up, "gx", ups[0])
    ehi = lax.ppermute(down, "gx", downs[0])
    sides = [(xlo, 0), (xlo, 1), (xhi, 0), (xhi, 1)]
    table = add_planes(table, sides, (clo, chi), eye, cells_x + 2, total_rows, 0)[0]
    outgoing = gather_rows(
        index.reshape(-1), wide, table, (zlo, zhi, elo, ehi), rows, coeffs
    )
    routed = lax.all_to_all(
        outgoing, ("gx", "gy", "gz"), split_axis=0, concat_axis=0, tiled=True
    )
    return relight(transfer, routed, basis, projector)


def solution(mesh):
    placed = (
        P(None, "gx", "gy", "gz"),
        P(None, None, ("gx", "gy", "gz")),
        P(None, ("gx", "gy", "gz")),
        P(None, ("gx", "gy", "gz")),
        P(None, ("gx", "gy", "gz")),
    )
    return jax.shard_map(
        halo_step,
        mesh=mesh,
        in_specs=placed,
        out_specs=P(None, ("gx", "gy", "gz")),
        check_vma=False,
    )
```

```python
import math

import jax
import jax.numpy as jnp
import numpy as np
from jax import lax
from jax.experimental import pallas as pl
from jax.experimental.pallas import tpu as pltpu
from jax.sharding import PartitionSpec as P


HALO = 2
SAMPLES = 8
DEGREES = 9
POLAR = 32
AZIMUTH = 32
LANES = 128
MIB = 1024 * 1024


def harmonic_values():
    polar = (np.arange(POLAR, dtype=np.float64) + 0.5) * (2.0 / POLAR) - 1.0
    beside = (np.arange(AZIMUTH, dtype=np.float64) + 0.5) * (2.0 * math.pi / AZIMUTH)
    cosines = np.repeat(polar, AZIMUTH)
    angles = np.tile(beside, POLAR)
    sines = np.sqrt(np.maximum(1.0 - cosines * cosines, 0.0))
    entries = {}
    for m in range(DEGREES):
        diagonal = (-1.0) ** m * float(math.prod(range(1, 2 * m, 2))) * sines**m
        legendre = {m: diagonal}
        if m + 1 < DEGREES:
            legendre[m + 1] = cosines * (2 * m + 1) * diagonal
        for l in range(m + 2, DEGREES):
            legendre[l] = (
                (2 * l - 1) * cosines * legendre[l - 1] - (l + m - 1) * legendre[l - 2]
            ) / (l - m)
        for l in range(m, DEGREES):
            factor = math.sqrt(
                (2 * l + 1) / (4.0 * math.pi) * math.factorial(l - m) / math.factorial(l + m)
            )
            if m == 0:
                entries[l, 0] = factor * legendre[l]
            else:
                entries[l, m] = math.sqrt(2.0) * factor * np.cos(m * angles) * legendre[l]
                entries[l, -m] = math.sqrt(2.0) * factor * np.sin(m * angles) * legendre[l]
    return np.stack([entries[l, m] for l in range(DEGREES) for m in range(-l, l + 1)])


def direction_tables():
    values = harmonic_values()
    basis = values.T.astype(np.float32).astype(jnp.bfloat16)
    projector = (values * (4.0 * math.pi / (POLAR * AZIMUTH))).astype(np.float32)
    return basis, projector.astype(jnp.bfloat16)


def fill_rows(get, spread, coeffs, rows_y, cells_z):
    halves = cells_z // LANES
    for c in range(coeffs):
        for h in range(halves):
            block = get(c, h).astype(jnp.float32)
            spread[h, pl.ds(c, rows_y, stride=coeffs), :] = block


def turn_rows(spread, eye, coeffs, rows_y, cells_z, put):
    halves = cells_z // LANES
    keep = -(-coeffs // 16) * 16
    zeros = jnp.zeros((LANES - keep, cells_z), jnp.bfloat16)
    for y in range(0, rows_y, 2):
        parts = []
        for i in (y, y + 1):
            rows = jnp.concatenate(
                [spread[h, i * coeffs : i * coeffs + keep, :] for h in range(halves)], axis=1
            )
            parts += [rows.astype(jnp.bfloat16), zeros]
        both = lax.dot_general(
            eye[...],
            jnp.concatenate(parts, axis=0),
            (((1,), (1,)), ((), ())),
            preferred_element_type=jnp.float32,
        )
        put(y, both[:, :LANES])
        put(y + 1, both[:, LANES:])


def spread_shape(coeffs, cells_y, cells_z):
    return pltpu.VMEM((cells_z // LANES, cells_y * coeffs + 16, LANES), jnp.float32)


def cut_faces(field):
    coeffs, cells_x, cells_y, cells_z = field.shape
    parts = 9
    per_part = coeffs // parts
    rows = cells_x * HALO

    def kernel(field, pick_in, last, first, top, bottom, *scratch):
        buf, high, low, sems, out_sems, pick, pick_sem = scratch

        def load(i):
            here = pl.ds(i * per_part, per_part)
            return pltpu.make_async_copy(field.at[here], buf.at[here], sems.at[i])

        def saves(i):
            here = pl.ds(i * per_part, per_part)
            return [
                pltpu.make_async_copy(high.at[here], top.at[here], out_sems.at[0, i]),
                pltpu.make_async_copy(low.at[here], bottom.at[here], out_sems.at[1, i]),
                pltpu.make_async_copy(
                    buf.at[here, pl.ds(cells_x - HALO, HALO)], last.at[here], out_sems.at[2, i]
                ),
                pltpu.make_async_copy(
                    buf.at[here, pl.ds(0, HALO)], first.at[here], out_sems.at[3, i]
                ),
            ]

        choice = pltpu.make_async_copy(pick_in, pick, pick_sem)
        choice.start()
        for i in range(parts):
            load(i).start()
        choice.wait()

        def body(i, _):
            load(i).wait()
            for k in range(per_part):
                c = i * per_part + k
                chosen = jnp.dot(
                    pick[...],
                    buf[c].reshape(cells_x * cells_y, cells_z),
                    preferred_element_type=jnp.float32,
                ).astype(jnp.bfloat16)
                high[c] = chosen[:rows]
                low[c] = chosen[rows:]
            for save in saves(i):
                save.start()
            return 0

        lax.fori_loop(0, parts, body, 0)
        for i in range(parts):
            for save in saves(i):
                save.wait()

    pick = np.zeros((2 * rows, cells_x * cells_y), np.float32)
    for x in range(cells_x):
        for j in range(HALO):
            pick[x * HALO + j, x * cells_y + cells_y - HALO + j] = 1.0
            pick[rows + x * HALO + j, x * cells_y + j] = 1.0
    shapes = [(coeffs, HALO, cells_y, cells_z)] * 2 + [(coeffs, rows, cells_z)] * 2
    hbm = pl.BlockSpec(memory_space=pl.ANY)
    return pl.pallas_call(
        kernel,
        out_shape=[pltpu.HBM(shape, jnp.bfloat16) for shape in shapes],
        in_specs=[hbm, hbm],
        out_specs=[hbm] * 4,
        scratch_shapes=[
            pltpu.VMEM(field.shape, jnp.bfloat16),
            pltpu.VMEM((coeffs, rows, cells_z), jnp.bfloat16),
            pltpu.VMEM((coeffs, rows, cells_z), jnp.bfloat16),
            pltpu.SemaphoreType.DMA((parts,)),
            pltpu.SemaphoreType.DMA((4, parts)),
            pltpu.VMEM(pick.shape, jnp.bfloat16),
            pltpu.SemaphoreType.DMA(()),
        ],
        compiler_params=pltpu.CompilerParams(vmem_limit_bytes=16 * MIB),
        name="cut_faces",
    )(
        field,
        pltpu.with_memory_space_constraint(jnp.asarray(pick.astype(jnp.bfloat16)), pltpu.HBM),
    )


def cut_corners(ylo, yhi):
    coeffs, rows, cells_z = ylo.shape
    per_step = 27
    corner = HALO * HALO

    def kernel(ylo, yhi, pick, up, down):
        for c in range(per_step):
            chosen = jnp.dot(
                pick[...],
                jnp.concatenate([ylo[c], yhi[c]], axis=0),
                preferred_element_type=jnp.float32,
            )
            up[c] = chosen[: 2 * corner].astype(jnp.bfloat16)
            down[c] = chosen[2 * corner :].astype(jnp.bfloat16)

    pick = np.zeros((4 * corner, 2 * rows), np.float32)
    for side in range(2):
        for i in range(corner):
            pick[side * corner + i, side * rows + rows - corner + i] = 1.0
            pick[2 * corner + side * corner + i, side * rows + i] = 1.0
    shape = (coeffs, 2 * corner, cells_z)
    face = pl.BlockSpec((per_step, rows, cells_z), lambda i: (i, 0, 0))
    piece = pl.BlockSpec((per_step,) + shape[1:], lambda i: (i, 0, 0))
    return pl.pallas_call(
        kernel,
        out_shape=[pltpu.HBM(shape, jnp.bfloat16)] * 2,
        grid=(coeffs // per_step,),
        in_specs=[face, face, pl.BlockSpec(pick.shape, lambda i: (0, 0))],
        out_specs=[piece, piece],
        compiler_params=pltpu.CompilerParams(vmem_limit_bytes=16 * MIB),
        name="cut_corners",
    )(ylo, yhi, jnp.asarray(pick.astype(jnp.bfloat16)))


def add_planes(table, planes, halves, eye, first_plane, total_rows, edge_lines):
    source = planes[0][0]
    coeffs, cells_y, cells_z = source.shape[0], source.shape[-2], source.shape[-1]
    count = len(planes)
    arrays = []
    for array, _ in planes:
        if not any(array is other for other in arrays):
            arrays.append(array)
    places = [next(i for i, o in enumerate(arrays) if o is array) for array, _ in planes]
    new = table is None

    def kernel(*refs):
        refs = list(refs)
        if not new:
            refs.pop(0)
        inputs = [refs.pop(0) for _ in arrays]
        shared = [refs.pop(0) for _ in halves]
        eye_in = refs.pop(0)
        table = refs.pop(0)
        edges = [refs.pop(0) for _ in range(2)] if edge_lines else []
        eye, eye_sem, buf, sems, spread = refs[:5]
        refs = refs[2:]
        copies = []
        for p, ((_, at), place) in enumerate(zip(planes, places)):
            ref = inputs[place] if at is None else inputs[place].at[:, at]
            copies.append(pltpu.make_async_copy(ref, buf.at[p], sems.at[p]))
        for q, piece in enumerate(shared):
            copies.append(pltpu.make_async_copy(piece, refs[3].at[q], refs[4].at[q]))
        for copy in copies:
            copy.start()
        eye_copy = pltpu.make_async_copy(eye_in, eye, eye_sem)
        eye_copy.start()
        eye_copy.wait()

        def turn(p):
            def put(y, block):
                at = pl.multiple_of(((first_plane + p) * cells_y + y) * cells_z, 8)
                table[pl.ds(at, cells_z), :] = block

            turn_rows(spread, eye, coeffs, cells_y, cells_z, put)

        def one(p, _):
            first = inputs[0] if planes[0][1] is None else inputs[0].at[:, 0]
            pltpu.make_async_copy(first, buf.at[p], sems.at[p]).wait()
            fill_rows(
                lambda c, h: buf[p, c, :, h * LANES : (h + 1) * LANES],
                spread,
                coeffs,
                cells_y,
                cells_z,
            )
            turn(p)
            return 0

        lax.fori_loop(0, count, one, 0)
        if halves:
            for copy in copies[count:]:
                copy.wait()
            fill_rows(
                lambda c, h: jnp.concatenate(
                    [
                        refs[3][q, c, :, h * LANES : (h + 1) * LANES].astype(jnp.float32)
                        for q in range(2)
                    ],
                    axis=0,
                ),
                spread,
                coeffs,
                cells_y,
                cells_z,
            )
            turn(count)
        for out, start in zip(edges, (0, cells_z - HALO)):
            for j in range(HALO):
                for line in range(0, edge_lines, 16):
                    parts = [
                        table[pl.ds((line + i) * cells_z + start + j, 8, stride=cells_z), :]
                        for i in (0, 8)
                    ]
                    at = j * edge_lines + line
                    out[at : at + 16, :] = jnp.concatenate(parts, axis=0).astype(jnp.bfloat16)

    vmem = pl.BlockSpec(memory_space=pltpu.VMEM)
    hbm = pl.BlockSpec(memory_space=pl.ANY)
    shapes = [pltpu.VMEM((total_rows, LANES), jnp.float32)]
    if edge_lines:
        shapes += [jax.ShapeDtypeStruct((HALO * edge_lines, LANES), jnp.bfloat16)] * 2
    scratch = [
        pltpu.VMEM(eye.shape, eye.dtype),
        pltpu.SemaphoreType.DMA(()),
        pltpu.VMEM((count, coeffs, cells_y, cells_z), jnp.bfloat16),
        pltpu.SemaphoreType.DMA((count,)),
        spread_shape(coeffs, cells_y, cells_z),
    ]
    if halves:
        scratch += [
            pltpu.VMEM((2, coeffs, cells_y // 2, cells_z), jnp.bfloat16),
            pltpu.SemaphoreType.DMA((2,)),
        ]
    held = [] if new else [table]
    return pl.pallas_call(
        kernel,
        out_shape=shapes,
        in_specs=[vmem] * len(held) + [hbm] * (len(arrays) + len(halves) + 1),
        out_specs=[vmem] * len(shapes),
        scratch_shapes=scratch,
        input_output_aliases={} if new else {0: 0},
        compiler_params=pltpu.CompilerParams(vmem_limit_bytes=TABLE_LIMIT * MIB),
        cost_estimate=pl.CostEstimate(
            flops=2 * 10**10, transcendentals=0, bytes_accessed=2 * 10**7
        ),
    )(*held, *arrays, *halves, eye)


def cut_ends(zlo, zhi, lines, cells_x, cells_y):
    own = cells_x * cells_y
    half = HALO * cells_y + 2 * HALO * HALO
    rows = 2 * HALO * half

    def kernel(zlo, zhi, pick, up, down):
        both = jnp.concatenate([zlo[...], zhi[...]], axis=0)
        chosen = jnp.dot(pick[...], both, preferred_element_type=jnp.float32)
        up[...] = chosen[:rows].astype(jnp.bfloat16)
        down[...] = chosen[rows:].astype(jnp.bfloat16)

    pick = np.zeros((2 * rows, 2 * HALO * lines), np.float32)
    for side in range(2):
        x = cells_x - HALO if side == 0 else 0
        places = [x * cells_y + i for i in range(HALO * cells_y)]
        for face in range(2):
            at = own + face * cells_y + x * HALO
            places += [at + i for i in range(HALO * HALO)]
        for z in range(2 * HALO):
            for i, place in enumerate(places):
                pick[side * rows + z * half + i, z * lines + place] = 1.0
    vmem = pl.BlockSpec(memory_space=pltpu.VMEM)
    return pl.pallas_call(
        kernel,
        out_shape=[jax.ShapeDtypeStruct((rows, LANES), jnp.bfloat16)] * 2,
        in_specs=[vmem] * 3,
        out_specs=[vmem] * 2,
        compiler_params=pltpu.CompilerParams(vmem_limit_bytes=8 * MIB),
        name="cut_ends",
    )(zlo, zhi, jnp.asarray(pick.astype(jnp.bfloat16)))


TABLE_LIMIT = 24
GROUP = 8
PARTS = 3


def prepare(samples, weights, slot, origin, cells, total):
    count = slot.shape[0]
    cells_x, cells_y, cells_z = cells
    own_lines = cells_x * cells_y
    early = own_lines + 2 * cells_y
    rows = (early + (2 * HALO + 1) * cells_y) * cells_z
    block = 256
    burst = 32
    kinds = (2 + PARTS) * SAMPLES
    corner = HALO * HALO
    end = HALO * cells_y + 2 * corner

    def locate(near_x, near_y, near_z):
        own_x = (near_x >= HALO) & (near_x < HALO + cells_x)
        own_y = (near_y >= HALO) & (near_y < HALO + cells_y)
        low_x = near_x < HALO
        low_y = near_y < HALO
        side_x = jnp.where(low_x, near_x, near_x - HALO - cells_x)
        side_y = jnp.where(low_y, near_y, near_y - HALO - cells_y)
        line_own = (near_x - HALO) * cells_y + near_y - HALO
        line_y = own_lines + jnp.where(low_y, 0, cells_y) + (near_x - HALO) * HALO + side_y
        line_early = jnp.where(own_y, line_own, line_y)
        in_face = side_x * cells_y + near_y - HALO
        in_corner = jnp.where(low_y, 0, corner) + side_x * HALO + side_y
        line_late = early + jnp.where(
            own_y,
            jnp.where(low_x, 0, HALO * cells_y) + in_face,
            2 * HALO * cells_y + jnp.where(low_x, 0, 2 * corner) + in_corner,
        )
        line = jnp.where(own_x, line_early, line_late)
        edge = jnp.where(near_z < HALO, near_z, near_z - cells_z)
        at_end = jnp.where(own_y, in_face, HALO * cells_y + in_corner)
        beyond = jnp.where(
            own_x,
            edge * early + line_early,
            2 * HALO * early + jnp.where(low_x, 0, 2 * HALO * end) + edge * end + at_end,
        )
        inside = (near_z >= HALO) & (near_z < HALO + cells_z)
        return jnp.where(inside, line * cells_z + near_z - HALO, rows + beyond)

    def kernel(origin, slot, samples, weights, eye, join, index, ordered, natural):
        def turn(j, _):
            at = pl.multiple_of(j * block, block)
            near = []
            for d in range(3):
                shift = samples[d, :, pl.ds(at, block)] - origin[d] + HALO
                shift = jnp.where(shift < 0, shift + total[d], shift)
                near.append(jnp.where(shift >= total[d], shift - total[d], shift))
            row = locate(*near)
            pieces = [(row >> 8).astype(jnp.float32), (row & 255).astype(jnp.float32)]
            rest = weights[:, pl.ds(at, block)]
            for _ in range(PARTS):
                piece = rest.astype(jnp.bfloat16).astype(jnp.float32)
                pieces.append(piece)
                rest = rest - piece
            pieces.append(jnp.zeros((LANES - kinds, block), jnp.float32))
            natural[pl.ds(at, block), :] = lax.dot_general(
                eye[...],
                jnp.concatenate(pieces, axis=0).astype(jnp.bfloat16),
                (((1,), (1,)), ((), ())),
                preferred_element_type=jnp.float32,
            )
            return 0

        lax.fori_loop(0, count // block, turn, 0)

        def scatter(j, _):
            at = pl.multiple_of(j * burst, burst)
            mine = slot.at[pl.ds(at, burst)]
            for g in range(0, burst, GROUP):
                tile = natural[pl.ds(at + g, GROUP), :]
                for k in range(GROUP):
                    ordered[pl.ds(mine[g + k], 1), :] = tile[k : k + 1, :]
            return 0

        lax.fori_loop(0, count // burst, scatter, 0)

        def collect(j, _):
            at = pl.multiple_of(j * 4 * LANES, 4 * LANES)
            wide = lax.dot_general(
                join[...],
                ordered[pl.ds(at, 4 * LANES), :].astype(jnp.bfloat16),
                (((1,), (1,)), ((), ())),
                preferred_element_type=jnp.float32,
            ).astype(jnp.int32)
            for i in range(4):
                to = pl.multiple_of((j * 4 + i) * SAMPLES, SAMPLES)
                index[pl.ds(to, SAMPLES), :] = wide[:SAMPLES, i * LANES : (i + 1) * LANES]
            return 0

        lax.fori_loop(0, count // (4 * LANES), collect, 0)

    join = np.zeros((16, LANES), np.float32)
    for s in range(SAMPLES):
        join[s, s] = 256.0
        join[s, SAMPLES + s] = 1.0
    vmem = pl.BlockSpec(memory_space=pltpu.VMEM)
    smem = pl.BlockSpec(memory_space=pltpu.SMEM)
    return pl.pallas_call(
        kernel,
        out_shape=(
            jax.ShapeDtypeStruct((count * SAMPLES // LANES, LANES), jnp.int32),
            jax.ShapeDtypeStruct((count, LANES), jnp.float32),
        ),
        in_specs=[smem, smem, vmem, vmem, vmem, vmem],
        out_specs=(vmem, vmem),
        scratch_shapes=[pltpu.VMEM((count, LANES), jnp.float32)],
        compiler_params=pltpu.CompilerParams(vmem_limit_bytes=12 * MIB),
        cost_estimate=pl.CostEstimate(
            flops=2 * 10**10, transcendentals=0, bytes_accessed=3 * 10**6
        ),
        name="prepare",
    )(
        origin,
        slot,
        samples,
        weights,
        jnp.asarray(np.eye(block, dtype=np.float32).astype(jnp.bfloat16)),
        jnp.asarray(join.astype(jnp.bfloat16)),
    )


def spread_weights(ordered):
    count = ordered.shape[0]
    block = 512

    def kernel(ordered, ones, wide):
        rows = ordered[...].astype(jnp.bfloat16)
        for h in range(0, SAMPLES, 2):
            both = jnp.dot(
                rows, ones[:, h * LANES : (h + 2) * LANES], preferred_element_type=jnp.float32
            )
            for s in range(2):
                for g in range(block // GROUP):
                    to = (g * SAMPLES + h + s) * GROUP
                    wide[to : to + GROUP, :] = both[
                        g * GROUP : (g + 1) * GROUP, s * LANES : (s + 1) * LANES
                    ]

    ones = np.zeros((LANES, SAMPLES * LANES), np.float32)
    for s in range(SAMPLES):
        for p in range(PARTS):
            ones[(2 + p) * SAMPLES + s, s * LANES : (s + 1) * LANES] = 1.0
    return pl.pallas_call(
        kernel,
        out_shape=pltpu.HBM((count * SAMPLES, LANES), jnp.float32),
        grid=(count // block,),
        in_specs=[
            pl.BlockSpec((block, LANES), lambda i: (i, 0)),
            pl.BlockSpec(ones.shape, lambda i: (0, 0)),
        ],
        out_specs=pl.BlockSpec((block * SAMPLES, LANES), lambda i: (i, 0)),
        compiler_params=pltpu.CompilerParams(vmem_limit_bytes=12 * MIB),
        cost_estimate=pl.CostEstimate(
            flops=10**10, transcendentals=0, bytes_accessed=3 * 10**6
        ),
        name="spread_weights",
    )(ordered, jnp.asarray(ones.astype(jnp.bfloat16)))


RING = 4
STREAM = 8
CHUNK = 1024


def gather_rows(index, wide, table, edges, first_edge, coeffs):
    count = wide.shape[0] // SAMPLES
    chunks = index.shape[0] // CHUNK
    per_chunk = CHUNK // SAMPLES
    groups = per_chunk // GROUP
    pairs = count // 32
    half = LANES // 2

    def kernel(index, wide, pick, *refs):
        table, out, local, sems, near, near_sems, rows, staged, out_sems = refs[len(edges) + 1 :]
        sublane = lax.broadcasted_iota(jnp.int32, (GROUP, LANES), 0)
        masks = [sublane == k for k in range(GROUP)]
        used = lax.broadcasted_iota(jnp.int32, (GROUP, LANES), 1) < coeffs

        def fetch(n, slot):
            return pltpu.make_async_copy(
                index.at[pl.ds(pl.multiple_of(n * CHUNK, CHUNK), CHUNK)],
                local.at[slot],
                sems.at[slot],
            )

        def stream(n, slot):
            return pltpu.make_async_copy(
                wide.at[pl.ds(pl.multiple_of(n * CHUNK, CHUNK), CHUNK), :],
                near.at[slot],
                near_sems.at[slot],
            )

        dests = groups // 4

        def save(n):
            here = pl.ds(n * dests, dests)
            return pltpu.make_async_copy(staged.at[here], out.at[here], out_sems.at[n])

        def pack(n):
            span = dests * GROUP
            at = pl.multiple_of(n * span, span)
            part = [rows[q, pl.ds(at, span), :].astype(jnp.bfloat16) for q in range(4)]
            even = jnp.concatenate([part[0], part[2]], axis=1)
            odd = jnp.concatenate([part[1], part[3]], axis=1)
            first = jnp.dot(even, pick[0], preferred_element_type=jnp.float32)
            second = jnp.dot(odd, pick[0], preferred_element_type=jnp.float32)
            third = jnp.dot(even, pick[1], preferred_element_type=jnp.float32)
            third += jnp.dot(odd, pick[2], preferred_element_type=jnp.float32)
            for d in range(dests):
                here = slice(d * GROUP, (d + 1) * GROUP)
                staged[n * dests + d, :16, :] = jnp.concatenate(
                    [first[here], second[here]], axis=0
                ).astype(jnp.bfloat16)
                staged[n * dests + d, 16:, :] = third[here].astype(jnp.bfloat16)

        for b in range(RING - 1):
            fetch(b, b).start()
        for b in range(STREAM - 1):
            stream(b, b).start()

        at = first_edge
        for edge in refs[: len(edges)]:
            table[pl.ds(at, edge.shape[0]), :] = edge[...].astype(jnp.float32)
            at += edge.shape[0]

        def body(i, _):
            for b in range(RING):
                n = i * RING + b
                slot = n % STREAM
                fetch(n, b).wait()
                stream(n, slot).wait()
                ahead = n + RING - 1
                later = n + STREAM - 1

                @pl.when(ahead < chunks)
                def _():
                    fetch(ahead, (b + RING - 1) % RING).start()

                @pl.when(later < chunks)
                def _():
                    stream(later, later % STREAM).start()

                @pl.when(n > 1)
                def _():
                    save(n - 2).start()

                pack(jnp.maximum(n - 1, 0))

                for q in range(groups):
                    total = None
                    for s in range(SAMPLES):
                        merged = None
                        for k in range(GROUP):
                            place = s * per_chunk + q * GROUP + k
                            row = table[pl.ds(local[b, place], GROUP, stride=0), :]
                            merged = row if merged is None else jnp.where(masks[k], row, merged)
                        at = (q * SAMPLES + s) * GROUP
                        term = merged * near[slot, at : at + GROUP, :]
                        total = term if total is None else total + term
                    to = pl.multiple_of((n * (groups // 4) + q // 4) * GROUP, GROUP)
                    rows[q % 4, pl.ds(to, GROUP), :] = jnp.where(used, total, 0.0)
            return 0

        lax.fori_loop(0, chunks // RING, body, 0)

        save(chunks - 2).start()
        pack(chunks - 1)
        save(chunks - 1).start()
        for n in range(chunks):
            save(n).wait()

    pick = np.zeros((3, 2 * LANES, LANES), np.float32)
    for c in range(half):
        pick[0, c, c] = 1.0
        pick[0, LANES + c, half + c] = 1.0
    for c in range(32):
        pick[1, half + c, c] = 1.0
        pick[1, LANES + half + c, 64 + c] = 1.0
        pick[2, half + c, 32 + c] = 1.0
        pick[2, LANES + half + c, 96 + c] = 1.0
    vmem = pl.BlockSpec(memory_space=pltpu.VMEM)
    return pl.pallas_call(
        kernel,
        out_shape=(
            pltpu.VMEM(table.shape, jnp.float32),
            pltpu.HBM((pairs, 24, LANES), jnp.bfloat16),
        ),
        in_specs=[pl.BlockSpec(memory_space=pl.ANY)] * 2 + [vmem] * (2 + len(edges)),
        out_specs=(vmem, pl.BlockSpec(memory_space=pl.ANY)),
        scratch_shapes=[
            pltpu.SMEM((RING, CHUNK), jnp.int32),
            pltpu.SemaphoreType.DMA((RING,)),
            pltpu.VMEM((STREAM, CHUNK, LANES), jnp.float32),
            pltpu.SemaphoreType.DMA((STREAM,)),
            pltpu.VMEM((4, pairs * GROUP, LANES), jnp.float32),
            pltpu.VMEM((pairs, 24, LANES), jnp.bfloat16),
            pltpu.SemaphoreType.DMA((chunks,)),
        ],
        input_output_aliases={3 + len(edges): 0},
        compiler_params=pltpu.CompilerParams(vmem_limit_bytes=24 * MIB),
        cost_estimate=pl.CostEstimate(
            flops=4 * 10**10, transcendentals=0, bytes_accessed=2 * 10**7
        ),
        name="gather_rows",
    )(index, wide, jnp.asarray(pick.astype(jnp.bfloat16)), *edges, table)[1]


def relight(transfer, routed, basis, projector):
    coeffs, count = transfer.shape
    sources, packed, _ = routed.shape
    per_pair = count // sources
    block = 512
    step = block // per_pair

    def kernel(transfer, routed, basis, wide, projector, out):
        low = lax.broadcasted_iota(jnp.int32, (GROUP, LANES), 1) < 64
        parts = []
        for i in range(step):
            head = routed[i, :16, :].astype(jnp.float32)
            first, second = head[:GROUP], head[GROUP:]
            third = routed[i, 16:, :].astype(jnp.float32)
            parts += [
                jnp.where(low, first, pltpu.roll(third, 64, 1)),
                jnp.where(low, second, pltpu.roll(third, 32, 1)),
                jnp.where(low, pltpu.roll(first, 64, 1), third),
                jnp.where(low, pltpu.roll(second, 64, 1), pltpu.roll(third, 96, 1)),
            ]
        rows = jnp.concatenate(parts, axis=0).astype(jnp.bfloat16)
        lit = jnp.dot(basis[...], transfer[...], preferred_element_type=jnp.float32)
        shade = lax.dot_general(
            wide[...], rows, (((1,), (1,)), ((), ())), preferred_element_type=jnp.float32
        )
        product = (lit * shade).astype(jnp.bfloat16)
        out[...] = jnp.dot(projector[...], product, preferred_element_type=jnp.float32).astype(
            jnp.bfloat16
        )

    directions = basis.shape[0]
    wide = np.zeros((directions, LANES), jnp.bfloat16)
    wide[:, :coeffs] = basis
    return pl.pallas_call(
        kernel,
        out_shape=jax.ShapeDtypeStruct((coeffs, count), jnp.bfloat16),
        grid=(count // block,),
        in_specs=[
            pl.BlockSpec((coeffs, block), lambda i: (0, i)),
            pl.BlockSpec((step, packed, LANES), lambda i: (i, 0, 0)),
            pl.BlockSpec((directions, coeffs), lambda i: (0, 0)),
            pl.BlockSpec((directions, LANES), lambda i: (0, 0)),
            pl.BlockSpec((coeffs, directions), lambda i: (0, 0)),
        ],
        out_specs=pl.BlockSpec((coeffs, block), lambda i: (0, i)),
        compiler_params=pltpu.CompilerParams(vmem_limit_bytes=40 * MIB),
        name="relight",
    )(transfer, routed, jnp.asarray(basis), jnp.asarray(wide), jnp.asarray(projector))


def moves(sizes, steps):
    pairs = []
    for x in range(sizes[0]):
        for y in range(sizes[1]):
            to_x, to_y = (x + steps[0]) % sizes[0], (y + steps[1]) % sizes[1]
            pairs.append((x * sizes[1] + y, to_x * sizes[1] + to_y))
    return pairs


def shift(array, axis, pairs):
    return pltpu.with_memory_space_constraint(lax.ppermute(array, axis, pairs), pltpu.HBM)


def halo_step(field, samples, weights, destination, transfer):
    basis, projector = direction_tables()
    coeffs, cells_x, cells_y, cells_z = field.shape
    count = transfer.shape[1]
    along = tuple(lax.axis_size(axis) for axis in ("gx", "gy", "gz"))
    ups = [moves((n, 1), (1, 0)) for n in along]
    downs = [moves((n, 1), (-1, 0)) for n in along]

    cells = (cells_x, cells_y, cells_z)
    total = tuple(c * n for c, n in zip(cells, along))
    origin = jnp.stack(
        [lax.axis_index(axis) * c for axis, c in zip(("gx", "gy", "gz"), cells)]
    ).astype(jnp.int32)
    devices = math.prod(along)
    per_pair = count // devices
    slot = destination[0] * per_pair + destination[1]

    field = pltpu.with_memory_space_constraint(field, pltpu.HBM)
    last, first, top, bottom = cut_faces(field)
    ylo = shift(top, "gy", ups[1])
    yhi = shift(bottom, "gy", downs[1])
    xlo = shift(last, "gx", ups[0])
    xhi = shift(first, "gx", downs[0])
    field, slot, origin = lax.optimization_barrier((field, slot, origin))

    eye = jnp.asarray(np.eye(cells_z, dtype=np.float32).astype(jnp.bfloat16))
    early = (cells_x + 2) * cells_y
    rows = (early + (2 * HALO + 1) * cells_y) * cells_z
    ends = HALO * cells_y + 2 * HALO * HALO
    total_rows = rows + 2 * HALO * (early + 2 * ends)
    own = [(field, x) for x in range(cells_x)]
    table = add_planes(None, own, (), eye, 0, total_rows, 0)[0]
    index, ordered = prepare(samples, weights, slot, origin, cells, total)
    table, index, ordered, ylo, yhi = lax.optimization_barrier((table, index, ordered, ylo, yhi))
    up, down = cut_corners(ylo, yhi)
    up, down, table = lax.optimization_barrier((up, down, table))
    clo = shift(up, "gx", ups[0])
    chi = shift(down, "gx", downs[0])
    table, bottoms, tops = add_planes(
        table, [(ylo, None), (yhi, None)], (), eye, cells_x, total_rows, early
    )
    zhi = lax.ppermute(bottoms, "gz", downs[2])
    zlo = lax.ppermute(tops, "gz", ups[2])
    bottoms, tops, ordered = lax.optimization_barrier((bottoms, tops, ordered))
    wide = spread_weights(ordered)
    zlo, zhi, wide = lax.optimization_barrier((zlo, zhi, wide))
    up, down = cut_ends(zlo, zhi, early, cells_x, cells_y)
    elo = lax.ppermute(up, "gx", ups[0])
    ehi = lax.ppermute(down, "gx", downs[0])
    sides = [(xlo, 0), (xlo, 1), (xhi, 0), (xhi, 1)]
    table = add_planes(table, sides, (clo, chi), eye, cells_x + 2, total_rows, 0)[0]
    outgoing = gather_rows(
        index.reshape(-1), wide, table, (zlo, zhi, elo, ehi), rows, coeffs
    )
    routed = lax.all_to_all(
        outgoing, ("gx", "gy", "gz"), split_axis=0, concat_axis=0, tiled=True
    )
    return relight(transfer, routed, basis, projector)


def solution(mesh):
    placed = (
        P(None, "gx", "gy", "gz"),
        P(None, None, ("gx", "gy", "gz")),
        P(None, ("gx", "gy", "gz")),
        P(None, ("gx", "gy", "gz")),
        P(None, ("gx", "gy", "gz")),
    )
    return jax.shard_map(
        halo_step,
        mesh=mesh,
        in_specs=placed,
        out_specs=P(None, ("gx", "gy", "gz")),
        check_vma=False,
    )
```
